32 devices in a mesh: section: 2 (over core), dp: 16 (over z, y, x).
Axes of the slice: x: 2, y: 2, z: 4, core: 2. Of those that a mesh axis runs over, the one named last changes fastest.
Arguments:
- tokens: bfloat16 [2, 16, 80, 1024], P(None, 'dp'), may hold values from -6 to 6
- w_qkv: bfloat16 [2, 1024, 1536], P('section', 'dp'), may hold values from -0.1875 to 0.1875
- w_output: bfloat16 [2, 512, 1024], P('section', None, 'dp'), may hold values from -0.25 to 0.25
- tangent_value: bfloat16 [2, 2, 1024, 512], P('section', None, 'dp'), may hold values from -0.1875 to 0.1875
- tangent_output: bfloat16 [2, 2, 512, 1024], P('section', None, None, 'dp'), may hold values from -0.25 to 0.25
- layer_gain: float32 [2, 1024], P('section'), may hold values from 0.5 to 1.5
- final_gain: float32 [1024], replicated, may hold values from 0.5 to 1.5
- head: bfloat16 [1024, 1000], P(None, 'section'), may hold values from -0.1875 to 0.1875
Outputs:
- mean_logits: float32 [2, 16, 1000], P(None, 'dp', 'section')
- variance: float32 [2, 16, 1000], P(None, 'dp', 'section')
The draws below stay inside these ranges and needn't reach their ends.
All inputs are finite; a program needn't handle non-finite values.
Results may differ from the reference program's by a relative error of at most 0.018.
Values may be sent and summed in bfloat16 or wider, within the bound.
A program may use at most 64 MiB of HBM per device.

```python
import jax
import jax.numpy as jnp
from jax import lax

D = 1024
HEADS = 8
HEAD = 64
CLASSES = 1000
TOK = 80
TANGENTS = 2
MICRO = 2
HD = 512
IMAGES = 16
SECTIONS = 2
N_SECTION = 2


def level_of(rng, extent, cuts, least, largest):
    def one(dim, shards_of):
        draws = jax.random.uniform(jax.random.fold_in(jax.random.fold_in(rng, 6), dim), (shards_of,), jnp.float32, least / len(cuts), largest / len(cuts))
        return jnp.repeat(jnp.exp(draws), extent[dim] // shards_of).reshape((-1,) + (1,) * (len(extent) - dim - 1))

    factor_of = one(*cuts[0])
    for cut in cuts[1:]:
        factor_of = factor_of * one(*cut)
    return factor_of


def bell_draw(stream_key, extent, spread, reach, split=(), held_as=jnp.bfloat16):
    result = jax.random.normal(stream_key, extent, jnp.float32) * spread
    if len(split) > 0:
        result = level_of(stream_key, extent, split, -0.22, 0.18) * result
    return jnp.clip(result, min=-reach, max=reach).astype(held_as)


def setup_inputs(seed: int = 0) -> dict:
    key_of = jax.random.split(jax.random.key(seed), 9)
    tokens = bell_draw(key_of[0], (MICRO, IMAGES, TOK, D), 1.0, 6.0, ((1, 16),))
    w_qkv = bell_draw(key_of[1], (SECTIONS, D, 3 * HD), D ** -0.5, 0.1875, ((0, 2), (1, 16)))
    w_output = bell_draw(key_of[2], (SECTIONS, HD, D), HD ** -0.5, 0.25, ((0, 2), (2, 16)))
    tangent_value = bell_draw(key_of[3], (SECTIONS, TANGENTS, D, HD), D ** -0.5, 0.1875, ((0, 2), (2, 16)))
    tangent_output = bell_draw(key_of[4], (SECTIONS, TANGENTS, HD, D), HD ** -0.5, 0.25, ((0, 2), (3, 16)))
    layer_gain = jnp.clip(1.0 + 0.1 * jax.random.normal(key_of[5], (SECTIONS, D), jnp.float32), 0.5, 1.5)
    final_gain = jnp.clip(1.0 + 0.1 * jax.random.normal(key_of[6], (D,), jnp.float32), 0.5, 1.5)
    head = bell_draw(key_of[7], (D, CLASSES), D ** -0.5, 0.1875, ((1, 2),))
    return {"tokens": tokens, "w_qkv": w_qkv, "w_output": w_output, "tangent_value": tangent_value, "tangent_output": tangent_output, "layer_gain": layer_gain, "final_gain": final_gain, "head": head}


epsilon = 1e-06

def widen(array):
    return array.astype(jnp.float32)

def norm_jvp(primal, tangents, gains):
    average = lax.optimization_barrier(jnp.mean(primal, -1, keepdims=True))
    centred = primal - average
    inverse = lax.rsqrt(lax.optimization_barrier(jnp.mean(centred * centred, -1, keepdims=True)) + epsilon)
    dcentred = tangents - lax.optimization_barrier(jnp.mean(tangents, -1, keepdims=True))
    dinverse = -inverse ** 3 * lax.optimization_barrier(jnp.mean(centred * dcentred, -1, keepdims=True))
    return (centred * inverse * gains, (dcentred * inverse + centred * dinverse) * gains)

def layer_step(state, qkv_weight, out_weight, value_tangent, out_tangent, gains):
    resid = widen(state)
    normed_zero, normed_rest = norm_jvp(resid[0], resid[1:], gains)
    normed = jnp.concatenate([normed_zero[None], normed_rest]).astype(jnp.bfloat16)
    streams, batch, tokens_here, width = normed.shape
    projected = jnp.einsum('sbtd,de->sbte', widen(normed), widen(qkv_weight))
    extra_value = jnp.einsum('btd,kde->kbte', widen(normed[0]), widen(value_tangent))
    queries = projected[..., :HD]
    key_rows = projected[..., HD:2 * HD]
    values = projected[..., 2 * HD:]
    values = jnp.concatenate([values[:1], values[1:] + extra_value])
    shape_heads = (streams, batch, tokens_here, HEADS, HEAD)
    queries = queries.astype(jnp.bfloat16).reshape(shape_heads)
    key_rows = key_rows.astype(jnp.bfloat16).reshape(shape_heads)
    values = values.astype(jnp.bfloat16).reshape(shape_heads)
    factor = HEAD ** (-0.5)
    scores = jnp.einsum('bqhe,bkhe->bhqk', widen(queries[0]), widen(key_rows[0])) * factor
    probs = jax.nn.softmax(scores, -1)
    dscores = (jnp.einsum('sbqhe,bkhe->sbhqk', widen(queries[1:]), widen(key_rows[0])) + jnp.einsum('bqhe,sbkhe->sbhqk', widen(queries[0]), widen(key_rows[1:]))) * factor
    dprobs = probs * (dscores - lax.optimization_barrier(jnp.sum(probs * dscores, -1, keepdims=True)))
    probs_low = probs.astype(jnp.bfloat16)
    dprobs_low = dprobs.astype(jnp.bfloat16)
    attended_zero = jnp.einsum('bhqk,bkhe->bqhe', widen(probs_low), widen(values[0]))
    attended_rest = jnp.einsum('sbhqk,bkhe->sbqhe', widen(dprobs_low), widen(values[0])) + jnp.einsum('bhqk,sbkhe->sbqhe', widen(probs_low), widen(values[1:]))
    attended = jnp.concatenate([attended_zero[None], attended_rest]).astype(jnp.bfloat16)
    attended = attended.reshape(streams, batch, tokens_here, HD)
    output = jnp.einsum('sbte,ed->sbtd', widen(attended), widen(out_weight))
    extra_out = jnp.einsum('bte,ked->kbtd', widen(attended[0]), widen(out_tangent))
    output = jnp.concatenate([output[:1], output[1:] + extra_out])
    return (resid + output).astype(jnp.bfloat16)

def reference(tokens, w_qkv, w_output, tangent_value, tangent_output, layer_gain, final_gain, head):
    micro_count, image_count = (tokens.shape[0], tokens.shape[1])
    flat = tokens.reshape(micro_count * image_count, TOK, D)
    state = jnp.concatenate([flat[None], jnp.zeros((TANGENTS, micro_count * image_count, TOK, D), jnp.bfloat16)])
    for layer in range(N_SECTION):
        state = layer_step(state, w_qkv[layer], w_output[layer], tangent_value[layer], tangent_output[layer], layer_gain[layer])
    class_rows = widen(state[:, :, 0, :])
    final_zero, final_rest = norm_jvp(class_rows[0], class_rows[1:], final_gain)
    normed_final = jnp.concatenate([final_zero[None], final_rest]).astype(jnp.bfloat16)
    logits = jnp.einsum('sbd,dc->sbc', widen(normed_final), widen(head))
    mean_logits = logits[0].reshape(micro_count, image_count, CLASSES)
    variance = lax.optimization_barrier(jnp.sum(logits[1:] * logits[1:], 0)).reshape(micro_count, image_count, CLASSES)
    return (mean_logits, variance)
```

```python
import functools

import jax
import jax.numpy as jnp
from jax import lax
from jax.experimental import pallas as pl
from jax.experimental.pallas import tpu as pltpu
from jax.sharding import PartitionSpec as P

HEAD = 64
epsilon = 1e-06
F32, BF16 = jnp.float32, jnp.bfloat16
MESH = pl.DeviceIdType.MESH


def contract(spec, left, right):
    return jnp.einsum(spec, left, right, preferred_element_type=jnp.float32)


def norm_jvp(primal, tangents, gains):
    average = jnp.mean(primal, -1, keepdims=True)
    centred = primal - average
    inverse = lax.rsqrt(jnp.mean(centred * centred, -1, keepdims=True) + epsilon)
    dcentred = tangents - jnp.mean(tangents, -1, keepdims=True)
    dinverse = -(inverse**3) * jnp.mean(centred * dcentred, -1, keepdims=True)
    return (centred * inverse * gains, (dcentred * inverse + centred * dinverse) * gains)


def layer_step(state, qkv_weight, out_weight, value_tangent, out_tangent, gains):
    hd = out_weight.shape[0]
    heads = hd // HEAD
    resid = state.astype(F32)
    normed_zero, normed_rest = norm_jvp(resid[0], resid[1:], gains)
    normed = jnp.concatenate([normed_zero[None], normed_rest]).astype(BF16)
    streams, batch, tokens_here, width = normed.shape
    projected = contract("sbtd,de->sbte", normed, qkv_weight)
    extra_value = contract("btd,kde->kbte", normed[0], value_tangent)
    queries = projected[..., :hd]
    key_rows = projected[..., hd : 2 * hd]
    values = projected[..., 2 * hd :]
    values = jnp.concatenate([values[:1], values[1:] + extra_value])
    shape_heads = (streams, batch, tokens_here, heads, HEAD)
    queries = queries.astype(BF16).reshape(shape_heads)
    key_rows = key_rows.astype(BF16).reshape(shape_heads)
    values = values.astype(BF16).reshape(shape_heads)
    factor = HEAD ** (-0.5)
    scores = contract("bqhe,bkhe->bhqk", queries[0], key_rows[0]) * factor
    probs = jax.nn.softmax(scores, -1)
    dscores = (
        contract("sbqhe,bkhe->sbhqk", queries[1:], key_rows[0])
        + contract("bqhe,sbkhe->sbhqk", queries[0], key_rows[1:])
    ) * factor
    dprobs = probs * (dscores - jnp.sum(probs * dscores, -1, keepdims=True))
    probs_low = probs.astype(BF16)
    dprobs_low = dprobs.astype(BF16)
    attended_zero = contract("bhqk,bkhe->bqhe", probs_low, values[0])
    attended_rest = contract("sbhqk,bkhe->sbqhe", dprobs_low, values[0]) + contract(
        "bhqk,sbkhe->sbqhe", probs_low, values[1:]
    )
    attended = jnp.concatenate([attended_zero[None], attended_rest]).astype(BF16)
    attended = attended.reshape(streams, batch, tokens_here, hd)
    output = contract("sbte,ed->sbtd", attended, out_weight)
    extra_out = contract("bte,ked->kbtd", attended[0], out_tangent)
    output = jnp.concatenate([output[:1], output[1:] + extra_out])
    return (resid + output).astype(BF16)


def relay_shards(tokens, w_qkv, w_output, tangent_value, tangent_output, layer_gain, final_gain, head):
    full_qkv, full_output, full_value_tan, full_output_tan = (
        lax.all_gather(w_qkv, "dp", axis=1, tiled=True),
        lax.all_gather(w_output, "dp", axis=2, tiled=True),
        lax.all_gather(tangent_value, "dp", axis=2, tiled=True),
        lax.all_gather(tangent_output, "dp", axis=3, tiled=True),
    )
    tangents = tangent_value.shape[1]

    def advance_layer(state):
        return layer_step(
            state, full_qkv[0], full_output[0], full_value_tan[0], full_output_tan[0], layer_gain[0]
        )

    section_index = lax.axis_index("section")
    section_count = lax.axis_size("section")
    route = [(i, i + 1) for i in range(section_count - 1)]
    micro, _, toks, width = tokens.shape
    entering = jnp.concatenate(
        [tokens.reshape(1, micro, toks, width), jnp.zeros((tangents, micro, toks, width), BF16)]
    )

    def advance(step, outgoing):
        incoming = lax.ppermute(outgoing, "section", route)
        source = jnp.where(step == 0, entering, incoming)
        return lax.cond(section_index == step, advance_layer, jnp.zeros_like, source)

    finished = lax.fori_loop(0, section_count, advance, jnp.zeros_like(entering))
    collected = finished[:, :, 0, :]
    mine = section_index == section_count - 1
    features = lax.psum(jnp.where(mine, collected, jnp.zeros_like(collected)), "section")
    widened = features.astype(F32)
    final_zero, final_rest = norm_jvp(widened[0], widened[1:], final_gain)
    normed_final = jnp.concatenate([final_zero[None], final_rest]).astype(BF16)
    logits = contract("sbd,dc->sbc", normed_final, head)
    return (logits[0][:, None, :], jnp.sum(logits[1:] * logits[1:], 0)[:, None, :])


def dot(a, b):
    return lax.dot_general(a, b, (((1,), (0,)), ((), ())), preferred_element_type=F32)


def dot_t(a, b):
    return lax.dot_general(a, b, (((1,), (1,)), ((), ())), preferred_element_type=F32)


class Gather:
    def __init__(self, n, g, full, send, recv):
        self.nz = n // 4
        self.full, self.send, self.recv = full, send, recv
        self.rows = full.shape[1] // n
        self.g = g
        self.sends = []
        self.slot = 0

    def copy(self, src, half, target, slot):
        depth = self.rows // 2
        at = pl.ds(pl.multiple_of(src * self.rows + half * depth, depth), depth)
        ref = self.full.at[:, at, :]
        return pltpu.make_async_remote_copy(
            src_ref=ref,
            dst_ref=ref,
            send_sem=self.send.at[slot],
            recv_sem=self.recv.at[src, half],
            device_id={"section": self.g.section, "dp": target},
            device_id_type=MESH,
        )

    def forward(self, cond, src, half, target):
        slot = self.slot
        self.slot += 1

        def go():
            self.copy(src, half, target, slot).start()

        def end():
            self.copy(src, half, target, slot).wait_send()

        go() if cond is None else pl.when(cond)(go)
        self.sends.append((cond, end))

    def arrived(self, src, half):
        self.copy(src, half, self.g.me, 0).wait_recv()

    def direct(self, d):
        g = self.g
        for shift, cond in g.sources(d):
            src = g.me + 4 * shift
            for half in range(2):
                if d > 0:
                    pl.when(cond)(functools.partial(self.arrived, src, half))
                if shift <= 0 and d < self.nz - 1:
                    self.forward(g.up if cond is None else cond & g.up, src, half, g.me + 4)
                if shift >= 0 and d < self.nz - 1:
                    self.forward(g.down if cond is None else cond & g.down, src, half, g.me - 4)
                for target in ((g.y_near, g.x_near), (g.x_near, g.y_near))[half]:
                    self.forward(cond, src, half, target)

    def relay(self, d):
        g = self.g
        for shift, cond in g.sources(d):
            for half, near, target in ((0, g.x_near, g.y_near), (1, g.y_near, g.x_near)):
                src = near + 4 * shift
                wait = functools.partial(self.arrived, src, half)
                wait() if cond is None else pl.when(cond)(wait)
                self.forward(cond, src, half, target)

    def rest(self):
        g = self.g
        for z in range(self.nz):
            up = 4 * (z - g.z)
            self.arrived(g.x_near + up, 1)
            self.arrived(g.y_near + up, 0)
            self.arrived(g.diagonal + up, 0)
            self.arrived(g.diagonal + up, 1)

    def drain(self):
        for cond, end in self.sends:
            end() if cond is None else pl.when(cond)(end)


def send_slots(n):
    nz = n // 4
    return 2 * (4 + 3 * 2 * (nz - 1) + 2 * nz)


class Place:
    def __init__(self, n):
        self.nz = n // 4
        self.me = lax.axis_index("dp")
        self.section = lax.axis_index("section")
        me = self.me
        self.x_near = me + 1 - 2 * (me % 2)
        self.y_near = me + 2 - 4 * ((me // 2) % 2)
        self.diagonal = self.x_near + self.y_near - me
        self.z = me // 4
        self.place = me % 4
        self.up, self.down = self.z + 1 < self.nz, self.z >= 1
        self.plane = (me, self.x_near, self.y_near, self.diagonal)

    def sources(self, d):
        if d == 0:
            return [(0, None)]
        return [(-d, self.z >= d), (d, self.z + d < self.nz)]


def norm_rows(x, gains):
    average = jnp.mean(x, -1, keepdims=True)
    centred = x - average
    inverse = lax.rsqrt(jnp.mean(centred * centred, -1, keepdims=True) + epsilon)
    return centred, inverse, centred * inverse * gains


def norm_tangent(t, centred, inverse, gains):
    dcentred = t - jnp.mean(t, -1, keepdims=True)
    dinverse = -(inverse * inverse * inverse) * jnp.mean(centred * dcentred, -1, keepdims=True)
    return (dcentred * inverse + centred * dinverse) * gains


def softmax(scores):
    e = jnp.exp(scores - jnp.max(scores, -1, keepdims=True))
    return e / jnp.sum(e, -1, keepdims=True)


def at_rows(i, count):
    return pl.ds(pl.multiple_of(i * count, count), count)


def first_norm(sizes, tok, gain, normed, slot):
    micro, toks, width, hd, tangents = sizes
    for b in range(micro):
        x = tok[slot, pl.ds(b * toks, toks), :].astype(F32)
        normed[at_rows(slot * micro + b, toks), :] = norm_rows(x, gain)[2].astype(BF16)


def first_attend(sizes, acc, att, slot, b):
    micro, toks, width, hd, tangents = sizes
    factor = HEAD ** (-0.5)
    part = 2 * HEAD
    streams = 1 + tangents
    even = lax.broadcasted_iota(jnp.int32, (toks, part), 1) < HEAD
    rows = at_rows(slot * micro + b, toks)
    q = acc[rows, pl.ds(0, part)]
    k = acc[rows, pl.ds(part, part)].astype(BF16)
    v = acc[rows, pl.ds(2 * part, streams * part)].astype(BF16)
    zero = jnp.zeros_like(q)
    both = jnp.concatenate([jnp.where(even, q, zero), jnp.where(even, zero, q)], 0).astype(BF16)
    low = softmax(dot_t(both, k) * factor).astype(BF16)
    out = dot(low, v)
    for s in range(streams):
        joined = jnp.where(even, out[:toks, s * part : (s + 1) * part], out[toks:, s * part : (s + 1) * part])
        att[slot, pl.ds((s * micro + b) * toks, toks), :] = joined.astype(BF16)


def first_out(sizes, tok, place, b_full, att, state):
    micro, toks, width, hd, tangents = sizes
    rows0 = micro * toks
    tile = 256
    for c in range(width // tile):
        at = pl.ds(c * tile, tile)
        out = dot_t(att[...], b_full[0, at, :])
        extra = [dot_t(att[pl.ds(0, rows0), :], b_full[1 + j, at, :]) for j in range(tangents)]
        x = tok[place, :, at].astype(F32)
        state[pl.ds(0, rows0), at] = (x + out[:rows0]).astype(BF16)
        for j in range(tangents):
            state[pl.ds((1 + j) * rows0, rows0), at] = (
                out[(1 + j) * rows0 : (2 + j) * rows0] + extra[j]
            ).astype(BF16)


def group_of(sizes):
    micro, toks, width, hd, tangents = sizes
    return -(-micro * (1 + tangents) // 8) * 8


def stream_of(sizes, shape):
    return (lax.broadcasted_iota(jnp.int32, shape, 0) % group_of(sizes)) // sizes[0]


def lowered(sizes, parts):
    micro, tangents = sizes[0], sizes[4]
    stream = stream_of(sizes, parts[0].shape)
    total = parts[0]
    for j in range(tangents):
        moved = pltpu.roll(parts[1 + j], micro * (1 + j), 0)
        total = total + jnp.where(stream == 1 + j, moved, jnp.zeros_like(moved))
    return total


def primal_rows(sizes, x):
    micro, tangents = sizes[0], sizes[4]
    stream = stream_of(sizes, x.shape)
    spread = x
    for j in range(tangents):
        spread = jnp.where(stream == 1 + j, pltpu.roll(x, micro * (1 + j), 0), spread)
    return spread


def norm_group(sizes, x, gains):
    stream = stream_of(sizes, x.shape)
    centred, inverse, y = norm_rows(primal_rows(sizes, x), gains)
    dy = norm_tangent(x, centred, inverse, gains)
    return jnp.where(stream == 0, y, dy).astype(BF16)


def class_rows(sizes, state):
    micro, toks, width, hd, tangents = sizes
    streams = 1 + tangents
    rows = [
        state[pl.ds((s * micro + b) * toks, 16), :].astype(F32)[:1] for s in range(streams) for b in range(micro)
    ]
    return jnp.concatenate(rows + [jnp.zeros((group_of(sizes) - micro * streams, width), F32)], 0)


def last_norm(sizes, gain, state, normed):
    micro, toks, width, hd, tangents = sizes
    rows0 = micro * toks
    for b in range(micro):
        at = pl.ds(b * toks, toks)
        centred, inverse, y = norm_rows(state[at, :].astype(F32), gain)
        normed[0, at, :] = y.astype(BF16)
        for j in range(tangents):
            t = state[pl.ds((1 + j) * rows0 + b * toks, toks), :].astype(F32)
            normed[1 + j, at, :] = norm_tangent(t, centred, inverse, gain).astype(BF16)


def last_attend(sizes, u, normed):
    micro, toks, width, hd, tangents = sizes
    factor = HEAD ** (-0.5)
    shape = (u.shape[0], micro * toks)
    stream = stream_of(sizes, shape)
    image = (lax.broadcasted_iota(jnp.int32, shape, 0) % group_of(sizes)) % micro
    valid = lax.broadcasted_iota(jnp.int32, shape, 1) // toks == image
    parts = [dot_t(u, normed[s]) * factor for s in range(1 + tangents)]
    probs = softmax(jnp.where(valid, parts[0], -jnp.inf))
    weights = primal_rows(sizes, probs)
    scores = lowered(sizes, parts)
    dprobs = weights * (scores - jnp.sum(weights * scores, -1, keepdims=True))
    zero = jnp.zeros_like(weights)
    total = dot(jnp.where(stream == 0, weights, dprobs).astype(BF16), normed[0])
    for j in range(tangents):
        total = total + dot(jnp.where(stream == 1 + j, weights, zero).astype(BF16), normed[1 + j])
    return total.astype(BF16)


TOK, LA, LB, ATT, CLS, U, M, O1, O0, GAIN, STAGES = range(11)


def kernel(
    n, sizes, tokens, w_qkv, tangent_value, w_out, t_out, gain_in, final_in, head_in, mean_ref, var_ref,
    a_stage, b_stage, a0, a1, b1, b_full, tok, normed_all, acc, att_out, att_in, state, normed,
    gains, final_gain, head, cls_out, cls_all, u_out, u_all, m_out, m_all, o_out, o_all, classes,
    loads, a_out, a_send, a_recv, stage_send, stage_recv, far_send, far_recv, b_send, b_recv,
):
    micro, toks, width, hd, tangents = sizes
    streams = 1 + tangents
    part = hd // 4
    share = part // HEAD
    g = Place(n)
    me, section, place, z, nz = g.me, g.section, g.place, g.z, g.nz
    other = 1 - section
    rows = width // n
    slab = 4 * rows
    group = group_of(sizes)
    own = at_rows(me, rows)

    barrier = pltpu.get_barrier_semaphore()

    def greet(target, sec):
        pl.semaphore_signal(
            barrier, inc=1, device_id={"section": sec, "dp": target}, device_id_type=MESH
        )

    for k in range(1, nz):
        greet(((z + k) % nz) * 4 + place, section)
    for near in (g.diagonal, g.x_near, g.y_near):
        greet(near, section)
        greet(near, other)
    greet(me, other)

    def column(p):
        return pl.ds(p * part, part) if isinstance(p, int) else at_rows(p, part)

    def load(i, src, dst):
        return pltpu.make_async_copy(src, dst, loads.at[i])

    def stage_loads():
        moves = []
        for p in range(4):
            for m in range(3):
                moves.append((w_qkv.at[:, pl.ds(m * hd + p * part, part)], a_stage.at[p, :, pl.ds(m * part, part)]))
            for j in range(tangents):
                moves.append(
                    (
                        tangent_value.at[j, :, pl.ds(p * part, part)],
                        a_stage.at[p, :, pl.ds((3 + j) * part, part)],
                    )
                )
        return [load(8 + i, *move) for i, move in enumerate(moves)]

    def own_loads():
        moves = []
        for m in range(3):
            moves.append((w_qkv.at[:, column(m * 4 + place)], a1.at[own, pl.ds(m * part, part)]))
        for j in range(tangents):
            moves.append((tangent_value.at[j, :, column(place)], a1.at[own, pl.ds((3 + j) * part, part)]))
        moves.append((w_out.at[:, column(place)], b1.at[0, own, :]))
        moves.append((t_out.at[:, :, column(place)], b1.at[pl.ds(1, tangents), own, :]))
        for p in range(4):
            moves.append((w_out.at[:, pl.ds(p * part, part)], b_stage.at[p, 0]))
            moves.append((t_out.at[:, :, pl.ds(p * part, part)], b_stage.at[p, pl.ds(1, tangents)]))
        return [load(8 + 4 * (3 + tangents) + i, *move) for i, move in enumerate(moves)]

    def b_loads():
        return [
            load(4, w_out, b_full.at[0, own, :]),
            load(5, t_out, b_full.at[pl.ds(1, tangents), own, :]),
        ]

    def start_all(moves):
        for move in moves:
            move.start()

    def wait_all(moves):
        for move in moves:
            move.wait()

    def gain_load():
        return load(0, gain_in, gains.at[section])

    def tok_load():
        return load(1, tokens, tok.at[place])

    def tail_loads():
        return [load(2, head_in, head), load(3, final_in, final_gain)]

    start_all(stage_loads() + [gain_load(), tok_load()])
    pl.when(section == 0)(lambda: start_all(b_loads()))
    pl.when(section == 1)(lambda: start_all(own_loads()))
    start_all(tail_loads())
    pl.semaphore_wait(barrier, 7 + nz - 1)

    def xfer(stage, i, src, dst, source, target, sec):
        return pltpu.make_async_remote_copy(
            src_ref=src,
            dst_ref=dst,
            send_sem=stage_send.at[stage, i],
            recv_sem=stage_recv.at[stage, source],
            device_id={"section": sec, "dp": target},
            device_id_type=MESH,
        )

    def arrived(stage, source, dst):
        xfer(stage, 0, dst, dst, source, me, other).wait_recv()

    FAR = (3, 1, 2, 0)

    def scatter(stage, src, dst, sec, skip_own=False):
        sends = []
        for i in FAR:
            if i == 0 and skip_own:
                continue
            target = g.plane[i]
            move = xfer(stage, i, src(target % 4), dst, place, target, sec)
            move.start()
            sends.append(move)
        return sends

    def drain(sends):
        for move in sends:
            move.wait_send()

    def a_ref(src):
        return a0.at[at_rows(src, rows), :]

    def a_copy(src_ref, src, sem, target, sec):
        return pltpu.make_async_remote_copy(
            src_ref=src_ref,
            dst_ref=a_ref(src),
            send_sem=sem,
            recv_sem=a_recv.at[src],
            device_id={"section": sec, "dp": target},
            device_id_type=MESH,
        )

    @pl.when(section == 0)
    def _():
        sends = []
        wait_all(stage_loads())
        for i in (0, 3, 1, 2):
            target = g.plane[i]
            move = a_copy(a_stage.at[target % 4], me, a_out.at[i], target, other)
            move.start()
            sends.append(move)
        gain_load().wait()
        move = xfer(GAIN, 0, gains.at[section], gains.at[section], 0, me, other)
        move.start()
        sends.append(move)
        wait_all(b_loads())
        gather = Gather(n, g, b_full, b_send, b_recv)
        lag = 2
        for d in range(nz + lag):
            if d < nz:
                gather.direct(d)
            if d >= lag:
                gather.relay(d - lag)
        tok_load().wait()
        gather.rest()
        for p in range(4):
            arrived(ATT, p, att_in.at[:, pl.ds(p * part, part)])
        first_out(sizes, tok, place, b_full, att_in, state)
        cls_out[...] = class_rows(sizes, state)
        sends += scatter(CLS, lambda p: cls_out, cls_all.at[place], other)
        arrived(GAIN, 0, gains.at[other])
        last_norm(sizes, gains[1], state, normed)
        for p in range(4):
            arrived(U, p, u_all.at[p])
        u = jnp.concatenate([u_all[p] for p in range(4)], 0)
        m = last_attend(sizes, u, normed)
        for p in range(4):
            m_out[p] = m[p * share * group : (p + 1) * share * group]
        sends += scatter(M, lambda p: m_out.at[p], m_all.at[place], other)
        classes[...] = cls_out[...]
        for p in range(4):
            arrived(O0, p, o_all.at[p])
        drain(sends)
        gather.drain()

    @pl.when(section == 1)
    def _():
        sends = []
        gain_load().wait()
        move = xfer(GAIN, 0, gains.at[section], gains.at[section], 0, me, other)
        move.start()
        sends.append(move)
        tok_load().wait()
        sends += scatter(TOK, lambda p: tok.at[place], tok.at[place], section, True)

        a_sends = []

        def relay(d):
            for shift, cond in g.sources(d):

                def step(shift=shift, d=d):
                    for near in g.plane:
                        src = near + 4 * shift
                        a_copy(a_ref(src), src, a_send.at[src, 0], me, section).wait_recv()
                        if shift <= 0 and d < nz - 1:
                            pl.when(g.up)(
                                lambda: a_copy(a_ref(src), src, a_send.at[src, 0], me + 4, section).start()
                            )
                        if shift >= 0 and d < nz - 1:
                            pl.when(g.down)(
                                lambda: a_copy(a_ref(src), src, a_send.at[src, 1], me - 4, section).start()
                            )

                step() if cond is None else pl.when(cond)(step)

        def relay_end(d):
            for shift, cond in g.sources(d):

                def step(shift=shift):
                    for near in g.plane:
                        src = near + 4 * shift
                        if shift <= 0:
                            pl.when(g.up)(
                                lambda: a_copy(a_ref(src), src, a_send.at[src, 0], me + 4, section).wait_send()
                            )
                        if shift >= 0:
                            pl.when(g.down)(
                                lambda: a_copy(a_ref(src), src, a_send.at[src, 1], me - 4, section).wait_send()
                            )

                step() if cond is None else pl.when(cond)(step)

        def project(d):
            for shift, cond in g.sources(d):

                def step(shift=shift):
                    at = at_rows(z + shift, slab)
                    term = dot(normed_all[:, at], a0[at, :])
                    acc[...] = term if d == 0 else acc[...] + term

                step() if cond is None else pl.when(cond)(step)

        relay(0)
        wait_all(stage_loads())
        wait_all(own_loads())
        sends += scatter(LA, lambda p: a_stage.at[p], a1.at[own, :], section, True)
        sends += scatter(LB, lambda p: b_stage.at[p], b1.at[:, own, :], section, True)
        arrived(GAIN, 0, gains.at[other])
        first_norm(sizes, tok, gains[0], normed_all, place)
        relay(1)
        for near in g.plane[1:]:
            arrived(TOK, near % 4, tok.at[near % 4])
            first_norm(sizes, tok, gains[0], normed_all, near % 4)
        for d in range(2, nz):
            relay(d)
            project(d - 2)
        for d in range(max(nz - 2, 0), nz):
            project(d)

        def far(kind, zc):
            at = at_rows(zc, slab)
            if kind == 0:
                return a1.at[at, pl.ds(0, 2 * part)]
            if kind == 1:
                return a1.at[at, pl.ds(2 * part, streams * part)]
            return b1.at[:, at, :]

        def far_copy(kind, zc, slot, target):
            return pltpu.make_async_remote_copy(
                src_ref=far(kind, zc),
                dst_ref=far(kind, zc),
                send_sem=far_send.at[kind, slot],
                recv_sem=far_recv.at[kind, zc],
                device_id={"section": section, "dp": target},
                device_id_type=MESH,
            )

        def far_each(act):
            for k in range(1, nz):
                pl.when(z + k < nz)(functools.partial(act, k, 2 * k))
                pl.when(z >= k)(functools.partial(act, -k, 2 * k + 1))

        def far_start(kind):
            far_each(lambda k, slot: far_copy(kind, z, slot, me + 4 * k).start())

        def far_wait(kind):
            far_each(lambda k, slot: far_copy(kind, z + k, 0, me).wait_recv())

        def far_end(kind):
            far_each(lambda k, slot: far_copy(kind, z, slot, me + 4 * k).wait_send())

        for near in g.plane[1:]:
            arrived(LA, near % 4, a1.at[at_rows(near, rows), :])
            arrived(LB, near % 4, b1.at[:, at_rows(near, rows), :])
        for kind in range(3):
            far_start(kind)

        for turn in (FAR[:2], FAR[2:]):
            for i in turn:
                for b in range(micro):
                    first_attend(sizes, acc, att_out, g.plane[i] % 4, b)
            for i in turn:
                target = g.plane[i]
                move = xfer(ATT, i, att_out.at[target % 4], att_in.at[:, column(place)], place, target, other)
                move.start()
                sends.append(move)

        far_wait(0)
        for p in range(4):
            arrived(CLS, p, cls_all.at[p])
        x = jnp.concatenate([cls_all[p] for p in range(4)], 0)
        q = dot(norm_group(sizes, x, gains[1]), a1[:, pl.ds(0, part)]).astype(BF16).astype(F32)
        owner = lax.broadcasted_iota(jnp.int32, (group, part), 1) // HEAD
        zero = jnp.zeros((group, part), F32)
        spread = [
            jnp.where(owner == h, q[p * group : (p + 1) * group], zero) for p in range(4) for h in range(share)
        ]
        u = dot_t(jnp.concatenate(spread, 0).astype(BF16), a1[:, pl.ds(part, part)]).astype(BF16)
        tall = share * group
        for p in range(4):
            u_out[p] = u[p * tall : (p + 1) * tall]
        sends += scatter(U, lambda p: u_out.at[p], u_all.at[place], other)
        far_wait(1)
        for p in range(4):
            arrived(M, p, m_all.at[p])
        m = jnp.concatenate([m_all[p] for p in range(4)], 0)
        r = dot(m, a1[:, pl.ds(2 * part, streams * part)])
        mixed = lowered(sizes, [r[:, s * part : (s + 1) * part] for s in range(streams)])
        chosen = []
        for p in range(4):
            block = zero
            for h in range(share):
                at = p * tall + h * group
                block = jnp.where(owner == h, mixed[at : at + group], block)
            chosen.append(block)
        attended = jnp.concatenate(chosen, 0).astype(BF16)
        far_wait(2)
        out = lowered(sizes, [dot_t(attended, b1[s]) for s in range(streams)])
        for p in range(4):
            o_out[p] = out[p * group : (p + 1) * group]
        sends += scatter(O1, lambda p: o_out.at[p], o_all.at[place], section, True)
        sends += scatter(O0, lambda p: o_out.at[p], o_all.at[place], other)
        o_all[place] = o_out[place]
        classes[...] = cls_all[place]
        for near in g.plane[1:]:
            arrived(O1, near % 4, o_all.at[near % 4])
        drain(sends)
        for d in range(nz - 1):
            relay_end(d)
        for kind in range(3):
            far_end(kind)

    wait_all(tail_loads())
    total = o_all[0] + o_all[1] + o_all[2] + o_all[3]
    final = (classes[...] + total).astype(BF16).astype(F32)
    features = norm_group(sizes, final, final_gain[...])
    count = head.shape[0]
    cut = count // 16 * 16
    for at in [pl.ds(0, cut)] + [pl.ds(cut, count - cut)] * (cut < count):
        logits = dot_t(features, head[at, :])
        mean_ref[:, 0, at] = logits[:micro]
        var_ref[:, 0, at] = sum(
            logits[(1 + j) * micro : (2 + j) * micro] * logits[(1 + j) * micro : (2 + j) * micro]
            for j in range(tangents)
        )


def two_sections(n):
    def shards(tokens, w_qkv, w_output, tangent_value, tangent_output, layer_gain, final_gain, head):
        micro, _, toks, width = tokens.shape
        tangents = tangent_value.shape[1]
        hd = w_output.shape[1]
        count = head.shape[1]
        rows = width // n
        part = hd // 4
        nz = n // 4
        sizes = (micro, toks, width, hd, tangents)
        streams = 1 + tangents
        rows0 = micro * toks
        group = group_of(sizes)
        tall = part // HEAD * group
        vmem = pl.BlockSpec(memory_space=pltpu.VMEM)
        anywhere = pl.BlockSpec(memory_space=pl.ANY)
        dma = pltpu.SemaphoreType.DMA
        mean, var = pl.pallas_call(
            functools.partial(kernel, n, sizes),
            out_shape=[jax.ShapeDtypeStruct((micro, 1, count), F32)] * 2,
            in_specs=[anywhere] * 8,
            out_specs=[vmem, vmem],
            scratch_shapes=[
                pltpu.VMEM((4, rows, (2 + streams) * part), BF16),
                pltpu.VMEM((4, streams, rows, part), BF16),
                pltpu.VMEM((width, (2 + streams) * part), BF16),
                pltpu.VMEM((width, (2 + streams) * part), BF16),
                pltpu.VMEM((streams, width, part), BF16),
                pltpu.VMEM((streams, width, hd), BF16),
                pltpu.VMEM((4, rows0, width), BF16),
                pltpu.VMEM((4 * rows0, width), BF16),
                pltpu.VMEM((4 * rows0, (2 + streams) * part), F32),
                pltpu.VMEM((4, streams * rows0, part), BF16),
                pltpu.VMEM((streams * rows0, hd), BF16),
                pltpu.VMEM((streams * rows0, width), BF16),
                pltpu.VMEM((streams, rows0, width), BF16),
                pltpu.VMEM((2, 1, width), F32),
                pltpu.VMEM((1, width), F32),
                pltpu.VMEM((count, width), BF16),
                pltpu.VMEM((group, width), F32),
                pltpu.VMEM((4, group, width), F32),
                pltpu.VMEM((4, tall, width), BF16),
                pltpu.VMEM((4, tall, width), BF16),
                pltpu.VMEM((4, tall, width), BF16),
                pltpu.VMEM((4, tall, width), BF16),
                pltpu.VMEM((4, group, width), F32),
                pltpu.VMEM((4, group, width), F32),
                pltpu.VMEM((group, width), F32),
                dma((64,)),
                dma((4,)),
                dma((n, 2)),
                dma((n,)),
                dma((STAGES, 4)),
                dma((STAGES, 4)),
                dma((3, 2 * nz)),
                dma((3, nz)),
                dma((send_slots(n),)),
                dma((n, 2)),
            ],
            compiler_params=pltpu.CompilerParams(
                collective_id=0, has_side_effects=True, vmem_limit_bytes=60 * 2**20
            ),
        )(
            tokens.reshape(rows0, width),
            w_qkv[0],
            tangent_value[0],
            jnp.swapaxes(w_output[0], 0, 1),
            jnp.swapaxes(tangent_output[0], 1, 2),
            layer_gain,
            final_gain[None],
            head.T,
        )
        return mean, var

    return shards


def solution(mesh):
    n = mesh.shape["dp"]
    fast = mesh.shape["section"] == 2 and n % 4 == 0
    return jax.shard_map(
        two_sections(n) if fast else relay_shards,
        mesh=mesh,
        in_specs=(
            P(None, "dp", None, None),
            P("section", "dp", None),
            P("section", None, "dp"),
            P("section", None, "dp", None),
            P("section", None, None, "dp"),
            P("section", None),
            P(),
            P(None, "section"),
        ),
        out_specs=(P(None, "dp", "section"), P(None, "dp", "section")),
        check_vma=False,
    )
```

```python
import functools

import jax
import jax.numpy as jnp
from jax import lax
from jax.experimental import pallas as pl
from jax.experimental.pallas import tpu as pltpu
from jax.sharding import PartitionSpec as P

HEAD = 64
epsilon = 1e-06
F32, BF16 = jnp.float32, jnp.bfloat16
MESH = pl.DeviceIdType.MESH


def contract(spec, left, right):
    return jnp.einsum(spec, left, right, preferred_element_type=jnp.float32)


def norm_jvp(primal, tangents, gains):
    average = jnp.mean(primal, -1, keepdims=True)
    centred = primal - average
    inverse = lax.rsqrt(jnp.mean(centred * centred, -1, keepdims=True) + epsilon)
    dcentred = tangents - jnp.mean(tangents, -1, keepdims=True)
    dinverse = -(inverse**3) * jnp.mean(centred * dcentred, -1, keepdims=True)
    return (centred * inverse * gains, (dcentred * inverse + centred * dinverse) * gains)


def layer_step(state, qkv_weight, out_weight, value_tangent, out_tangent, gains):
    hd = out_weight.shape[0]
    heads = hd // HEAD
    resid = state.astype(F32)
    normed_zero, normed_rest = norm_jvp(resid[0], resid[1:], gains)
    normed = jnp.concatenate([normed_zero[None], normed_rest]).astype(BF16)
    streams, batch, tokens_here, width = normed.shape
    projected = contract("sbtd,de->sbte", normed, qkv_weight)
    extra_value = contract("btd,kde->kbte", normed[0], value_tangent)
    queries = projected[..., :hd]
    key_rows = projected[..., hd : 2 * hd]
    values = projected[..., 2 * hd :]
    values = jnp.concatenate([values[:1], values[1:] + extra_value])
    shape_heads = (streams, batch, tokens_here, heads, HEAD)
    queries = queries.astype(BF16).reshape(shape_heads)
    key_rows = key_rows.astype(BF16).reshape(shape_heads)
    values = values.astype(BF16).reshape(shape_heads)
    factor = HEAD ** (-0.5)
    scores = contract("bqhe,bkhe->bhqk", queries[0], key_rows[0]) * factor
    probs = jax.nn.softmax(scores, -1)
    dscores = (
        contract("sbqhe,bkhe->sbhqk", queries[1:], key_rows[0])
        + contract("bqhe,sbkhe->sbhqk", queries[0], key_rows[1:])
    ) * factor
    dprobs = probs * (dscores - jnp.sum(probs * dscores, -1, keepdims=True))
    probs_low = probs.astype(BF16)
    dprobs_low = dprobs.astype(BF16)
    attended_zero = contract("bhqk,bkhe->bqhe", probs_low, values[0])
    attended_rest = contract("sbhqk,bkhe->sbqhe", dprobs_low, values[0]) + contract(
        "bhqk,sbkhe->sbqhe", probs_low, values[1:]
    )
    attended = jnp.concatenate([attended_zero[None], attended_rest]).astype(BF16)
    attended = attended.reshape(streams, batch, tokens_here, hd)
    output = contract("sbte,ed->sbtd", attended, out_weight)
    extra_out = contract("bte,ked->kbtd", attended[0], out_tangent)
    output = jnp.concatenate([output[:1], output[1:] + extra_out])
    return (resid + output).astype(BF16)


def relay_shards(tokens, w_qkv, w_output, tangent_value, tangent_output, layer_gain, final_gain, head):
    full_qkv, full_output, full_value_tan, full_output_tan = (
        lax.all_gather(w_qkv, "dp", axis=1, tiled=True),
        lax.all_gather(w_output, "dp", axis=2, tiled=True),
        lax.all_gather(tangent_value, "dp", axis=2, tiled=True),
        lax.all_gather(tangent_output, "dp", axis=3, tiled=True),
    )
    tangents = tangent_value.shape[1]

    def advance_layer(state):
        return layer_step(
            state, full_qkv[0], full_output[0], full_value_tan[0], full_output_tan[0], layer_gain[0]
        )

    section_index = lax.axis_index("section")
    section_count = lax.axis_size("section")
    route = [(i, i + 1) for i in range(section_count - 1)]
    micro, _, toks, width = tokens.shape
    entering = jnp.concatenate(
        [tokens.reshape(1, micro, toks, width), jnp.zeros((tangents, micro, toks, width), BF16)]
    )

    def advance(step, outgoing):
        incoming = lax.ppermute(outgoing, "section", route)
        source = jnp.where(step == 0, entering, incoming)
        return lax.cond(section_index == step, advance_layer, jnp.zeros_like, source)

    finished = lax.fori_loop(0, section_count, advance, jnp.zeros_like(entering))
    collected = finished[:, :, 0, :]
    mine = section_index == section_count - 1
    features = lax.psum(jnp.where(mine, collected, jnp.zeros_like(collected)), "section")
    widened = features.astype(F32)
    final_zero, final_rest = norm_jvp(widened[0], widened[1:], final_gain)
    normed_final = jnp.concatenate([final_zero[None], final_rest]).astype(BF16)
    logits = contract("sbd,dc->sbc", normed_final, head)
    return (logits[0][:, None, :], jnp.sum(logits[1:] * logits[1:], 0)[:, None, :])


def dot(a, b):
    return lax.dot_general(a, b, (((1,), (0,)), ((), ())), preferred_element_type=F32)


def dot_t(a, b):
    return lax.dot_general(a, b, (((1,), (1,)), ((), ())), preferred_element_type=F32)


class Gather:
    def __init__(self, n, g, full, send, recv):
        self.nz = n // 4
        self.full, self.send, self.recv = full, send, recv
        self.rows = full.shape[1] // n
        self.g = g
        self.ends = []

    def span(self, start, count):
        return self.full.at[:, pl.ds(pl.multiple_of(start, self.rows // 2), count), :]

    def remote(self, ref, target, sem, recv):
        return pltpu.make_async_remote_copy(
            src_ref=ref,
            dst_ref=ref,
            send_sem=self.send.at[sem],
            recv_sem=recv,
            device_id={"section": self.g.section, "dp": target},
            device_id_type=MESH,
        )

    def copy(self, src, half, target, sem):
        depth = self.rows // 2
        ref = self.span(src * self.rows + half * depth, depth)
        return self.remote(ref, target, sem, self.recv.at[src, half])

    def forward(self, cond, src, half, target, sem):
        def go():
            self.copy(src, half, target, sem).start()

        go() if cond is None else pl.when(cond)(go)

    def ended(self, cond, pieces, sem):
        def end():
            self.remote(self.span(0, pieces * self.rows), self.g.me, sem, self.recv.at[0, 0]).wait_send()

        self.ends.append((cond, end))

    def arrived(self, src, half):
        self.copy(src, half, self.g.me, 0).wait_recv()

    def direct(self, d):
        g = self.g
        for side, (shift, cond) in enumerate(g.sources(d)):
            src = g.me + 4 * shift
            for half in range(2):
                if d > 0:
                    pl.when(cond)(functools.partial(self.arrived, src, half))
                if shift <= 0 and d < self.nz - 1:
                    self.forward(g.up if cond is None else cond & g.up, src, half, g.me + 4, 4 * d)
                if shift >= 0 and d < self.nz - 1:
                    self.forward(g.down if cond is None else cond & g.down, src, half, g.me - 4, 4 * d + 1)
                for target in ((g.y_near, g.x_near), (g.x_near, g.y_near))[half]:
                    self.forward(cond, src, half, target, 4 * d + 2 + side)
            if shift <= 0 and d < self.nz - 1:
                self.ended(g.up if cond is None else cond & g.up, 1, 4 * d)
            if shift >= 0 and d < self.nz - 1:
                self.ended(g.down if cond is None else cond & g.down, 1, 4 * d + 1)
            self.ended(cond, 3, 4 * d + 2 + side)

    def relay(self, d):
        g = self.g
        for side, (shift, cond) in enumerate(g.sources(d)):
            for half, near, target in ((0, g.x_near, g.y_near), (1, g.y_near, g.x_near)):
                src = near + 4 * shift
                wait = functools.partial(self.arrived, src, half)
                wait() if cond is None else pl.when(cond)(wait)
                self.forward(cond, src, half, target, 4 * d + 2 + side)

    def rest(self):
        g = self.g
        for z in range(self.nz):
            up = 4 * (z - g.z)
            self.arrived(g.x_near + up, 1)
            self.arrived(g.y_near + up, 0)
            self.arrived(g.diagonal + up, 0)
            self.arrived(g.diagonal + up, 1)

    def drain(self):
        for cond, end in self.ends:
            end() if cond is None else pl.when(cond)(end)


class Place:
    def __init__(self, n):
        self.nz = n // 4
        self.me = lax.axis_index("dp")
        self.section = lax.axis_index("section")
        me = self.me
        self.x_near = me + 1 - 2 * (me % 2)
        self.y_near = me + 2 - 4 * ((me // 2) % 2)
        self.diagonal = self.x_near + self.y_near - me
        self.z = me // 4
        self.place = me % 4
        self.up, self.down = self.z + 1 < self.nz, self.z >= 1
        self.plane = (me, self.x_near, self.y_near, self.diagonal)

    def sources(self, d):
        if d == 0:
            return [(0, None)]
        return [(-d, self.z >= d), (d, self.z + d < self.nz)]


def norm_rows(x, gains):
    average = jnp.mean(x, -1, keepdims=True)
    centred = x - average
    inverse = lax.rsqrt(jnp.mean(centred * centred, -1, keepdims=True) + epsilon)
    return centred, inverse, centred * inverse * gains


def norm_tangent(t, centred, inverse, gains):
    dcentred = t - jnp.mean(t, -1, keepdims=True)
    dinverse = -(inverse * inverse * inverse) * jnp.mean(centred * dcentred, -1, keepdims=True)
    return (dcentred * inverse + centred * dinverse) * gains


def softmax(scores):
    e = jnp.exp(scores - jnp.max(scores, -1, keepdims=True))
    return e / jnp.sum(e, -1, keepdims=True)


def at_rows(i, count):
    return pl.ds(pl.multiple_of(i * count, count), count)


def first_norm(sizes, tok, gain, normed, slot):
    micro, toks, width, hd, tangents = sizes
    for b in range(micro):
        x = tok[slot, pl.ds(b * toks, toks), :].astype(F32)
        normed[at_rows(slot * micro + b, toks), :] = norm_rows(x, gain)[2].astype(BF16)


def first_attend(sizes, acc, att, slot, b):
    micro, toks, width, hd, tangents = sizes
    factor = HEAD ** (-0.5)
    part = 2 * HEAD
    streams = 1 + tangents
    even = lax.broadcasted_iota(jnp.int32, (toks, part), 1) < HEAD
    rows = at_rows(slot * micro + b, toks)
    q = acc[rows, pl.ds(0, part)]
    k = acc[rows, pl.ds(part, part)].astype(BF16)
    v = acc[rows, pl.ds(2 * part, streams * part)].astype(BF16)
    zero = jnp.zeros_like(q)
    both = jnp.concatenate([jnp.where(even, q, zero), jnp.where(even, zero, q)], 0).astype(BF16)
    low = softmax(dot_t(both, k) * factor).astype(BF16)
    out = dot(low, v)
    for s in range(streams):
        joined = jnp.where(even, out[:toks, s * part : (s + 1) * part], out[toks:, s * part : (s + 1) * part])
        att[slot, pl.ds((s * micro + b) * toks, toks), :] = joined.astype(BF16)


def first_out(sizes, tok, place, b_full, att, state):
    micro, toks, width, hd, tangents = sizes
    rows0 = micro * toks
    tile = 256
    for c in range(width // tile):
        at = pl.ds(c * tile, tile)
        out = dot_t(att[...], b_full[0, at, :])
        extra = [dot_t(att[pl.ds(0, rows0), :], b_full[1 + j, at, :]) for j in range(tangents)]
        x = tok[place, :, at].astype(F32)
        state[pl.ds(0, rows0), at] = (x + out[:rows0]).astype(BF16)
        for j in range(tangents):
            state[pl.ds((1 + j) * rows0, rows0), at] = (
                out[(1 + j) * rows0 : (2 + j) * rows0] + extra[j]
            ).astype(BF16)


def group_of(sizes):
    micro, toks, width, hd, tangents = sizes
    return -(-micro * (1 + tangents) // 8) * 8


def stream_of(sizes, shape):
    return (lax.broadcasted_iota(jnp.int32, shape, 0) % group_of(sizes)) // sizes[0]


def lowered(sizes, parts):
    micro, tangents = sizes[0], sizes[4]
    stream = stream_of(sizes, parts[0].shape)
    total = parts[0]
    for j in range(tangents):
        moved = pltpu.roll(parts[1 + j], micro * (1 + j), 0)
        total = total + jnp.where(stream == 1 + j, moved, jnp.zeros_like(moved))
    return total


def primal_rows(sizes, x):
    micro, tangents = sizes[0], sizes[4]
    stream = stream_of(sizes, x.shape)
    spread = x
    for j in range(tangents):
        spread = jnp.where(stream == 1 + j, pltpu.roll(x, micro * (1 + j), 0), spread)
    return spread


def norm_group(sizes, x, gains):
    stream = stream_of(sizes, x.shape)
    centred, inverse, y = norm_rows(primal_rows(sizes, x), gains)
    dy = norm_tangent(x, centred, inverse, gains)
    return jnp.where(stream == 0, y, dy).astype(BF16)


def class_rows(sizes, state):
    micro, toks, width, hd, tangents = sizes
    streams = 1 + tangents
    rows = [
        state[pl.ds((s * micro + b) * toks, 16), :].astype(F32)[:1] for s in range(streams) for b in range(micro)
    ]
    return jnp.concatenate(rows + [jnp.zeros((group_of(sizes) - micro * streams, width), F32)], 0)


def last_norm(sizes, gain, state, normed):
    micro, toks, width, hd, tangents = sizes
    rows0 = micro * toks
    for b in range(micro):
        at = pl.ds(b * toks, toks)
        centred, inverse, y = norm_rows(state[at, :].astype(F32), gain)
        normed[0, at, :] = y.astype(BF16)
        for j in range(tangents):
            t = state[pl.ds((1 + j) * rows0 + b * toks, toks), :].astype(F32)
            normed[1 + j, at, :] = norm_tangent(t, centred, inverse, gain).astype(BF16)


def last_attend(sizes, u, normed):
    micro, toks, width, hd, tangents = sizes
    factor = HEAD ** (-0.5)
    shape = (u.shape[0], micro * toks)
    stream = stream_of(sizes, shape)
    image = (lax.broadcasted_iota(jnp.int32, shape, 0) % group_of(sizes)) % micro
    valid = lax.broadcasted_iota(jnp.int32, shape, 1) // toks == image
    parts = [dot_t(u, normed[s]) * factor for s in range(1 + tangents)]
    probs = softmax(jnp.where(valid, parts[0], -jnp.inf))
    weights = primal_rows(sizes, probs)
    scores = lowered(sizes, parts)
    dprobs = weights * (scores - jnp.sum(weights * scores, -1, keepdims=True))
    zero = jnp.zeros_like(weights)
    total = dot(jnp.where(stream == 0, weights, dprobs).astype(BF16), normed[0])
    for j in range(tangents):
        total = total + dot(jnp.where(stream == 1 + j, weights, zero).astype(BF16), normed[1 + j])
    return total.astype(BF16)


TOK, LA, LB, ATT, ATC, CLS, U, M, O1, O0, GAIN, FIRST, STAGES = range(13)


def kernel(
    n, sizes, tokens, w_qkv, tangent_value, w_out, t_out, gain_in, final_in, head_in, logit_ref,
    a_stage, b_stage, a0, a1, b1, b_full, tok, normed_all, acc, att_out, att_in, state, normed,
    gains, final_gain, head, atc_out, atc_all, atc_in, cls_out, cls_in, cls_all, u_out, u_all, m_out, m_all, o_out, o_all, classes,
    loads, a_send, a_recv, stage_send, stage_recv, far_send, far_recv, b_send, b_recv,
):
    micro, toks, width, hd, tangents = sizes
    streams = 1 + tangents
    part = hd // 4
    share = part // HEAD
    g = Place(n)
    me, section, place, z, nz = g.me, g.section, g.place, g.z, g.nz
    other = 1 - section
    rows = width // n
    slab = 4 * rows
    group = group_of(sizes)
    own = at_rows(me, rows)

    barrier = pltpu.get_barrier_semaphore()

    def greet(target, sec):
        pl.semaphore_signal(
            barrier, inc=1, device_id={"section": sec, "dp": target}, device_id_type=MESH
        )

    for k in range(1, nz):
        greet(((z + k) % nz) * 4 + place, section)
    for near in (g.diagonal, g.x_near, g.y_near):
        greet(near, section)
        greet(near, other)
    greet(me, other)

    def column(p):
        return pl.ds(p * part, part) if isinstance(p, int) else at_rows(p, part)

    def load(i, src, dst):
        return pltpu.make_async_copy(src, dst, loads.at[i])

    def stage_loads():
        for p in range(4):
            for m in range(3):
                load(5, w_qkv.at[:, pl.ds(m * hd + p * part, part)], a_stage.at[p, :, pl.ds(m * part, part)]).start()
            for j in range(tangents):
                load(
                    5,
                    tangent_value.at[j, :, pl.ds(p * part, part)],
                    a_stage.at[p, :, pl.ds((3 + j) * part, part)],
                ).start()

    def own_loads():
        for m in range(3):
            load(6, w_qkv.at[:, column(m * 4 + place)], a1.at[own, pl.ds(m * part, part)]).start()
        for j in range(tangents):
            load(6, tangent_value.at[j, :, column(place)], a1.at[own, pl.ds((3 + j) * part, part)]).start()
        load(7, w_out.at[:, column(place)], b1.at[0, own, :]).start()
        load(7, t_out.at[:, :, column(place)], b1.at[pl.ds(1, tangents), own, :]).start()
        for p in range(4):
            load(8, w_out.at[:, pl.ds(p * part, part)], b_stage.at[p, 0]).start()
            load(8, t_out.at[:, :, pl.ds(p * part, part)], b_stage.at[p, pl.ds(1, tangents)]).start()

    def b_loads():
        load(4, w_out, b_full.at[0, own, :]).start()
        load(4, t_out, b_full.at[pl.ds(1, tangents), own, :]).start()

    def loaded(i, ref):
        load(i, ref, ref).wait()

    def gain_load():
        return load(0, gain_in, gains.at[section])

    def tok_load():
        return load(1, tokens, tok.at[place])

    def tail_loads():
        return [load(2, head_in, head), load(3, final_in, final_gain)]

    stage_loads()
    gain_load().start()
    tok_load().start()
    pl.when(section == 0)(b_loads)
    pl.when(section == 1)(own_loads)
    for move in tail_loads():
        move.start()
    pl.semaphore_wait(barrier, 7 + nz - 1)

    def xfer(stage, src, dst, target, sec):
        return pltpu.make_async_remote_copy(
            src_ref=src,
            dst_ref=dst,
            send_sem=stage_send.at[stage],
            recv_sem=stage_recv.at[stage],
            device_id={"section": sec, "dp": target},
            device_id_type=MESH,
        )

    def arrived(stage, ref):
        xfer(stage, ref, ref, me, other).wait_recv()

    sent = []

    FAR = (3, 1, 2, 0)

    def scatter(stage, src, dst, sec, total, skip_own=False):
        for i in FAR:
            if i > 0 or not skip_own:
                target = g.plane[i]
                xfer(stage, src(target % 4), dst, target, sec).start()
        sent.append((stage, total))

    def drain():
        for stage, ref in sent:
            xfer(stage, ref, ref, me, other).wait_send()
        sent.clear()

    def a_ref(src):
        return a0.at[at_rows(src, rows), :]

    def a_copy(src_ref, src, sem, target, sec):
        return pltpu.make_async_remote_copy(
            src_ref=src_ref,
            dst_ref=a_ref(src),
            send_sem=sem,
            recv_sem=a_recv.at[src],
            device_id={"section": sec, "dp": target},
            device_id_type=MESH,
        )

    @pl.when(section == 0)
    def _():
        loaded(5, a_stage)
        for i in range(4):
            target = g.plane[i]
            a_copy(a_stage.at[target % 4], me, stage_send.at[FIRST], target, other).start()
        sent.append((FIRST, a_stage))
        gain_load().wait()
        xfer(GAIN, gains.at[section], gains.at[section], me, other).start()
        sent.append((GAIN, gains.at[section]))
        loaded(4, b_full.at[:, own, :])
        gather = Gather(n, g, b_full, b_send, b_recv)
        lag = 2
        for d in range(nz + lag):
            if d < nz:
                gather.direct(d)
            if d >= lag:
                gather.relay(d - lag)
        tok_load().wait()
        gather.rest()
        arrived(ATC, atc_in)
        arrived(ATT, att_in)
        cls_out[...] = lowered(sizes, [dot_t(atc_in[...], b_full[s]) for s in range(streams)])
        xfer(CLS, cls_out, cls_in, me, other).start()
        sent.append((CLS, cls_out))
        first_out(sizes, tok, place, b_full, att_in, state)
        arrived(GAIN, gains.at[other])
        last_norm(sizes, gains[1], state, normed)
        arrived(U, u_all)
        u = jnp.concatenate([u_all[p] for p in range(4)], 0)
        m = last_attend(sizes, u, normed)
        for p in range(4):
            m_out[p] = m[p * share * group : (p + 1) * share * group]
        scatter(M, lambda p: m_out.at[p], m_all.at[place], other, m_out)
        classes[...] = class_rows(sizes, state)
        arrived(O0, o_all)
        drain()
        gather.drain()

    @pl.when(section == 1)
    def _():
        gain_load().wait()
        xfer(GAIN, gains.at[section], gains.at[section], me, other).start()
        sent.append((GAIN, gains.at[section]))
        tok_load().wait()
        scatter(TOK, lambda p: tok.at[place], tok.at[place], section, tok.at[pl.ds(0, 3)], True)

        def relay(d):
            for shift, cond in g.sources(d):

                def step(shift=shift, d=d):
                    for near in g.plane:
                        src = near + 4 * shift
                        a_copy(a_ref(src), src, a_send.at[d, 0], me, section).wait_recv()
                        if shift <= 0 and d < nz - 1:
                            pl.when(g.up)(
                                lambda: a_copy(a_ref(src), src, a_send.at[d, 0], me + 4, section).start()
                            )
                        if shift >= 0 and d < nz - 1:
                            pl.when(g.down)(
                                lambda: a_copy(a_ref(src), src, a_send.at[d, 1], me - 4, section).start()
                            )

                step() if cond is None else pl.when(cond)(step)

        def relay_end(d):
            slab_ref = a0.at[pl.ds(0, slab), :]
            for shift, cond in g.sources(d):

                def end(way):
                    pltpu.make_async_remote_copy(
                        src_ref=slab_ref,
                        dst_ref=slab_ref,
                        send_sem=a_send.at[d, way],
                        recv_sem=a_recv.at[0],
                        device_id={"section": section, "dp": me},
                        device_id_type=MESH,
                    ).wait_send()

                if shift <= 0:
                    pl.when(g.up if cond is None else cond & g.up)(functools.partial(end, 0))
                if shift >= 0:
                    pl.when(g.down if cond is None else cond & g.down)(functools.partial(end, 1))

        def project(d):
            for shift, cond in g.sources(d):

                def step(shift=shift):
                    at = at_rows(z + shift, slab)
                    term = dot(normed_all[:, at], a0[at, :])
                    acc[...] = term if d == 0 else acc[...] + term

                step() if cond is None else pl.when(cond)(step)

        relay(0)
        loaded(5, a_stage)
        loaded(6, a1.at[own, :])
        loaded(7, b1.at[:, own, :])
        loaded(8, b_stage)
        scatter(LA, lambda p: a_stage.at[p], a1.at[own, :], section, a_stage.at[pl.ds(0, 3)], True)
        scatter(LB, lambda p: b_stage.at[p], b1.at[:, own, :], section, b_stage.at[pl.ds(0, 3)], True)
        arrived(GAIN, gains.at[other])
        first_norm(sizes, tok, gains[0], normed_all, place)
        relay(1)
        arrived(TOK, tok.at[pl.ds(0, 3)])
        for near in g.plane[1:]:
            first_norm(sizes, tok, gains[0], normed_all, near % 4)
        for d in range(2, nz):
            relay(d)
            project(d - 2)
        for d in range(max(nz - 2, 0), nz):
            project(d)

        def far(kind, zc):
            at = at_rows(zc, slab)
            if kind == 0:
                return a1.at[at, pl.ds(0, 2 * part)]
            if kind == 1:
                return a1.at[at, pl.ds(2 * part, streams * part)]
            return b1.at[:, at, :]

        def far_copy(kind, zc, slot, target):
            return pltpu.make_async_remote_copy(
                src_ref=far(kind, zc),
                dst_ref=far(kind, zc),
                send_sem=far_send.at[kind, slot],
                recv_sem=far_recv.at[kind, zc],
                device_id={"section": section, "dp": target},
                device_id_type=MESH,
            )

        ends = (z == 0) | (z == nz - 1)

        def far_sends(kind):
            for k in range(1, nz):
                for way, slot in ((k, 2 * k), (-k, 2 * k + 1)):
                    there = z + way
                    when = (there >= 0) & (there < nz)
                    if k > 1:
                        when = when & (ends | ((there > 0) & (there < nz - 1)))
                    yield when, functools.partial(far_copy, kind, z, slot, me + 4 * way)

        def far_relay(kind):
            for k in range(1, nz - 2):
                yield (z == 1) & (z + k < nz - 1), z + k, functools.partial(far_copy, kind, z + k, 2 * nz + k, me - 4)
                yield (z == nz - 2) & (z - k > 0), z - k, functools.partial(far_copy, kind, z - k, 3 * nz + k, me + 4)

        def far_start(kind):
            for when, move in far_sends(kind):
                pl.when(when)(lambda: move().start())

        def far_pass(kind):
            for when, zc, move in far_relay(kind):

                def step():
                    far_copy(kind, zc, 0, me).wait_recv()
                    move().start()

                pl.when(when)(step)

        def far_wait(kind):
            for k in range(1, nz):
                for way in (k, -k):
                    there = z + way
                    when = (there >= 0) & (there < nz)
                    if 0 < k < nz - 2:
                        passed = ((z == 1) & (there > 1) & (there < nz - 1)) | (
                            (z == nz - 2) & (there > 0) & (there < nz - 2)
                        )
                        when = when & jnp.logical_not(passed)
                    pl.when(when)(lambda: far_copy(kind, there, 0, me).wait_recv())

        def far_end(kind):
            for when, move in far_sends(kind):
                pl.when(when)(lambda: move().wait_send())
            for when, zc, move in far_relay(kind):
                pl.when(when)(lambda: move().wait_send())

        arrived(LA, a1.at[pl.ds(0, 3 * rows), :])
        arrived(LB, b1.at[:, pl.ds(0, 3 * rows), :])
        for kind in range(3):
            far_start(kind)

        for i in FAR:
            for b in range(micro):
                first_attend(sizes, acc, att_out, g.plane[i] % 4, b)
            target = g.plane[i]
            xfer(ATT, att_out.at[target % 4], att_in.at[:, column(place)], target, other).start()
        sent.append((ATT, att_out))
        firsts = []
        for p in range(4):
            for i in range(group):
                at = pl.ds(i * toks, 16) if i < streams * micro else pl.ds(0, 16)
                firsts.append(att_out[p, at, :].astype(F32)[:1])
        atc_out[...] = jnp.concatenate(firsts, 0).astype(BF16)
        scatter(ATC, lambda p: atc_out, atc_in.at[:, column(place)], other, atc_all)
        far_pass(0)
        fresh = []
        blank = jnp.zeros((group - micro, width), F32)
        for p in range(4):
            fresh += [tok[p, pl.ds(b * toks, 16), :].astype(F32)[:1] for b in range(micro)] + [blank]
        fresh = jnp.concatenate(fresh, 0)
        far_wait(0)
        arrived(CLS, cls_in)
        x = (fresh + cls_in[...]).astype(BF16).astype(F32)
        for p in range(4):
            cls_all[p] = x[p * group : (p + 1) * group]
        q = dot(norm_group(sizes, x, gains[1]), a1[:, pl.ds(0, part)]).astype(BF16).astype(F32)
        owner = lax.broadcasted_iota(jnp.int32, (group, part), 1) // HEAD
        zero = jnp.zeros((group, part), F32)
        spread = [
            jnp.where(owner == h, q[p * group : (p + 1) * group], zero) for p in range(4) for h in range(share)
        ]
        u = dot_t(jnp.concatenate(spread, 0).astype(BF16), a1[:, pl.ds(part, part)]).astype(BF16)
        tall = share * group
        for p in range(4):
            u_out[p] = u[p * tall : (p + 1) * tall]
        scatter(U, lambda p: u_out.at[p], u_all.at[place], other, u_out)
        far_pass(1)
        far_pass(2)
        far_wait(1)
        arrived(M, m_all)
        m = jnp.concatenate([m_all[p] for p in range(4)], 0)
        r = dot(m, a1[:, pl.ds(2 * part, streams * part)])
        mixed = lowered(sizes, [r[:, s * part : (s + 1) * part] for s in range(streams)])
        chosen = []
        for p in range(4):
            block = zero
            for h in range(share):
                at = p * tall + h * group
                block = jnp.where(owner == h, mixed[at : at + group], block)
            chosen.append(block)
        attended = jnp.concatenate(chosen, 0).astype(BF16)
        far_wait(2)
        out = lowered(sizes, [dot_t(attended, b1[s]) for s in range(streams)])
        for p in range(4):
            o_out[p] = out[p * group : (p + 1) * group]
        scatter(O1, lambda p: o_out.at[p], o_all.at[place], section, o_out.at[pl.ds(0, 3)], True)
        scatter(O0, lambda p: o_out.at[p], o_all.at[place], other, o_out)
        o_all[place] = o_out[place]
        classes[...] = cls_all[place]
        arrived(O1, o_all.at[pl.ds(0, 3)])
        drain()
        for d in range(nz - 1):
            relay_end(d)
        for kind in range(3):
            far_end(kind)

    for move in tail_loads():
        move.wait()
    total = o_all[0] + o_all[1] + o_all[2] + o_all[3]
    final = (classes[...] + total).astype(BF16).astype(F32)
    features = norm_group(sizes, final, final_gain[...])
    logits = dot_t(features, head[...])
    for s in range(streams):
        logit_ref[s, :, 0, :] = logits[s * micro : (s + 1) * micro]


def two_sections(n):
    def shards(tokens, w_qkv, w_output, tangent_value, tangent_output, layer_gain, final_gain, head):
        micro, _, toks, width = tokens.shape
        tangents = tangent_value.shape[1]
        hd = w_output.shape[1]
        count = head.shape[1]
        rows = width // n
        part = hd // 4
        nz = n // 4
        sizes = (micro, toks, width, hd, tangents)
        streams = 1 + tangents
        rows0 = micro * toks
        group = group_of(sizes)
        tall = part // HEAD * group
        vmem = pl.BlockSpec(memory_space=pltpu.VMEM)
        anywhere = pl.BlockSpec(memory_space=pl.ANY)
        dma = pltpu.SemaphoreType.DMA
        logits = pl.pallas_call(
            functools.partial(kernel, n, sizes),
            out_shape=jax.ShapeDtypeStruct((streams, micro, 1, count), F32),
            in_specs=[anywhere] * 8,
            out_specs=vmem,
            scratch_shapes=[
                pltpu.VMEM((4, rows, (2 + streams) * part), BF16),
                pltpu.VMEM((4, streams, rows, part), BF16),
                pltpu.VMEM((width, (2 + streams) * part), BF16),
                pltpu.VMEM((width, (2 + streams) * part), BF16),
                pltpu.VMEM((streams, width, part), BF16),
                pltpu.VMEM((streams, width, hd), BF16),
                pltpu.VMEM((4, rows0, width), BF16),
                pltpu.VMEM((4 * rows0, width), BF16),
                pltpu.VMEM((4 * rows0, (2 + streams) * part), F32),
                pltpu.VMEM((4, streams * rows0, part), BF16),
                pltpu.VMEM((streams * rows0, hd), BF16),
                pltpu.VMEM((streams * rows0, width), BF16),
                pltpu.VMEM((streams, rows0, width), BF16),
                pltpu.VMEM((2, 1, width), F32),
                pltpu.VMEM((1, width), F32),
                pltpu.VMEM((count, width), BF16),
                pltpu.VMEM((4 * group, part), BF16),
                pltpu.VMEM((16 * group, part), BF16),
                pltpu.VMEM((4 * group, hd), BF16),
                pltpu.VMEM((4 * group, width), F32),
                pltpu.VMEM((4 * group, width), F32),
                pltpu.VMEM((4, group, width), F32),
                pltpu.VMEM((4, tall, width), BF16),
                pltpu.VMEM((4, tall, width), BF16),
                pltpu.VMEM((4, tall, width), BF16),
                pltpu.VMEM((4, tall, width), BF16),
                pltpu.VMEM((4, group, width), F32),
                pltpu.VMEM((4, group, width), F32),
                pltpu.VMEM((group, width), F32),
                dma((9,)),
                dma((nz, 2)),
                dma((n,)),
                dma((STAGES,)),
                dma((STAGES,)),
                dma((3, 4 * nz)),
                dma((3, nz)),
                dma((4 * nz,)),
                dma((n, 2)),
            ],
            compiler_params=pltpu.CompilerParams(
                collective_id=0, has_side_effects=True, vmem_limit_bytes=60 * 2**20
            ),
        )(
            tokens.reshape(rows0, width),
            w_qkv[0],
            tangent_value[0],
            jnp.swapaxes(w_output[0], 0, 1),
            jnp.swapaxes(tangent_output[0], 1, 2),
            layer_gain,
            final_gain[None],
            head.T,
        )
        return logits[0], sum(logits[1 + j] * logits[1 + j] for j in range(tangents))

    return shards


def solution(mesh):
    n = mesh.shape["dp"]
    fast = mesh.shape["section"] == 2 and n % 4 == 0
    return jax.shard_map(
        two_sections(n) if fast else relay_shards,
        mesh=mesh,
        in_specs=(
            P(None, "dp", None, None),
            P("section", "dp", None),
            P("section", None, "dp"),
            P("section", None, "dp", None),
            P("section", None, None, "dp"),
            P("section", None),
            P(),
            P(None, "section"),
        ),
        out_specs=(P(None, "dp", "section"), P(None, "dp", "section")),
        check_vma=False,
    )
```

```python
import functools

import jax
import jax.numpy as jnp
from jax import lax
from jax.experimental import pallas as pl
from jax.experimental.pallas import tpu as pltpu
from jax.sharding import PartitionSpec as P

HEAD = 64
epsilon = 1e-06
F32, BF16 = jnp.float32, jnp.bfloat16
MESH = pl.DeviceIdType.MESH


def contract(spec, left, right):
    return jnp.einsum(spec, left, right, preferred_element_type=jnp.float32)


def norm_jvp(primal, tangents, gains):
    average = jnp.mean(primal, -1, keepdims=True)
    centred = primal - average
    inverse = lax.rsqrt(jnp.mean(centred * centred, -1, keepdims=True) + epsilon)
    dcentred = tangents - jnp.mean(tangents, -1, keepdims=True)
    dinverse = -(inverse**3) * jnp.mean(centred * dcentred, -1, keepdims=True)
    return (centred * inverse * gains, (dcentred * inverse + centred * dinverse) * gains)


def layer_step(state, qkv_weight, out_weight, value_tangent, out_tangent, gains):
    hd = out_weight.shape[0]
    heads = hd // HEAD
    resid = state.astype(F32)
    normed_zero, normed_rest = norm_jvp(resid[0], resid[1:], gains)
    normed = jnp.concatenate([normed_zero[None], normed_rest]).astype(BF16)
    streams, batch, tokens_here, width = normed.shape
    projected = contract("sbtd,de->sbte", normed, qkv_weight)
    extra_value = contract("btd,kde->kbte", normed[0], value_tangent)
    queries = projected[..., :hd]
    key_rows = projected[..., hd : 2 * hd]
    values = projected[..., 2 * hd :]
    values = jnp.concatenate([values[:1], values[1:] + extra_value])
    shape_heads = (streams, batch, tokens_here, heads, HEAD)
    queries = queries.astype(BF16).reshape(shape_heads)
    key_rows = key_rows.astype(BF16).reshape(shape_heads)
    values = values.astype(BF16).reshape(shape_heads)
    factor = HEAD ** (-0.5)
    scores = contract("bqhe,bkhe->bhqk", queries[0], key_rows[0]) * factor
    probs = jax.nn.softmax(scores, -1)
    dscores = (
        contract("sbqhe,bkhe->sbhqk", queries[1:], key_rows[0])
        + contract("bqhe,sbkhe->sbhqk", queries[0], key_rows[1:])
    ) * factor
    dprobs = probs * (dscores - jnp.sum(probs * dscores, -1, keepdims=True))
    probs_low = probs.astype(BF16)
    dprobs_low = dprobs.astype(BF16)
    attended_zero = contract("bhqk,bkhe->bqhe", probs_low, values[0])
    attended_rest = contract("sbhqk,bkhe->sbqhe", dprobs_low, values[0]) + contract(
        "bhqk,sbkhe->sbqhe", probs_low, values[1:]
    )
    attended = jnp.concatenate([attended_zero[None], attended_rest]).astype(BF16)
    attended = attended.reshape(streams, batch, tokens_here, hd)
    output = contract("sbte,ed->sbtd", attended, out_weight)
    extra_out = contract("bte,ked->kbtd", attended[0], out_tangent)
    output = jnp.concatenate([output[:1], output[1:] + extra_out])
    return (resid + output).astype(BF16)


def relay_shards(tokens, w_qkv, w_output, tangent_value, tangent_output, layer_gain, final_gain, head):
    full_qkv, full_output, full_value_tan, full_output_tan = (
        lax.all_gather(w_qkv, "dp", axis=1, tiled=True),
        lax.all_gather(w_output, "dp", axis=2, tiled=True),
        lax.all_gather(tangent_value, "dp", axis=2, tiled=True),
        lax.all_gather(tangent_output, "dp", axis=3, tiled=True),
    )
    tangents = tangent_value.shape[1]

    def advance_layer(state):
        return layer_step(
            state, full_qkv[0], full_output[0], full_value_tan[0], full_output_tan[0], layer_gain[0]
        )

    section_index = lax.axis_index("section")
    section_count = lax.axis_size("section")
    route = [(i, i + 1) for i in range(section_count - 1)]
    micro, _, toks, width = tokens.shape
    entering = jnp.concatenate(
        [tokens.reshape(1, micro, toks, width), jnp.zeros((tangents, micro, toks, width), BF16)]
    )

    def advance(step, outgoing):
        incoming = lax.ppermute(outgoing, "section", route)
        source = jnp.where(step == 0, entering, incoming)
        return lax.cond(section_index == step, advance_layer, jnp.zeros_like, source)

    finished = lax.fori_loop(0, section_count, advance, jnp.zeros_like(entering))
    collected = finished[:, :, 0, :]
    mine = section_index == section_count - 1
    features = lax.psum(jnp.where(mine, collected, jnp.zeros_like(collected)), "section")
    widened = features.astype(F32)
    final_zero, final_rest = norm_jvp(widened[0], widened[1:], final_gain)
    normed_final = jnp.concatenate([final_zero[None], final_rest]).astype(BF16)
    logits = contract("sbd,dc->sbc", normed_final, head)
    return (logits[0][:, None, :], jnp.sum(logits[1:] * logits[1:], 0)[:, None, :])


def dot(a, b):
    return lax.dot_general(a, b, (((1,), (0,)), ((), ())), preferred_element_type=F32)


def dot_t(a, b):
    return lax.dot_general(a, b, (((1,), (1,)), ((), ())), preferred_element_type=F32)


class Gather:
    def __init__(self, n, g, full, send, recv):
        self.nz = n // 4
        self.full, self.send, self.recv = full, send, recv
        self.rows = full.shape[1] // n
        self.g = g
        self.ends = []

    def span(self, start, count):
        return self.full.at[:, pl.ds(pl.multiple_of(start, self.rows // 2), count), :]

    def remote(self, ref, target, sem, recv):
        return pltpu.make_async_remote_copy(
            src_ref=ref,
            dst_ref=ref,
            send_sem=self.send.at[sem],
            recv_sem=recv,
            device_id={"section": self.g.section, "dp": target},
            device_id_type=MESH,
        )

    def copy(self, src, half, target, sem):
        depth = self.rows // 2
        ref = self.span(src * self.rows + half * depth, depth)
        return self.remote(ref, target, sem, self.recv.at[src, half])

    def forward(self, cond, src, half, target, sem):
        def go():
            self.copy(src, half, target, sem).start()

        go() if cond is None else pl.when(cond)(go)

    def ended(self, cond, pieces, sem):
        def end():
            self.remote(self.span(0, pieces * self.rows), self.g.me, sem, self.recv.at[0, 0]).wait_send()

        self.ends.append((cond, end))

    def arrived(self, src, half):
        self.copy(src, half, self.g.me, 0).wait_recv()

    def along(self):
        g, nz = self.g, self.nz
        for k in range(1, nz):
            for way in (k, -k):
                when = g.reaches(way)
                for half in range(2):
                    self.forward(when, g.me, half, g.me + 4 * way, g.z + way)
                self.ended(when, 1, g.z + way)

    def pass_on(self, d):
        g = self.g
        for shift, cond in g.sources(d):
            passed = g.passes(shift)
            if passed is not None:
                src = g.me + 4 * shift
                for half in range(2):
                    pl.when(passed)(functools.partial(self.arrived, src, half))
                    self.forward(passed, src, half, g.me - 4 if shift > 0 else g.me + 4, self.nz + d)
                self.ended(passed, 1, self.nz + d)

    def direct(self, d):
        g = self.g
        for side, (shift, cond) in enumerate(g.sources(d)):
            src = g.me + 4 * shift
            passed = g.passes(shift)
            for half in range(2):
                if d > 0:
                    fresh = cond if passed is None else cond & jnp.logical_not(passed)
                    pl.when(fresh)(functools.partial(self.arrived, src, half))
                for target in ((g.y_near, g.x_near), (g.x_near, g.y_near))[half]:
                    self.forward(cond, src, half, target, 2 * self.nz + 2 * d + side)
            self.ended(cond, 3, 2 * self.nz + 2 * d + side)

    def relay(self, d):
        g = self.g
        for side, (shift, cond) in enumerate(g.sources(d)):
            for half, near, target in ((0, g.x_near, g.y_near), (1, g.y_near, g.x_near)):
                src = near + 4 * shift
                wait = functools.partial(self.arrived, src, half)
                wait() if cond is None else pl.when(cond)(wait)
                self.forward(cond, src, half, target, 2 * self.nz + 2 * d + side)

    def rest(self):
        g = self.g
        for z in range(self.nz):
            up = 4 * (z - g.z)
            self.arrived(g.x_near + up, 1)
            self.arrived(g.y_near + up, 0)
            self.arrived(g.diagonal + up, 0)
            self.arrived(g.diagonal + up, 1)

    def drain(self):
        for cond, end in self.ends:
            end() if cond is None else pl.when(cond)(end)


class Place:
    def __init__(self, n):
        self.nz = n // 4
        self.me = lax.axis_index("dp")
        self.section = lax.axis_index("section")
        me = self.me
        self.x_near = me + 1 - 2 * (me % 2)
        self.y_near = me + 2 - 4 * ((me // 2) % 2)
        self.diagonal = self.x_near + self.y_near - me
        self.z = me // 4
        self.place = me % 4
        self.up, self.down = self.z + 1 < self.nz, self.z >= 1
        self.plane = (me, self.x_near, self.y_near, self.diagonal)

    def sources(self, d):
        if d == 0:
            return [(0, None)]
        return [(-d, self.z >= d), (d, self.z + d < self.nz)]

    def reaches(self, way):
        z, nz = self.z, self.nz
        there = z + way
        when = (there >= 0) & (there < nz)
        if abs(way) > 1:
            when = when & ((z == 0) | (z == nz - 1) | ((there > 0) & (there < nz - 1)))
        return when

    def passes(self, shift):
        z, nz = self.z, self.nz
        if not 0 < abs(shift) < nz - 2:
            return None
        return (z == 1) & (z + shift < nz - 1) if shift > 0 else (z == nz - 2) & (z + shift > 0)


def norm_rows(x, gains):
    average = jnp.mean(x, -1, keepdims=True)
    centred = x - average
    inverse = lax.rsqrt(jnp.mean(centred * centred, -1, keepdims=True) + epsilon)
    return centred, inverse, centred * inverse * gains


def norm_tangent(t, centred, inverse, gains):
    dcentred = t - jnp.mean(t, -1, keepdims=True)
    dinverse = -(inverse * inverse * inverse) * jnp.mean(centred * dcentred, -1, keepdims=True)
    return (dcentred * inverse + centred * dinverse) * gains


def softmax(scores):
    e = jnp.exp(scores - jnp.max(scores, -1, keepdims=True))
    return e / jnp.sum(e, -1, keepdims=True)


def at_rows(i, count):
    return pl.ds(pl.multiple_of(i * count, count), count)


def first_norm(sizes, tok, gain, normed, slot):
    micro, toks, width, hd, tangents = sizes
    for b in range(micro):
        x = tok[slot, pl.ds(b * toks, toks), :].astype(F32)
        normed[at_rows(slot * micro + b, toks), :] = norm_rows(x, gain)[2].astype(BF16)


def first_attend(sizes, acc, att, slot, b):
    micro, toks, width, hd, tangents = sizes
    factor = HEAD ** (-0.5)
    part = 2 * HEAD
    streams = 1 + tangents
    even = lax.broadcasted_iota(jnp.int32, (toks, part), 1) < HEAD
    rows = at_rows(slot * micro + b, toks)
    q = acc[rows, pl.ds(0, part)]
    k = acc[rows, pl.ds(part, part)].astype(BF16)
    v = acc[rows, pl.ds(2 * part, streams * part)].astype(BF16)
    zero = jnp.zeros_like(q)
    both = jnp.concatenate([jnp.where(even, q, zero), jnp.where(even, zero, q)], 0).astype(BF16)
    low = softmax(dot_t(both, k) * factor).astype(BF16)
    out = dot(low, v)
    for s in range(streams):
        joined = jnp.where(even, out[:toks, s * part : (s + 1) * part], out[toks:, s * part : (s + 1) * part])
        att[slot, pl.ds((s * micro + b) * toks, toks), :] = joined.astype(BF16)


def first_out(sizes, tok, place, b_full, att, state):
    micro, toks, width, hd, tangents = sizes
    rows0 = micro * toks
    tile = 256
    for c in range(width // tile):
        at = pl.ds(c * tile, tile)
        out = dot_t(att[...], b_full[0, at, :])
        extra = [dot_t(att[pl.ds(0, rows0), :], b_full[1 + j, at, :]) for j in range(tangents)]
        x = tok[place, :, at].astype(F32)
        state[pl.ds(0, rows0), at] = (x + out[:rows0]).astype(BF16)
        for j in range(tangents):
            state[pl.ds((1 + j) * rows0, rows0), at] = (
                out[(1 + j) * rows0 : (2 + j) * rows0] + extra[j]
            ).astype(BF16)


def group_of(sizes):
    micro, toks, width, hd, tangents = sizes
    return -(-micro * (1 + tangents) // 8) * 8


def stream_of(sizes, shape):
    return (lax.broadcasted_iota(jnp.int32, shape, 0) % group_of(sizes)) // sizes[0]


def lowered(sizes, parts):
    micro, tangents = sizes[0], sizes[4]
    stream = stream_of(sizes, parts[0].shape)
    total = parts[0]
    for j in range(tangents):
        moved = pltpu.roll(parts[1 + j], micro * (1 + j), 0)
        total = total + jnp.where(stream == 1 + j, moved, jnp.zeros_like(moved))
    return total


def primal_rows(sizes, x):
    micro, tangents = sizes[0], sizes[4]
    stream = stream_of(sizes, x.shape)
    spread = x
    for j in range(tangents):
        spread = jnp.where(stream == 1 + j, pltpu.roll(x, micro * (1 + j), 0), spread)
    return spread


def norm_group(sizes, x, gains):
    stream = stream_of(sizes, x.shape)
    centred, inverse, y = norm_rows(primal_rows(sizes, x), gains)
    dy = norm_tangent(x, centred, inverse, gains)
    return jnp.where(stream == 0, y, dy).astype(BF16)


def class_rows(sizes, state):
    micro, toks, width, hd, tangents = sizes
    streams = 1 + tangents
    rows = [
        state[pl.ds((s * micro + b) * toks, 16), :].astype(F32)[:1] for s in range(streams) for b in range(micro)
    ]
    return jnp.concatenate(rows + [jnp.zeros((group_of(sizes) - micro * streams, width), F32)], 0)


def last_norm(sizes, gain, state, normed):
    micro, toks, width, hd, tangents = sizes
    rows0 = micro * toks
    for b in range(micro):
        at = pl.ds(b * toks, toks)
        centred, inverse, y = norm_rows(state[at, :].astype(F32), gain)
        normed[0, at, :] = y.astype(BF16)
        for j in range(tangents):
            t = state[pl.ds((1 + j) * rows0 + b * toks, toks), :].astype(F32)
            normed[1 + j, at, :] = norm_tangent(t, centred, inverse, gain).astype(BF16)


def last_attend(sizes, u, normed):
    micro, toks, width, hd, tangents = sizes
    factor = HEAD ** (-0.5)
    shape = (u.shape[0], micro * toks)
    stream = stream_of(sizes, shape)
    image = (lax.broadcasted_iota(jnp.int32, shape, 0) % group_of(sizes)) % micro
    valid = lax.broadcasted_iota(jnp.int32, shape, 1) // toks == image
    parts = [dot_t(u, normed[s]) * factor for s in range(1 + tangents)]
    probs = softmax(jnp.where(valid, parts[0], -jnp.inf))
    weights = primal_rows(sizes, probs)
    scores = lowered(sizes, parts)
    dprobs = weights * (scores - jnp.sum(weights * scores, -1, keepdims=True))
    zero = jnp.zeros_like(weights)
    total = dot(jnp.where(stream == 0, weights, dprobs).astype(BF16), normed[0])
    for j in range(tangents):
        total = total + dot(jnp.where(stream == 1 + j, weights, zero).astype(BF16), normed[1 + j])
    return total.astype(BF16)


TOK, TOKY, TOKD, LA, LB, ATT, ATC, CLS, U, M, O1, O0, GAIN, FIRST, STAGES = range(15)


def kernel(
    n, sizes, tokens, w_qkv, tangent_value, w_out, t_out, gain_in, final_in, head_in, logit_ref,
    a_stage, b_stage, a0, a1, b1, b_full, tok, normed_all, acc, att_out, att_in, state, normed,
    gains, final_gain, head, atc_out, atc_all, atc_in, cls_out, cls_in, cls_all, u_out, u_all, m_out, m_all, o_out, o_all, classes,
    loads, a_send, a_recv, stage_send, stage_recv, far_send, far_recv, b_send, b_recv,
):
    micro, toks, width, hd, tangents = sizes
    streams = 1 + tangents
    part = hd // 4
    share = part // HEAD
    g = Place(n)
    me, section, place, z, nz = g.me, g.section, g.place, g.z, g.nz
    other = 1 - section
    rows = width // n
    slab = 4 * rows
    group = group_of(sizes)
    own = at_rows(me, rows)

    barrier = pltpu.get_barrier_semaphore()

    def greet(target, sec):
        pl.semaphore_signal(
            barrier, inc=1, device_id={"section": sec, "dp": target}, device_id_type=MESH
        )

    for k in range(1, nz):
        greet(((z + k) % nz) * 4 + place, section)
    for near in (g.diagonal, g.x_near, g.y_near):
        greet(near, section)
        greet(near, other)
    greet(me, other)

    def column(p):
        return pl.ds(p * part, part) if isinstance(p, int) else at_rows(p, part)

    def load(i, src, dst):
        return pltpu.make_async_copy(src, dst, loads.at[i])

    def stage_loads():
        for p in range(4):
            for m in range(3):
                load(5, w_qkv.at[:, pl.ds(m * hd + p * part, part)], a_stage.at[p, :, pl.ds(m * part, part)]).start()
            for j in range(tangents):
                load(
                    5,
                    tangent_value.at[j, :, pl.ds(p * part, part)],
                    a_stage.at[p, :, pl.ds((3 + j) * part, part)],
                ).start()

    def own_loads():
        for m in range(3):
            load(6, w_qkv.at[:, column(m * 4 + place)], a1.at[own, pl.ds(m * part, part)]).start()
        for j in range(tangents):
            load(6, tangent_value.at[j, :, column(place)], a1.at[own, pl.ds((3 + j) * part, part)]).start()
        load(7, w_out.at[:, column(place)], b1.at[0, own, :]).start()
        load(7, t_out.at[:, :, column(place)], b1.at[pl.ds(1, tangents), own, :]).start()
        for p in range(4):
            load(8, w_out.at[:, pl.ds(p * part, part)], b_stage.at[p, 0]).start()
            load(8, t_out.at[:, :, pl.ds(p * part, part)], b_stage.at[p, pl.ds(1, tangents)]).start()

    def b_loads():
        load(4, w_out, b_full.at[0, own, :]).start()
        load(4, t_out, b_full.at[pl.ds(1, tangents), own, :]).start()

    def loaded(i, ref):
        load(i, ref, ref).wait()

    def gain_load():
        return load(0, gain_in, gains.at[section])

    def tok_load():
        return load(1, tokens, tok.at[place])

    def tail_loads():
        return [load(2, head_in, head), load(3, final_in, final_gain)]

    stage_loads()
    gain_load().start()
    tok_load().start()
    pl.when(section == 0)(b_loads)
    pl.when(section == 1)(own_loads)
    for move in tail_loads():
        move.start()
    pl.semaphore_wait(barrier, 7 + nz - 1)

    def xfer(stage, src, dst, target, sec):
        return pltpu.make_async_remote_copy(
            src_ref=src,
            dst_ref=dst,
            send_sem=stage_send.at[stage],
            recv_sem=stage_recv.at[stage],
            device_id={"section": sec, "dp": target},
            device_id_type=MESH,
        )

    def arrived(stage, ref):
        xfer(stage, ref, ref, me, other).wait_recv()

    sent = []

    FAR = (3, 1, 2, 0)

    def scatter(stage, src, dst, sec, total, skip_own=False):
        for i in FAR:
            if i > 0 or not skip_own:
                target = g.plane[i]
                xfer(stage, src(target % 4), dst, target, sec).start()
        sent.append((stage, total))

    def drain():
        for stage, ref in sent:
            xfer(stage, ref, ref, me, other).wait_send()
        sent.clear()

    def a_ref(src):
        return a0.at[at_rows(src, rows), :]

    def a_copy(src_ref, src, sem, target, sec):
        return pltpu.make_async_remote_copy(
            src_ref=src_ref,
            dst_ref=a_ref(src),
            send_sem=sem,
            recv_sem=a_recv.at[src],
            device_id={"section": sec, "dp": target},
            device_id_type=MESH,
        )

    @pl.when(section == 0)
    def _():
        loaded(5, a_stage)
        for i in range(4):
            target = g.plane[i]
            a_copy(a_stage.at[target % 4], me, stage_send.at[FIRST], target, other).start()
        sent.append((FIRST, a_stage))
        gain_load().wait()
        xfer(GAIN, gains.at[section], gains.at[section], me, other).start()
        sent.append((GAIN, gains.at[section]))
        loaded(4, b_full.at[:, own, :])
        gather = Gather(n, g, b_full, b_send, b_recv)
        lag = 2
        gather.along()
        for d in range(nz + lag):
            if d < nz:
                gather.pass_on(d)
                gather.direct(d)
            if d >= lag:
                gather.relay(d - lag)
        tok_load().wait()
        gather.rest()
        arrived(ATC, atc_in)
        cls_out[...] = lowered(sizes, [dot_t(atc_in[...], b_full[s]) for s in range(streams)])
        xfer(CLS, cls_out, cls_in, me, other).start()
        sent.append((CLS, cls_out))
        arrived(ATT, att_in)
        first_out(sizes, tok, place, b_full, att_in, state)
        arrived(GAIN, gains.at[other])
        last_norm(sizes, gains[1], state, normed)
        arrived(U, u_all)
        u = jnp.concatenate([u_all[p] for p in range(4)], 0)
        m = last_attend(sizes, u, normed)
        for p in range(4):
            m_out[p] = m[p * share * group : (p + 1) * share * group]
        scatter(M, lambda p: m_out.at[p], m_all.at[place], other, m_out)
        classes[...] = class_rows(sizes, state)
        arrived(O0, o_all)
        drain()
        gather.drain()

    @pl.when(section == 1)
    def _():
        gain_load().wait()
        xfer(GAIN, gains.at[section], gains.at[section], me, other).start()
        sent.append((GAIN, gains.at[section]))
        tok_load().wait()

        def relay(d, some=g.plane):
            for shift, cond in g.sources(d):

                def step(shift=shift, d=d):
                    for near in some:
                        src = near + 4 * shift
                        a_copy(a_ref(src), src, a_send.at[d, 0], me, section).wait_recv()
                        if shift <= 0 and d < nz - 1:
                            pl.when(g.up)(
                                lambda: a_copy(a_ref(src), src, a_send.at[d, 0], me + 4, section).start()
                            )
                        if shift >= 0 and d < nz - 1:
                            pl.when(g.down)(
                                lambda: a_copy(a_ref(src), src, a_send.at[d, 1], me - 4, section).start()
                            )

                step() if cond is None else pl.when(cond)(step)

        def relay_end(d):
            slab_ref = a0.at[pl.ds(0, slab), :]
            for shift, cond in g.sources(d):

                def end(way):
                    pltpu.make_async_remote_copy(
                        src_ref=slab_ref,
                        dst_ref=slab_ref,
                        send_sem=a_send.at[d, way],
                        recv_sem=a_recv.at[0],
                        device_id={"section": section, "dp": me},
                        device_id_type=MESH,
                    ).wait_send()

                if shift <= 0:
                    pl.when(g.up if cond is None else cond & g.up)(functools.partial(end, 0))
                if shift >= 0:
                    pl.when(g.down if cond is None else cond & g.down)(functools.partial(end, 1))

        def project(d):
            for shift, cond in g.sources(d):

                def step(shift=shift):
                    at = at_rows(z + shift, slab)
                    term = dot(normed_all[:, at], a0[at, :])
                    acc[...] = term if d == 0 else acc[...] + term

                step() if cond is None else pl.when(cond)(step)

        relay(0, g.plane[:1])
        for stage, near in ((TOK, g.x_near), (TOKY, g.y_near)):
            xfer(stage, tok.at[place], tok.at[place], near, section).start()
            sent.append((stage, tok.at[place]))
        loaded(5, a_stage)
        loaded(6, a1.at[own, :])
        loaded(7, b1.at[:, own, :])
        scatter(LA, lambda p: a_stage.at[p], a1.at[own, :], section, a_stage.at[pl.ds(0, 3)], True)
        relay(0, g.plane[1:])
        arrived(GAIN, gains.at[other])
        first_norm(sizes, tok, gains[0], normed_all, place)
        relay(1)
        half = micro * toks // 2
        for stage, near, target, first in ((TOK, g.x_near, g.y_near, 0), (TOKY, g.y_near, g.x_near, half)):
            arrived(stage, tok.at[near % 4])
            piece = tok.at[near % 4, pl.ds(first, half), :]
            xfer(TOKD, piece, piece, target, section).start()
        sent.append((TOKD, tok.at[0]))
        loaded(8, b_stage)
        scatter(LB, lambda p: b_stage.at[p], b1.at[:, own, :], section, b_stage.at[pl.ds(0, 3)], True)

        def far(kind, zc):
            at = at_rows(zc, slab)
            if kind == 0:
                return a1.at[at, pl.ds(0, 2 * part)]
            if kind == 1:
                return a1.at[at, pl.ds(2 * part, streams * part)]
            return b1.at[:, at, :]

        def far_copy(kind, zc, slot, target):
            return pltpu.make_async_remote_copy(
                src_ref=far(kind, zc),
                dst_ref=far(kind, zc),
                send_sem=far_send.at[kind, slot],
                recv_sem=far_recv.at[kind, zc],
                device_id={"section": section, "dp": target},
                device_id_type=MESH,
            )

        ends = (z == 0) | (z == nz - 1)

        def far_sends(kind):
            for k in range(1, nz):
                for way in (k, -k):
                    there = z + way
                    when = (there >= 0) & (there < nz)
                    if k > 1:
                        when = when & (ends | ((there > 0) & (there < nz - 1)))
                    yield when, functools.partial(far_copy, kind, z, there, me + 4 * way)

        def far_relay(kind):
            for k in range(1, nz - 2):
                yield (z == 1) & (z + k < nz - 1), z + k, functools.partial(far_copy, kind, z + k, nz + k, me - 4)
                yield (z == nz - 2) & (z - k > 0), z - k, functools.partial(far_copy, kind, z - k, nz + k, me + 4)

        def far_start(kind, late):
            for k, (when, move) in enumerate(far_sends(kind)):
                if (k // 2 == nz - 2) == late:
                    pl.when(when)(lambda: move().start())

        def far_pass(kind):
            for when, zc, move in far_relay(kind):

                def step():
                    far_copy(kind, zc, 0, me).wait_recv()
                    move().start()

                pl.when(when)(step)

        def far_wait(kind):
            for k in range(1, nz):
                for way in (k, -k):
                    there = z + way
                    when = (there >= 0) & (there < nz)
                    if 0 < k < nz - 2:
                        passed = ((z == 1) & (there > 1) & (there < nz - 1)) | (
                            (z == nz - 2) & (there > 0) & (there < nz - 2)
                        )
                        when = when & jnp.logical_not(passed)
                    pl.when(when)(lambda: far_copy(kind, there, 0, me).wait_recv())

        def far_end(kind):
            for when, move in far_sends(kind):
                pl.when(when)(lambda: move().wait_send())
            for when, zc, move in far_relay(kind):
                pl.when(when)(lambda: move().wait_send())

        def far_begin():
            arrived(LA, a1.at[pl.ds(0, 3 * rows), :])
            far_start(0, False)
            far_start(1, False)

        for near in (g.x_near, g.y_near):
            first_norm(sizes, tok, gains[0], normed_all, near % 4)
        for d in range(2, nz - 1):
            relay(d)
        arrived(TOKD, tok.at[g.diagonal % 4])
        first_norm(sizes, tok, gains[0], normed_all, g.diagonal % 4)
        for d in range(nz - 1):
            project(d)
        far_begin()
        if nz > 2:
            relay(nz - 1)
        far_start(0, True)
        far_start(1, True)
        project(nz - 1)
        def give(i):
            target = g.plane[i]
            xfer(ATT, att_out.at[target % 4], att_in.at[:, column(place)], target, other).start()

        for i in FAR:
            for b in range(micro):
                first_attend(sizes, acc, att_out, g.plane[i] % 4, b)
            if i > 0:
                give(i)
            if i == FAR[1]:
                arrived(LB, b1.at[:, pl.ds(0, 3 * rows), :])
                far_start(2, False)
                far_start(2, True)
        firsts = []
        for p in range(4):
            for i in range(group):
                at = pl.ds(i * toks, 16) if i < streams * micro else pl.ds(0, 16)
                firsts.append(att_out[p, at, :].astype(F32)[:1])
        atc_out[...] = jnp.concatenate(firsts, 0).astype(BF16)
        scatter(ATC, lambda p: atc_out, atc_in.at[:, column(place)], other, atc_all)
        give(0)
        sent.append((ATT, att_out))
        far_pass(0)
        fresh = []
        blank = jnp.zeros((group - micro, width), F32)
        for p in range(4):
            fresh += [tok[p, pl.ds(b * toks, 16), :].astype(F32)[:1] for b in range(micro)] + [blank]
        fresh = jnp.concatenate(fresh, 0)
        far_wait(0)
        arrived(CLS, cls_in)
        x = (fresh + cls_in[...]).astype(BF16).astype(F32)
        for p in range(4):
            cls_all[p] = x[p * group : (p + 1) * group]
        q = dot(norm_group(sizes, x, gains[1]), a1[:, pl.ds(0, part)]).astype(BF16).astype(F32)
        owner = lax.broadcasted_iota(jnp.int32, (group, part), 1) // HEAD
        zero = jnp.zeros((group, part), F32)
        spread = [
            jnp.where(owner == h, q[p * group : (p + 1) * group], zero) for p in range(4) for h in range(share)
        ]
        u = dot_t(jnp.concatenate(spread, 0).astype(BF16), a1[:, pl.ds(part, part)]).astype(BF16)
        tall = share * group
        for p in range(4):
            u_out[p] = u[p * tall : (p + 1) * tall]
        scatter(U, lambda p: u_out.at[p], u_all.at[place], other, u_out)
        far_pass(1)
        far_pass(2)
        far_wait(1)
        arrived(M, m_all)
        m = jnp.concatenate([m_all[p] for p in range(4)], 0)
        r = dot(m, a1[:, pl.ds(2 * part, streams * part)])
        mixed = lowered(sizes, [r[:, s * part : (s + 1) * part] for s in range(streams)])
        chosen = []
        for p in range(4):
            block = zero
            for h in range(share):
                at = p * tall + h * group
                block = jnp.where(owner == h, mixed[at : at + group], block)
            chosen.append(block)
        attended = jnp.concatenate(chosen, 0).astype(BF16)
        far_wait(2)
        out = lowered(sizes, [dot_t(attended, b1[s]) for s in range(streams)])
        for p in range(4):
            o_out[p] = out[p * group : (p + 1) * group].astype(BF16)
        scatter(O1, lambda p: o_out.at[p], o_all.at[place], section, o_out.at[pl.ds(0, 3)], True)
        scatter(O0, lambda p: o_out.at[p], o_all.at[place], other, o_out)
        o_all[place] = o_out[place]
        classes[...] = cls_all[place]
        arrived(O1, o_all.at[pl.ds(0, 3)])
        drain()
        for d in range(nz - 1):
            relay_end(d)
        for kind in range(3):
            far_end(kind)

    for move in tail_loads():
        move.wait()
    total = sum(o_all[p].astype(F32) for p in range(4))
    final = (classes[...] + total).astype(BF16).astype(F32)
    features = norm_group(sizes, final, final_gain[...])
    logits = dot_t(features, head[...])
    for s in range(streams):
        logit_ref[s, :, 0, :] = logits[s * micro : (s + 1) * micro]


def two_sections(n):
    def shards(tokens, w_qkv, w_output, tangent_value, tangent_output, layer_gain, final_gain, head):
        micro, _, toks, width = tokens.shape
        tangents = tangent_value.shape[1]
        hd = w_output.shape[1]
        count = head.shape[1]
        rows = width // n
        part = hd // 4
        nz = n // 4
        sizes = (micro, toks, width, hd, tangents)
        streams = 1 + tangents
        rows0 = micro * toks
        group = group_of(sizes)
        tall = part // HEAD * group
        vmem = pl.BlockSpec(memory_space=pltpu.VMEM)
        anywhere = pl.BlockSpec(memory_space=pl.ANY)
        dma = pltpu.SemaphoreType.DMA
        logits = pl.pallas_call(
            functools.partial(kernel, n, sizes),
            out_shape=jax.ShapeDtypeStruct((streams, micro, 1, count), F32),
            in_specs=[anywhere] * 8,
            out_specs=vmem,
            scratch_shapes=[
                pltpu.VMEM((4, rows, (2 + streams) * part), BF16),
                pltpu.VMEM((4, streams, rows, part), BF16),
                pltpu.VMEM((width, (2 + streams) * part), BF16),
                pltpu.VMEM((width, (2 + streams) * part), BF16),
                pltpu.VMEM((streams, width, part), BF16),
                pltpu.VMEM((streams, width, hd), BF16),
                pltpu.VMEM((4, rows0, width), BF16),
                pltpu.VMEM((4 * rows0, width), BF16),
                pltpu.VMEM((4 * rows0, (2 + streams) * part), F32),
                pltpu.VMEM((4, streams * rows0, part), BF16),
                pltpu.VMEM((streams * rows0, hd), BF16),
                pltpu.VMEM((streams * rows0, width), BF16),
                pltpu.VMEM((streams, rows0, width), BF16),
                pltpu.VMEM((2, 1, width), F32),
                pltpu.VMEM((1, width), F32),
                pltpu.VMEM((count, width), BF16),
                pltpu.VMEM((4 * group, part), BF16),
                pltpu.VMEM((16 * group, part), BF16),
                pltpu.VMEM((4 * group, hd), BF16),
                pltpu.VMEM((4 * group, width), F32),
                pltpu.VMEM((4 * group, width), F32),
                pltpu.VMEM((4, group, width), F32),
                pltpu.VMEM((4, tall, width), BF16),
                pltpu.VMEM((4, tall, width), BF16),
                pltpu.VMEM((4, tall, width), BF16),
                pltpu.VMEM((4, tall, width), BF16),
                pltpu.VMEM((4, group, width), BF16),
                pltpu.VMEM((4, group, width), BF16),
                pltpu.VMEM((group, width), F32),
                dma((9,)),
                dma((nz, 2)),
                dma((n,)),
                dma((STAGES,)),
                dma((STAGES,)),
                dma((3, 2 * nz)),
                dma((3, nz)),
                dma((4 * nz,)),
                dma((n, 2)),
            ],
            compiler_params=pltpu.CompilerParams(
                collective_id=0, has_side_effects=True, vmem_limit_bytes=60 * 2**20
            ),
        )(
            tokens.reshape(rows0, width),
            w_qkv[0],
            tangent_value[0],
            jnp.swapaxes(w_output[0], 0, 1),
            jnp.swapaxes(tangent_output[0], 1, 2),
            layer_gain,
            final_gain[None],
            head.T,
        )
        return logits[0], sum(logits[1 + j] * logits[1 + j] for j in range(tangents))

    return shards


def solution(mesh):
    n = mesh.shape["dp"]
    fast = mesh.shape["section"] == 2 and n % 4 == 0
    return jax.shard_map(
        two_sections(n) if fast else relay_shards,
        mesh=mesh,
        in_specs=(
            P(None, "dp", None, None),
            P("section", "dp", None),
            P("section", None, "dp"),
            P("section", None, "dp", None),
            P("section", None, None, "dp"),
            P("section", None),
            P(),
            P(None, "section"),
        ),
        out_specs=(P(None, "dp", "section"), P(None, "dp", "section")),
        check_vma=False,
    )
```

```python
import functools

import jax
import jax.numpy as jnp
from jax import lax
from jax.experimental import pallas as pl
from jax.experimental.pallas import tpu as pltpu
from jax.sharding import PartitionSpec as P

HEAD = 64
epsilon = 1e-06
F32, BF16 = jnp.float32, jnp.bfloat16
MESH = pl.DeviceIdType.MESH


def contract(spec, left, right):
    return jnp.einsum(spec, left, right, preferred_element_type=jnp.float32)


def norm_jvp(primal, tangents, gains):
    average = jnp.mean(primal, -1, keepdims=True)
    centred = primal - average
    inverse = lax.rsqrt(jnp.mean(centred * centred, -1, keepdims=True) + epsilon)
    dcentred = tangents - jnp.mean(tangents, -1, keepdims=True)
    dinverse = -(inverse**3) * jnp.mean(centred * dcentred, -1, keepdims=True)
    return (centred * inverse * gains, (dcentred * inverse + centred * dinverse) * gains)


def layer_step(state, qkv_weight, out_weight, value_tangent, out_tangent, gains):
    hd = out_weight.shape[0]
    heads = hd // HEAD
    resid = state.astype(F32)
    normed_zero, normed_rest = norm_jvp(resid[0], resid[1:], gains)
    normed = jnp.concatenate([normed_zero[None], normed_rest]).astype(BF16)
    streams, batch, tokens_here, width = normed.shape
    projected = contract("sbtd,de->sbte", normed, qkv_weight)
    extra_value = contract("btd,kde->kbte", normed[0], value_tangent)
    queries = projected[..., :hd]
    key_rows = projected[..., hd : 2 * hd]
    values = projected[..., 2 * hd :]
    values = jnp.concatenate([values[:1], values[1:] + extra_value])
    shape_heads = (streams, batch, tokens_here, heads, HEAD)
    queries = queries.astype(BF16).reshape(shape_heads)
    key_rows = key_rows.astype(BF16).reshape(shape_heads)
    values = values.astype(BF16).reshape(shape_heads)
    factor = HEAD ** (-0.5)
    scores = contract("bqhe,bkhe->bhqk", queries[0], key_rows[0]) * factor
    probs = jax.nn.softmax(scores, -1)
    dscores = (
        contract("sbqhe,bkhe->sbhqk", queries[1:], key_rows[0])
        + contract("bqhe,sbkhe->sbhqk", queries[0], key_rows[1:])
    ) * factor
    dprobs = probs * (dscores - jnp.sum(probs * dscores, -1, keepdims=True))
    probs_low = probs.astype(BF16)
    dprobs_low = dprobs.astype(BF16)
    attended_zero = contract("bhqk,bkhe->bqhe", probs_low, values[0])
    attended_rest = contract("sbhqk,bkhe->sbqhe", dprobs_low, values[0]) + contract(
        "bhqk,sbkhe->sbqhe", probs_low, values[1:]
    )
    attended = jnp.concatenate([attended_zero[None], attended_rest]).astype(BF16)
    attended = attended.reshape(streams, batch, tokens_here, hd)
    output = contract("sbte,ed->sbtd", attended, out_weight)
    extra_out = contract("bte,ked->kbtd", attended[0], out_tangent)
    output = jnp.concatenate([output[:1], output[1:] + extra_out])
    return (resid + output).astype(BF16)


def relay_shards(tokens, w_qkv, w_output, tangent_value, tangent_output, layer_gain, final_gain, head):
    full_qkv, full_output, full_value_tan, full_output_tan = (
        lax.all_gather(w_qkv, "dp", axis=1, tiled=True),
        lax.all_gather(w_output, "dp", axis=2, tiled=True),
        lax.all_gather(tangent_value, "dp", axis=2, tiled=True),
        lax.all_gather(tangent_output, "dp", axis=3, tiled=True),
    )
    tangents = tangent_value.shape[1]

    def advance_layer(state):
        return layer_step(
            state, full_qkv[0], full_output[0], full_value_tan[0], full_output_tan[0], layer_gain[0]
        )

    section_index = lax.axis_index("section")
    section_count = lax.axis_size("section")
    route = [(i, i + 1) for i in range(section_count - 1)]
    micro, _, toks, width = tokens.shape
    entering = jnp.concatenate(
        [tokens.reshape(1, micro, toks, width), jnp.zeros((tangents, micro, toks, width), BF16)]
    )

    def advance(step, outgoing):
        incoming = lax.ppermute(outgoing, "section", route)
        source = jnp.where(step == 0, entering, incoming)
        return lax.cond(section_index == step, advance_layer, jnp.zeros_like, source)

    finished = lax.fori_loop(0, section_count, advance, jnp.zeros_like(entering))
    collected = finished[:, :, 0, :]
    mine = section_index == section_count - 1
    features = lax.psum(jnp.where(mine, collected, jnp.zeros_like(collected)), "section")
    widened = features.astype(F32)
    final_zero, final_rest = norm_jvp(widened[0], widened[1:], final_gain)
    normed_final = jnp.concatenate([final_zero[None], final_rest]).astype(BF16)
    logits = contract("sbd,dc->sbc", normed_final, head)
    return (logits[0][:, None, :], jnp.sum(logits[1:] * logits[1:], 0)[:, None, :])


def dot(a, b):
    return lax.dot_general(a, b, (((1,), (0,)), ((), ())), preferred_element_type=F32)


def dot_t(a, b):
    return lax.dot_general(a, b, (((1,), (1,)), ((), ())), preferred_element_type=F32)


class Gather:
    def __init__(self, n, g, full, send, recv):
        self.nz = n // 4
        self.full, self.send, self.recv = full, send, recv
        self.rows = full.shape[1] // n
        self.g = g
        self.ends = []

    def span(self, start, count):
        return self.full.at[:, pl.ds(pl.multiple_of(start, self.rows // 2), count), :]

    def remote(self, ref, target, sem, recv):
        return pltpu.make_async_remote_copy(
            src_ref=ref,
            dst_ref=ref,
            send_sem=self.send.at[sem],
            recv_sem=recv,
            device_id={"section": self.g.section, "dp": target},
            device_id_type=MESH,
        )

    def copy(self, src, half, target, sem):
        depth = self.rows // 2
        ref = self.span(src * self.rows + half * depth, depth)
        return self.remote(ref, target, sem, self.recv.at[src, half])

    def forward(self, cond, src, half, target, sem):
        def go():
            self.copy(src, half, target, sem).start()

        go() if cond is None else pl.when(cond)(go)

    def ended(self, cond, pieces, sem):
        def end():
            self.remote(self.span(0, pieces * self.rows), self.g.me, sem, self.recv.at[0, 0]).wait_send()

        self.ends.append((cond, end))

    def arrived(self, src, half):
        self.copy(src, half, self.g.me, 0).wait_recv()

    def along(self, far):
        g, nz = self.g, self.nz
        for k in range(2, nz) if far else range(1, min(nz, 2)):
            for way in (k, -k):
                when = g.reaches(way)
                for half in range(2):
                    self.forward(when, g.me, half, g.me + 4 * way, g.z + way)
                self.ended(when, 1, g.z + way)

    def pass_on(self, d):
        g = self.g
        for shift, cond in g.sources(d):
            passed = g.passes(shift)
            if passed is not None:
                src = g.me + 4 * shift
                for half in range(2):
                    pl.when(passed)(functools.partial(self.arrived, src, half))
                    self.forward(passed, src, half, g.me - 4 if shift > 0 else g.me + 4, self.nz + d)
                self.ended(passed, 1, self.nz + d)

    def direct(self, d):
        g = self.g
        for side, (shift, cond) in enumerate(g.sources(d)):
            src = g.me + 4 * shift
            passed = g.passes(shift)
            for half in range(2):
                if d > 0:
                    fresh = cond if passed is None else cond & jnp.logical_not(passed)
                    pl.when(fresh)(functools.partial(self.arrived, src, half))
                for target in ((g.y_near, g.x_near), (g.x_near, g.y_near))[half]:
                    self.forward(cond, src, half, target, 2 * self.nz + 2 * d + side)
            self.ended(cond, 3, 2 * self.nz + 2 * d + side)

    def relay(self, d):
        g = self.g
        for side, (shift, cond) in enumerate(g.sources(d)):
            for half, near, target in ((0, g.x_near, g.y_near), (1, g.y_near, g.x_near)):
                src = near + 4 * shift
                wait = functools.partial(self.arrived, src, half)
                wait() if cond is None else pl.when(cond)(wait)
                self.forward(cond, src, half, target, 2 * self.nz + 2 * d + side)

    def rest(self):
        g = self.g
        for z in range(self.nz):
            up = 4 * (z - g.z)
            self.arrived(g.x_near + up, 1)
            self.arrived(g.y_near + up, 0)
            self.arrived(g.diagonal + up, 0)
            self.arrived(g.diagonal + up, 1)

    def drain(self):
        for cond, end in self.ends:
            end() if cond is None else pl.when(cond)(end)


class Place:
    def __init__(self, n):
        self.nz = n // 4
        self.me = lax.axis_index("dp")
        self.section = lax.axis_index("section")
        me = self.me
        self.x_near = me + 1 - 2 * (me % 2)
        self.y_near = me + 2 - 4 * ((me // 2) % 2)
        self.diagonal = self.x_near + self.y_near - me
        self.z = me // 4
        self.place = me % 4
        self.up, self.down = self.z + 1 < self.nz, self.z >= 1
        self.plane = (me, self.x_near, self.y_near, self.diagonal)

    def sources(self, d):
        if d == 0:
            return [(0, None)]
        return [(-d, self.z >= d), (d, self.z + d < self.nz)]

    def reaches(self, way):
        z, nz = self.z, self.nz
        there = z + way
        when = (there >= 0) & (there < nz)
        if abs(way) > 1:
            when = when & ((z == 0) | (z == nz - 1) | ((there > 0) & (there < nz - 1)))
        return when

    def passes(self, shift):
        z, nz = self.z, self.nz
        if not 0 < abs(shift) < nz - 2:
            return None
        return (z == 1) & (z + shift < nz - 1) if shift > 0 else (z == nz - 2) & (z + shift > 0)


def norm_rows(x, gains):
    average = jnp.mean(x, -1, keepdims=True)
    centred = x - average
    inverse = lax.rsqrt(jnp.mean(centred * centred, -1, keepdims=True) + epsilon)
    return centred, inverse, centred * inverse * gains


def norm_tangent(t, centred, inverse, gains):
    dcentred = t - jnp.mean(t, -1, keepdims=True)
    dinverse = -(inverse * inverse * inverse) * jnp.mean(centred * dcentred, -1, keepdims=True)
    return (dcentred * inverse + centred * dinverse) * gains


def softmax(scores):
    e = jnp.exp(scores - jnp.max(scores, -1, keepdims=True))
    return e / jnp.sum(e, -1, keepdims=True)


def at_rows(i, count):
    return pl.ds(pl.multiple_of(i * count, count), count)


def first_norm(sizes, tok, gain, normed, slot):
    micro, toks, width, hd, tangents = sizes
    for b in range(micro):
        x = tok[slot, pl.ds(b * toks, toks), :].astype(F32)
        normed[at_rows(slot * micro + b, toks), :] = norm_rows(x, gain)[2].astype(BF16)


def first_attend(sizes, acc, att, slot, b):
    micro, toks, width, hd, tangents = sizes
    factor = HEAD ** (-0.5)
    part = 2 * HEAD
    streams = 1 + tangents
    even = lax.broadcasted_iota(jnp.int32, (toks, part), 1) < HEAD
    rows = at_rows(slot * micro + b, toks)
    q = acc[rows, pl.ds(0, part)]
    k = acc[rows, pl.ds(part, part)].astype(BF16)
    v = acc[rows, pl.ds(2 * part, streams * part)].astype(BF16)
    zero = jnp.zeros_like(q)
    both = jnp.concatenate([jnp.where(even, q, zero), jnp.where(even, zero, q)], 0).astype(BF16)
    scores = dot_t(both, k) * factor
    low = jnp.exp(scores - jnp.max(scores, -1, keepdims=True)).astype(BF16)
    out = dot(low, jnp.concatenate([v, jnp.ones((toks, part), BF16)], 1))

    def joined(s):
        at = slice(s * part, (s + 1) * part)
        return jnp.where(even, out[:toks, at], out[toks:, at])

    scale = 1.0 / joined(streams)
    for s in range(streams):
        att[slot, pl.ds((s * micro + b) * toks, toks), :] = (joined(s) * scale).astype(BF16)


def first_out(sizes, tok, place, b_full, att, state):
    micro, toks, width, hd, tangents = sizes
    rows0 = micro * toks
    tile = 256
    for c in range(width // tile):
        at = pl.ds(c * tile, tile)
        out = dot_t(att[...], b_full[0, at, :])
        extra = [dot_t(att[pl.ds(0, rows0), :], b_full[1 + j, at, :]) for j in range(tangents)]
        x = tok[place, :, at].astype(F32)
        state[pl.ds(0, rows0), at] = (x + out[:rows0]).astype(BF16)
        for j in range(tangents):
            state[pl.ds((1 + j) * rows0, rows0), at] = (
                out[(1 + j) * rows0 : (2 + j) * rows0] + extra[j]
            ).astype(BF16)


def group_of(sizes):
    micro, toks, width, hd, tangents = sizes
    return -(-micro * (1 + tangents) // 8) * 8


def stream_of(sizes, shape):
    return (lax.broadcasted_iota(jnp.int32, shape, 0) % group_of(sizes)) // sizes[0]


def lowered(sizes, parts):
    micro, tangents = sizes[0], sizes[4]
    stream = stream_of(sizes, parts[0].shape)
    total = parts[0]
    for j in range(tangents):
        moved = pltpu.roll(parts[1 + j], micro * (1 + j), 0)
        total = total + jnp.where(stream == 1 + j, moved, jnp.zeros_like(moved))
    return total


def primal_rows(sizes, x):
    micro, tangents = sizes[0], sizes[4]
    stream = stream_of(sizes, x.shape)
    spread = x
    for j in range(tangents):
        spread = jnp.where(stream == 1 + j, pltpu.roll(x, micro * (1 + j), 0), spread)
    return spread


def norm_group(sizes, x, gains):
    stream = stream_of(sizes, x.shape)
    centred, inverse, y = norm_rows(primal_rows(sizes, x), gains)
    dy = norm_tangent(x, centred, inverse, gains)
    return jnp.where(stream == 0, y, dy).astype(BF16)


def class_rows(sizes, state):
    micro, toks, width, hd, tangents = sizes
    streams = 1 + tangents
    rows = [
        state[pl.ds((s * micro + b) * toks, 16), :].astype(F32)[:1] for s in range(streams) for b in range(micro)
    ]
    return jnp.concatenate(rows + [jnp.zeros((group_of(sizes) - micro * streams, width), F32)], 0)


def last_norm(sizes, gain, state, normed):
    micro, toks, width, hd, tangents = sizes
    rows0 = micro * toks
    for b in range(micro):
        at = pl.ds(b * toks, toks)
        centred, inverse, y = norm_rows(state[at, :].astype(F32), gain)
        normed[0, at, :] = y.astype(BF16)
        for j in range(tangents):
            t = state[pl.ds((1 + j) * rows0 + b * toks, toks), :].astype(F32)
            normed[1 + j, at, :] = norm_tangent(t, centred, inverse, gain).astype(BF16)


def last_attend(sizes, u, normed):
    micro, toks, width, hd, tangents = sizes
    factor = HEAD ** (-0.5)
    shape = (u.shape[0], micro * toks)
    stream = stream_of(sizes, shape)
    image = (lax.broadcasted_iota(jnp.int32, shape, 0) % group_of(sizes)) % micro
    valid = lax.broadcasted_iota(jnp.int32, shape, 1) // toks == image
    parts = [dot_t(u, normed[s]) * factor for s in range(1 + tangents)]
    probs = softmax(jnp.where(valid, parts[0], -jnp.inf))
    weights = primal_rows(sizes, probs)
    scores = lowered(sizes, parts)
    dprobs = weights * (scores - jnp.sum(weights * scores, -1, keepdims=True))
    zero = jnp.zeros_like(weights)
    total = dot(jnp.where(stream == 0, weights, dprobs).astype(BF16), normed[0])
    for j in range(tangents):
        total = total + dot(jnp.where(stream == 1 + j, weights, zero).astype(BF16), normed[1 + j])
    return total.astype(BF16)


TOK, TOKY, TOKD, LA, LB, ATT, ATC, CLS, U, M, O1, O0, GAIN, FIRST, EARLY, STAGES = range(16)


def kernel(
    n, sizes, tokens, w_qkv, tangent_value, w_out, t_out, gain_in, final_in, head_in, logit_ref,
    a_stage, b_stage, a0, a1, b1, b_full, tok, normed_all, acc, att_out, att_in, state, normed,
    gains, final_gain, head, atc_out, atc_all, atc_in, cls_out, cls_in, cls_all, u_out, u_all, m_out, m_all, o_out, o_all, classes,
    loads, line, a_send, a_recv, stage_send, stage_recv, far_send, far_recv, b_send, b_recv,
):
    micro, toks, width, hd, tangents = sizes
    streams = 1 + tangents
    part = hd // 4
    share = part // HEAD
    g = Place(n)
    me, section, place, z, nz = g.me, g.section, g.place, g.z, g.nz
    other = 1 - section
    rows = width // n
    slab = 4 * rows
    group = group_of(sizes)
    own = at_rows(me, rows)

    barrier = pltpu.get_barrier_semaphore()

    def greet(target, sec):
        pl.semaphore_signal(
            barrier, inc=1, device_id={"section": sec, "dp": target}, device_id_type=MESH
        )

    pl.when(g.up)(lambda: greet(me + 4, section))
    pl.when(g.down)(lambda: greet(me - 4, section))
    for near in (g.diagonal, g.x_near, g.y_near):
        greet(near, section)
        greet(near, other)
    greet(me, other)

    def met():
        if nz > 1:
            middle = g.up & g.down
            pl.when(middle)(lambda: pl.semaphore_wait(barrier, 9))
            pl.when(jnp.logical_not(middle))(lambda: pl.semaphore_wait(barrier, 8))
        else:
            pl.semaphore_wait(barrier, 7)

    def column(p):
        return pl.ds(p * part, part) if isinstance(p, int) else at_rows(p, part)

    def load(i, src, dst):
        return pltpu.make_async_copy(src, dst, loads.at[i])

    def stage_loads():
        for p in range(4):
            for m in range(3):
                load(5, w_qkv.at[:, pl.ds(m * hd + p * part, part)], a_stage.at[p, :, pl.ds(m * part, part)]).start()
            for j in range(tangents):
                load(
                    5,
                    tangent_value.at[j, :, pl.ds(p * part, part)],
                    a_stage.at[p, :, pl.ds((3 + j) * part, part)],
                ).start()

    def own_loads():
        for m in range(3):
            load(6, w_qkv.at[:, column(m * 4 + place)], a1.at[own, pl.ds(m * part, part)]).start()
        for j in range(tangents):
            load(6, tangent_value.at[j, :, column(place)], a1.at[own, pl.ds((3 + j) * part, part)]).start()
        load(7, w_out.at[:, column(place)], b1.at[0, own, :]).start()
        load(7, t_out.at[:, :, column(place)], b1.at[pl.ds(1, tangents), own, :]).start()
        for p in range(4):
            load(8, w_out.at[:, pl.ds(p * part, part)], b_stage.at[p, 0]).start()
            load(8, t_out.at[:, :, pl.ds(p * part, part)], b_stage.at[p, pl.ds(1, tangents)]).start()

    def b_loads():
        load(4, w_out, b_full.at[0, own, :]).start()
        load(4, t_out, b_full.at[pl.ds(1, tangents), own, :]).start()

    def loaded(i, ref):
        load(i, ref, ref).wait()

    def gain_load():
        return load(0, gain_in, gains.at[section])

    def tok_load():
        return load(1, tokens, tok.at[place])

    def tail_loads():
        return [load(2, head_in, head), load(3, final_in, final_gain)]

    stage_loads()
    gain_load().start()
    tok_load().start()
    pl.when(section == 0)(b_loads)
    pl.when(section == 1)(own_loads)
    for move in tail_loads():
        move.start()
    met()

    def tell(way, level, target):
        pl.semaphore_signal(
            line.at[way, level], inc=1, device_id={"section": section, "dp": target}, device_id_type=MESH
        )

    if nz > 2:

        @pl.when(g.up & g.down)
        def _():
            tell(0, 1, me + 4)
            tell(1, 1, me - 4)

    def far_met():
        for level in range(1, nz - 1):

            @pl.when(z - 1 - level >= 0)
            def _():
                pl.semaphore_wait(line.at[0, level], 1)
                if level + 1 < nz - 1:
                    pl.when(g.up)(lambda: tell(0, level + 1, me + 4))

            @pl.when(z + 1 + level < nz)
            def _():
                pl.semaphore_wait(line.at[1, level], 1)
                if level + 1 < nz - 1:
                    pl.when(g.down)(lambda: tell(1, level + 1, me - 4))


    def xfer(stage, src, dst, target, sec):
        return pltpu.make_async_remote_copy(
            src_ref=src,
            dst_ref=dst,
            send_sem=stage_send.at[stage],
            recv_sem=stage_recv.at[stage],
            device_id={"section": sec, "dp": target},
            device_id_type=MESH,
        )

    def arrived(stage, ref):
        xfer(stage, ref, ref, me, other).wait_recv()

    sent = []

    FAR = (3, 1, 2, 0)

    def scatter(stage, src, dst, sec, total, skip_own=False):
        for i in FAR:
            if i > 0 or not skip_own:
                target = g.plane[i]
                xfer(stage, src(target % 4), dst, target, sec).start()
        sent.append((stage, total))

    def drain():
        for stage, ref in sent:
            xfer(stage, ref, ref, me, other).wait_send()
        sent.clear()

    def a_ref(src):
        return a0.at[at_rows(src, rows), :]

    def a_copy(src_ref, src, sem, target, sec):
        return pltpu.make_async_remote_copy(
            src_ref=src_ref,
            dst_ref=a_ref(src),
            send_sem=sem,
            recv_sem=a_recv.at[src],
            device_id={"section": sec, "dp": target},
            device_id_type=MESH,
        )

    @pl.when(section == 0)
    def _():
        loaded(5, a_stage)
        for i in range(4):
            target = g.plane[i]
            a_copy(a_stage.at[target % 4], me, stage_send.at[FIRST], target, other).start()
        sent.append((FIRST, a_stage))
        gain_load().wait()
        xfer(GAIN, gains.at[section], gains.at[section], me, other).start()
        sent.append((GAIN, gains.at[section]))
        loaded(4, b_full.at[:, own, :])
        gather = Gather(n, g, b_full, b_send, b_recv)
        lag = 2
        gather.along(False)
        for d in range(nz + lag):
            if d < nz:
                gather.pass_on(d)
                gather.direct(d)
                if d == 0:
                    far_met()
                    gather.along(True)
            if d >= lag:
                gather.relay(d - lag)
        tok_load().wait()
        gather.rest()
        arrived(ATC, atc_in)
        cls_out[...] = lowered(sizes, [dot_t(atc_in[...], b_full[s]) for s in range(streams)])
        xfer(CLS, cls_out, cls_in, me, other).start()
        sent.append((CLS, cls_out))
        arrived(ATT, att_in)
        first_out(sizes, tok, place, b_full, att_in, state)
        arrived(GAIN, gains.at[other])
        last_norm(sizes, gains[1], state, normed)
        arrived(U, u_all)
        u = jnp.concatenate([u_all[p] for p in range(4)], 0)
        m = last_attend(sizes, u, normed)
        for p in range(4):
            m_out[p] = m[p * share * group : (p + 1) * share * group]
        scatter(M, lambda p: m_out.at[p], m_all.at[place], other, m_out)
        classes[...] = class_rows(sizes, state)
        arrived(O0, o_all)
        drain()
        gather.drain()

    @pl.when(section == 1)
    def _():
        gain_load().wait()
        xfer(GAIN, gains.at[section], gains.at[section], me, other).start()
        sent.append((GAIN, gains.at[section]))
        tok_load().wait()

        def relay(d, some=g.plane):
            for shift, cond in g.sources(d):

                def step(shift=shift, d=d):
                    for near in some:
                        src = near + 4 * shift
                        a_copy(a_ref(src), src, a_send.at[d, 0], me, section).wait_recv()
                        if shift <= 0 and d < nz - 1:
                            pl.when(g.up)(
                                lambda: a_copy(a_ref(src), src, a_send.at[d, 0], me + 4, section).start()
                            )
                        if shift >= 0 and d < nz - 1:
                            pl.when(g.down)(
                                lambda: a_copy(a_ref(src), src, a_send.at[d, 1], me - 4, section).start()
                            )

                step() if cond is None else pl.when(cond)(step)

        def relay_end(d):
            slab_ref = a0.at[pl.ds(0, slab), :]
            for shift, cond in g.sources(d):

                def end(way):
                    pltpu.make_async_remote_copy(
                        src_ref=slab_ref,
                        dst_ref=slab_ref,
                        send_sem=a_send.at[d, way],
                        recv_sem=a_recv.at[0],
                        device_id={"section": section, "dp": me},
                        device_id_type=MESH,
                    ).wait_send()

                if shift <= 0:
                    pl.when(g.up if cond is None else cond & g.up)(functools.partial(end, 0))
                if shift >= 0:
                    pl.when(g.down if cond is None else cond & g.down)(functools.partial(end, 1))

        def project(d):
            for shift, cond in g.sources(d):

                def step(shift=shift):
                    at = at_rows(z + shift, slab)
                    term = dot(normed_all[:, at], a0[at, :])
                    acc[...] = term if d == 0 else acc[...] + term

                step() if cond is None else pl.when(cond)(step)

        loaded(7, b1.at[:, own, :])
        early = b1.at[:, pl.ds(0, (nz - 1) * rows), :]

        def ahead(k):
            for way in (k, -k):
                there = (z + way >= 0) & (z + way < nz)

                def go():
                    xfer(EARLY, b1.at[:, own, :], b1.at[:, own, :], me + 4 * way, section).start()

                pl.when(there)(go)

        if nz > 1:
            ahead(1)
        if nz > 1:
            sent.append((EARLY, early))
        relay(0, g.plane[:1])
        for stage, near in ((TOK, g.x_near), (TOKY, g.y_near)):
            xfer(stage, tok.at[place], tok.at[place], near, section).start()
            sent.append((stage, tok.at[place]))
        loaded(5, a_stage)
        loaded(6, a1.at[own, :])
        scatter(LA, lambda p: a_stage.at[p], a1.at[own, :], section, a_stage.at[pl.ds(0, 3)], True)
        far_met()
        for k in range(2, nz):
            ahead(k)
        relay(0, g.plane[1:])
        arrived(GAIN, gains.at[other])
        first_norm(sizes, tok, gains[0], normed_all, place)
        relay(1)
        half = micro * toks // 2
        for stage, near, target, first in ((TOK, g.x_near, g.y_near, 0), (TOKY, g.y_near, g.x_near, half)):
            arrived(stage, tok.at[near % 4])
            piece = tok.at[near % 4, pl.ds(first, half), :]
            xfer(TOKD, piece, piece, target, section).start()
        sent.append((TOKD, tok.at[0]))
        loaded(8, b_stage)
        scatter(LB, lambda p: b_stage.at[p], b1.at[:, own, :], section, b_stage.at[pl.ds(0, 3)], True)

        def far_refs(kind, zc):
            at = at_rows(zc, slab)
            if kind == 0:
                return [a1.at[at, pl.ds(0, 2 * part)]]
            if kind == 1:
                return [a1.at[at, pl.ds(2 * part, streams * part)]]
            return [b1.at[:, at_rows(near + 4 * (zc - z), rows), :] for near in g.plane[1:]]

        def far_total(kind):
            return far_refs(kind, 0)[0] if kind < 2 else b1.at[:, pl.ds(0, 3 * rows), :]

        def far_copy(ref, kind, zc, slot, target):
            return pltpu.make_async_remote_copy(
                src_ref=ref,
                dst_ref=ref,
                send_sem=far_send.at[kind, slot],
                recv_sem=far_recv.at[kind, zc],
                device_id={"section": section, "dp": target},
                device_id_type=MESH,
            )

        def far_moves(kind):
            for k in range(1, nz):
                for way in (k, -k):
                    there = z + way
                    when = (there >= 0) & (there < nz) if kind in (0,) else g.reaches(way)
                    yield when, None, z, there, me + 4 * way
            for k in () if kind in (0,) else range(1, nz - 2):
                for way in (k, -k):
                    yield g.passes(way), way, z + way, nz + k, me - 4 if way > 0 else me + 4

        def far_start(kind):
            for when, way, zc, slot, target in far_moves(kind):

                def go():
                    for ref in far_refs(kind, zc):
                        far_copy(ref, kind, zc, slot, target).start()

                if way is None:
                    pl.when(when)(go)

        def far_pass(kind):
            for when, way, zc, slot, target in far_moves(kind):

                def step():
                    far_copy(far_total(kind), kind, zc, 0, me).wait_recv()
                    for ref in far_refs(kind, zc):
                        far_copy(ref, kind, zc, slot, target).start()

                if way is not None:
                    pl.when(when)(step)

        def far_wait(kind):
            for k in range(1, nz):
                for way in (k, -k):
                    there = z + way
                    when = (there >= 0) & (there < nz)
                    if kind not in (0,) and g.passes(way) is not None:
                        when = when & jnp.logical_not(g.passes(way))
                    pl.when(when)(lambda: far_copy(far_total(kind), kind, there, 0, me).wait_recv())

        def far_end(kind):
            for when, way, zc, slot, target in far_moves(kind):
                pl.when(when)(lambda: far_copy(far_total(kind), kind, zc, slot, target).wait_send())

        def far_begin():
            arrived(LA, a1.at[pl.ds(0, 3 * rows), :])
            far_start(0)
            far_start(1)

        for near in (g.x_near, g.y_near):
            first_norm(sizes, tok, gains[0], normed_all, near % 4)
        for d in range(2, nz - 1):
            relay(d)
        far_begin()
        arrived(TOKD, tok.at[g.diagonal % 4])
        first_norm(sizes, tok, gains[0], normed_all, g.diagonal % 4)
        for d in range(nz - 1):
            project(d)
        if nz > 2:
            relay(nz - 1)
        project(nz - 1)
        def give(i):
            target = g.plane[i]
            xfer(ATT, att_out.at[target % 4], att_in.at[:, column(place)], target, other).start()

        for i in FAR:
            for b in range(micro):
                first_attend(sizes, acc, att_out, g.plane[i] % 4, b)
            if i == FAR[1]:
                arrived(LB, b1.at[:, pl.ds(0, 3 * rows), :])
                far_start(2)
        firsts = []
        for p in range(4):
            for i in range(group):
                at = pl.ds(i * toks, 16) if i < streams * micro else pl.ds(0, 16)
                firsts.append(att_out[p, at, :].astype(F32)[:1])
        atc_out[...] = jnp.concatenate(firsts, 0).astype(BF16)
        scatter(ATC, lambda p: atc_out, atc_in.at[:, column(place)], other, atc_all)
        for i in FAR:
            give(i)
        sent.append((ATT, att_out))
        fresh = []
        blank = jnp.zeros((group - micro, width), F32)
        for p in range(4):
            fresh += [tok[p, pl.ds(b * toks, 16), :].astype(F32)[:1] for b in range(micro)] + [blank]
        fresh = jnp.concatenate(fresh, 0)
        far_wait(0)
        arrived(CLS, cls_in)
        x = (fresh + cls_in[...]).astype(BF16).astype(F32)
        for p in range(4):
            cls_all[p] = x[p * group : (p + 1) * group]
        q = dot(norm_group(sizes, x, gains[1]), a1[:, pl.ds(0, part)]).astype(BF16).astype(F32)
        owner = lax.broadcasted_iota(jnp.int32, (group, part), 1) // HEAD
        zero = jnp.zeros((group, part), F32)
        spread = [
            jnp.where(owner == h, q[p * group : (p + 1) * group], zero) for p in range(4) for h in range(share)
        ]
        u = dot_t(jnp.concatenate(spread, 0).astype(BF16), a1[:, pl.ds(part, part)]).astype(BF16)
        tall = share * group
        for p in range(4):
            u_out[p] = u[p * tall : (p + 1) * tall]
        scatter(U, lambda p: u_out.at[p], u_all.at[place], other, u_out)
        far_pass(1)
        far_pass(2)
        far_wait(1)
        arrived(M, m_all)
        m = jnp.concatenate([m_all[p] for p in range(4)], 0)
        r = dot(m, a1[:, pl.ds(2 * part, streams * part)])
        mixed = lowered(sizes, [r[:, s * part : (s + 1) * part] for s in range(streams)])
        chosen = []
        for p in range(4):
            block = zero
            for h in range(share):
                at = p * tall + h * group
                block = jnp.where(owner == h, mixed[at : at + group], block)
            chosen.append(block)
        attended = jnp.concatenate(chosen, 0).astype(BF16)
        far_wait(2)
        if nz > 1:
            arrived(EARLY, early)
        out = lowered(sizes, [dot_t(attended, b1[s]) for s in range(streams)])
        for p in range(4):
            o_out[p] = out[p * group : (p + 1) * group].astype(BF16)
        scatter(O1, lambda p: o_out.at[p], o_all.at[place], section, o_out.at[pl.ds(0, 3)], True)
        scatter(O0, lambda p: o_out.at[p], o_all.at[place], other, o_out)
        o_all[place] = o_out[place]
        classes[...] = cls_all[place]
        arrived(O1, o_all.at[pl.ds(0, 3)])
        drain()
        for d in range(nz - 1):
            relay_end(d)
        for kind in range(3):
            far_end(kind)

    for move in tail_loads():
        move.wait()
    total = sum(o_all[p].astype(F32) for p in range(4))
    final = (classes[...] + total).astype(BF16).astype(F32)
    features = norm_group(sizes, final, final_gain[...])
    logits = dot_t(features, head[...])
    for s in range(streams):
        logit_ref[s, :, 0, :] = logits[s * micro : (s + 1) * micro]


def two_sections(n):
    def shards(tokens, w_qkv, w_output, tangent_value, tangent_output, layer_gain, final_gain, head):
        micro, _, toks, width = tokens.shape
        tangents = tangent_value.shape[1]
        hd = w_output.shape[1]
        count = head.shape[1]
        rows = width // n
        part = hd // 4
        nz = n // 4
        sizes = (micro, toks, width, hd, tangents)
        streams = 1 + tangents
        rows0 = micro * toks
        group = group_of(sizes)
        tall = part // HEAD * group
        vmem = pl.BlockSpec(memory_space=pltpu.VMEM)
        anywhere = pl.BlockSpec(memory_space=pl.ANY)
        dma = pltpu.SemaphoreType.DMA
        logits = pl.pallas_call(
            functools.partial(kernel, n, sizes),
            out_shape=pltpu.VMEM((streams, micro, 1, count), F32),
            in_specs=[anywhere] * 8,
            out_specs=vmem,
            scratch_shapes=[
                pltpu.VMEM((4, rows, (2 + streams) * part), BF16),
                pltpu.VMEM((4, streams, rows, part), BF16),
                pltpu.VMEM((width, (2 + streams) * part), BF16),
                pltpu.VMEM((width, (2 + streams) * part), BF16),
                pltpu.VMEM((streams, width, part), BF16),
                pltpu.VMEM((streams, width, hd), BF16),
                pltpu.VMEM((4, rows0, width), BF16),
                pltpu.VMEM((4 * rows0, width), BF16),
                pltpu.VMEM((4 * rows0, (2 + streams) * part), F32),
                pltpu.VMEM((4, streams * rows0, part), BF16),
                pltpu.VMEM((streams * rows0, hd), BF16),
                pltpu.VMEM((streams * rows0, width), BF16),
                pltpu.VMEM((streams, rows0, width), BF16),
                pltpu.VMEM((2, 1, width), F32),
                pltpu.VMEM((1, width), F32),
                pltpu.VMEM((count, width), BF16),
                pltpu.VMEM((4 * group, part), BF16),
                pltpu.VMEM((16 * group, part), BF16),
                pltpu.VMEM((4 * group, hd), BF16),
                pltpu.VMEM((4 * group, width), F32),
                pltpu.VMEM((4 * group, width), F32),
                pltpu.VMEM((4, group, width), F32),
                pltpu.VMEM((4, tall, width), BF16),
                pltpu.VMEM((4, tall, width), BF16),
                pltpu.VMEM((4, tall, width), BF16),
                pltpu.VMEM((4, tall, width), BF16),
                pltpu.VMEM((4, group, width), BF16),
                pltpu.VMEM((4, group, width), BF16),
                pltpu.VMEM((group, width), F32),
                dma((9,)),
                pltpu.SemaphoreType.REGULAR((2, max(nz - 1, 1))),
                dma((nz, 2)),
                dma((n,)),
                dma((STAGES,)),
                dma((STAGES,)),
                dma((3, 2 * nz)),
                dma((3, nz)),
                dma((4 * nz,)),
                dma((n, 2)),
            ],
            compiler_params=pltpu.CompilerParams(
                collective_id=0, has_side_effects=True, vmem_limit_bytes=63 * 2**20
            ),
        )(
            tokens.reshape(rows0, width),
            w_qkv[0],
            tangent_value[0],
            jnp.swapaxes(w_output[0], 0, 1),
            jnp.swapaxes(tangent_output[0], 1, 2),
            layer_gain,
            final_gain[None],
            head.T,
        )
        return logits[0], sum(logits[1 + j] * logits[1 + j] for j in range(tangents))

    return shards


def solution(mesh):
    n = mesh.shape["dp"]
    fast = mesh.shape["section"] == 2 and n % 4 == 0
    return jax.shard_map(
        two_sections(n) if fast else relay_shards,
        mesh=mesh,
        in_specs=(
            P(None, "dp", None, None),
            P("section", "dp", None),
            P("section", None, "dp"),
            P("section", None, "dp", None),
            P("section", None, None, "dp"),
            P("section", None),
            P(),
            P(None, "section"),
        ),
        out_specs=(P(None, "dp", "section"), P(None, "dp", "section")),
        check_vma=False,
    )
```

```python
import functools

import jax
import jax.numpy as jnp
from jax import lax
from jax.experimental import pallas as pl
from jax.experimental.pallas import tpu as pltpu
from jax.sharding import PartitionSpec as P

HEAD = 64
epsilon = 1e-06
F32, BF16 = jnp.float32, jnp.bfloat16
MESH = pl.DeviceIdType.MESH


def contract(spec, left, right):
    return jnp.einsum(spec, left, right, preferred_element_type=jnp.float32)


def norm_jvp(primal, tangents, gains):
    average = jnp.mean(primal, -1, keepdims=True)
    centred = primal - average
    inverse = lax.rsqrt(jnp.mean(centred * centred, -1, keepdims=True) + epsilon)
    dcentred = tangents - jnp.mean(tangents, -1, keepdims=True)
    dinverse = -(inverse**3) * jnp.mean(centred * dcentred, -1, keepdims=True)
    return (centred * inverse * gains, (dcentred * inverse + centred * dinverse) * gains)


def layer_step(state, qkv_weight, out_weight, value_tangent, out_tangent, gains):
    hd = out_weight.shape[0]
    heads = hd // HEAD
    resid = state.astype(F32)
    normed_zero, normed_rest = norm_jvp(resid[0], resid[1:], gains)
    normed = jnp.concatenate([normed_zero[None], normed_rest]).astype(BF16)
    streams, batch, tokens_here, width = normed.shape
    projected = contract("sbtd,de->sbte", normed, qkv_weight)
    extra_value = contract("btd,kde->kbte", normed[0], value_tangent)
    queries = projected[..., :hd]
    key_rows = projected[..., hd : 2 * hd]
    values = projected[..., 2 * hd :]
    values = jnp.concatenate([values[:1], values[1:] + extra_value])
    shape_heads = (streams, batch, tokens_here, heads, HEAD)
    queries = queries.astype(BF16).reshape(shape_heads)
    key_rows = key_rows.astype(BF16).reshape(shape_heads)
    values = values.astype(BF16).reshape(shape_heads)
    factor = HEAD ** (-0.5)
    scores = contract("bqhe,bkhe->bhqk", queries[0], key_rows[0]) * factor
    probs = jax.nn.softmax(scores, -1)
    dscores = (
        contract("sbqhe,bkhe->sbhqk", queries[1:], key_rows[0])
        + contract("bqhe,sbkhe->sbhqk", queries[0], key_rows[1:])
    ) * factor
    dprobs = probs * (dscores - jnp.sum(probs * dscores, -1, keepdims=True))
    probs_low = probs.astype(BF16)
    dprobs_low = dprobs.astype(BF16)
    attended_zero = contract("bhqk,bkhe->bqhe", probs_low, values[0])
    attended_rest = contract("sbhqk,bkhe->sbqhe", dprobs_low, values[0]) + contract(
        "bhqk,sbkhe->sbqhe", probs_low, values[1:]
    )
    attended = jnp.concatenate([attended_zero[None], attended_rest]).astype(BF16)
    attended = attended.reshape(streams, batch, tokens_here, hd)
    output = contract("sbte,ed->sbtd", attended, out_weight)
    extra_out = contract("bte,ked->kbtd", attended[0], out_tangent)
    output = jnp.concatenate([output[:1], output[1:] + extra_out])
    return (resid + output).astype(BF16)


def relay_shards(tokens, w_qkv, w_output, tangent_value, tangent_output, layer_gain, final_gain, head):
    full_qkv, full_output, full_value_tan, full_output_tan = (
        lax.all_gather(w_qkv, "dp", axis=1, tiled=True),
        lax.all_gather(w_output, "dp", axis=2, tiled=True),
        lax.all_gather(tangent_value, "dp", axis=2, tiled=True),
        lax.all_gather(tangent_output, "dp", axis=3, tiled=True),
    )
    tangents = tangent_value.shape[1]

    def advance_layer(state):
        return layer_step(
            state, full_qkv[0], full_output[0], full_value_tan[0], full_output_tan[0], layer_gain[0]
        )

    section_index = lax.axis_index("section")
    section_count = lax.axis_size("section")
    route = [(i, i + 1) for i in range(section_count - 1)]
    micro, _, toks, width = tokens.shape
    entering = jnp.concatenate(
        [tokens.reshape(1, micro, toks, width), jnp.zeros((tangents, micro, toks, width), BF16)]
    )

    def advance(step, outgoing):
        incoming = lax.ppermute(outgoing, "section", route)
        source = jnp.where(step == 0, entering, incoming)
        return lax.cond(section_index == step, advance_layer, jnp.zeros_like, source)

    finished = lax.fori_loop(0, section_count, advance, jnp.zeros_like(entering))
    collected = finished[:, :, 0, :]
    mine = section_index == section_count - 1
    features = lax.psum(jnp.where(mine, collected, jnp.zeros_like(collected)), "section")
    widened = features.astype(F32)
    final_zero, final_rest = norm_jvp(widened[0], widened[1:], final_gain)
    normed_final = jnp.concatenate([final_zero[None], final_rest]).astype(BF16)
    logits = contract("sbd,dc->sbc", normed_final, head)
    return (logits[0][:, None, :], jnp.sum(logits[1:] * logits[1:], 0)[:, None, :])


def dot(a, b):
    return lax.dot_general(a, b, (((1,), (0,)), ((), ())), preferred_element_type=F32)


def dot_t(a, b):
    return lax.dot_general(a, b, (((1,), (1,)), ((), ())), preferred_element_type=F32)


class Gather:
    def __init__(self, n, g, full, send, recv):
        self.nz = n // 4
        self.full, self.send, self.recv = full, send, recv
        self.rows = full.shape[1] // n
        self.g = g
        self.ends = []

    def span(self, start, count):
        return self.full.at[:, pl.ds(pl.multiple_of(start, self.rows // 2), count), :]

    def remote(self, ref, target, sem, recv):
        return pltpu.make_async_remote_copy(
            src_ref=ref,
            dst_ref=ref,
            send_sem=self.send.at[sem],
            recv_sem=recv,
            device_id={"section": self.g.section, "dp": target},
            device_id_type=MESH,
        )

    def copy(self, src, half, target, sem):
        depth = self.rows // 2
        ref = self.span(src * self.rows + half * depth, depth)
        return self.remote(ref, target, sem, self.recv.at[src, half])

    def forward(self, cond, src, half, target, sem):
        def go():
            self.copy(src, half, target, sem).start()

        go() if cond is None else pl.when(cond)(go)

    def ended(self, cond, pieces, sem):
        def end():
            self.remote(self.span(0, pieces * self.rows), self.g.me, sem, self.recv.at[0, 0]).wait_send()

        self.ends.append((cond, end))

    def arrived(self, src, half):
        self.copy(src, half, self.g.me, 0).wait_recv()

    def along(self, far):
        g, nz = self.g, self.nz
        for k in range(2, nz) if far else range(1, min(nz, 2)):
            for way in (k, -k):
                when = g.reaches(way)
                for half in range(2):
                    self.forward(when, g.me, half, g.me + 4 * way, g.z + way)
                self.ended(when, 1, g.z + way)

    def pass_on(self, d):
        g = self.g
        for shift, cond in g.sources(d):
            passed = g.passes(shift)
            if passed is not None:
                src = g.me + 4 * shift
                for half in range(2):
                    pl.when(passed)(functools.partial(self.arrived, src, half))
                    self.forward(passed, src, half, g.me - 4 if shift > 0 else g.me + 4, self.nz + d)
                self.ended(passed, 1, self.nz + d)

    def direct(self, d):
        g = self.g
        for side, (shift, cond) in enumerate(g.sources(d)):
            src = g.me + 4 * shift
            passed = g.passes(shift)
            for half in range(2):
                if d > 0:
                    fresh = cond if passed is None else cond & jnp.logical_not(passed)
                    pl.when(fresh)(functools.partial(self.arrived, src, half))
                for target in ((g.y_near, g.x_near), (g.x_near, g.y_near))[half]:
                    self.forward(cond, src, half, target, 2 * self.nz + 2 * d + side)
            self.ended(cond, 3, 2 * self.nz + 2 * d + side)

    def relay(self, d):
        g = self.g
        for side, (shift, cond) in enumerate(g.sources(d)):
            for half, near, target in ((0, g.x_near, g.y_near), (1, g.y_near, g.x_near)):
                src = near + 4 * shift
                wait = functools.partial(self.arrived, src, half)
                wait() if cond is None else pl.when(cond)(wait)
                self.forward(cond, src, half, target, 2 * self.nz + 2 * d + side)

    def rest(self):
        g = self.g
        for z in range(self.nz):
            up = 4 * (z - g.z)
            self.arrived(g.x_near + up, 1)
            self.arrived(g.y_near + up, 0)
            self.arrived(g.diagonal + up, 0)
            self.arrived(g.diagonal + up, 1)

    def drain(self):
        for cond, end in self.ends:
            end() if cond is None else pl.when(cond)(end)


class Place:
    def __init__(self, n):
        self.nz = n // 4
        self.me = lax.axis_index("dp")
        self.section = lax.axis_index("section")
        me = self.me
        self.x_near = me + 1 - 2 * (me % 2)
        self.y_near = me + 2 - 4 * ((me // 2) % 2)
        self.diagonal = self.x_near + self.y_near - me
        self.z = me // 4
        self.place = me % 4
        self.up, self.down = self.z + 1 < self.nz, self.z >= 1
        self.plane = (me, self.x_near, self.y_near, self.diagonal)

    def sources(self, d):
        if d == 0:
            return [(0, None)]
        return [(-d, self.z >= d), (d, self.z + d < self.nz)]

    def reaches(self, way):
        z, nz = self.z, self.nz
        there = z + way
        when = (there >= 0) & (there < nz)
        if abs(way) > 1:
            when = when & ((z == 0) | (z == nz - 1) | ((there > 0) & (there < nz - 1)))
        return when

    def passes(self, shift):
        z, nz = self.z, self.nz
        if not 0 < abs(shift) < nz - 2:
            return None
        return (z == 1) & (z + shift < nz - 1) if shift > 0 else (z == nz - 2) & (z + shift > 0)


def norm_rows(x, gains):
    average = jnp.mean(x, -1, keepdims=True)
    centred = x - average
    inverse = lax.rsqrt(jnp.mean(centred * centred, -1, keepdims=True) + epsilon)
    return centred, inverse, centred * inverse * gains


def norm_tangent(t, centred, inverse, gains):
    dcentred = t - jnp.mean(t, -1, keepdims=True)
    dinverse = -(inverse * inverse * inverse) * jnp.mean(centred * dcentred, -1, keepdims=True)
    return (dcentred * inverse + centred * dinverse) * gains


def softmax(scores):
    e = jnp.exp(scores - jnp.max(scores, -1, keepdims=True))
    return e / jnp.sum(e, -1, keepdims=True)


def at_rows(i, count):
    return pl.ds(pl.multiple_of(i * count, count), count)


def first_norm(sizes, tok, gain, normed, slot):
    micro, toks, width, hd, tangents = sizes
    for b in range(micro):
        x = tok[slot, pl.ds(b * toks, toks), :].astype(F32)
        normed[at_rows(slot * micro + b, toks), :] = norm_rows(x, gain)[2].astype(BF16)


def first_attend(sizes, acc, att, slot, b):
    micro, toks, width, hd, tangents = sizes
    factor = HEAD ** (-0.5)
    part = 2 * HEAD
    streams = 1 + tangents
    even = lax.broadcasted_iota(jnp.int32, (toks, part), 1) < HEAD
    rows = at_rows(slot * micro + b, toks)
    q = acc[rows, pl.ds(0, part)]
    k = acc[rows, pl.ds(part, part)].astype(BF16)
    v = acc[rows, pl.ds(2 * part, streams * part)].astype(BF16)
    zero = jnp.zeros_like(q)
    both = jnp.concatenate([jnp.where(even, q, zero), jnp.where(even, zero, q)], 0).astype(BF16)
    scores = dot_t(both, k) * factor
    low = jnp.exp(scores - jnp.max(scores, -1, keepdims=True)).astype(BF16)
    out = dot(low, jnp.concatenate([v, jnp.ones((toks, part), BF16)], 1))

    def joined(s):
        at = slice(s * part, (s + 1) * part)
        return jnp.where(even, out[:toks, at], out[toks:, at])

    scale = 1.0 / joined(streams)
    for s in range(streams):
        att[slot, pl.ds((s * micro + b) * toks, toks), :] = (joined(s) * scale).astype(BF16)


def first_out(sizes, tok, place, b_full, att, state):
    micro, toks, width, hd, tangents = sizes
    rows0 = micro * toks
    tile = 256
    for c in range(width // tile):
        at = pl.ds(c * tile, tile)
        out = dot_t(att[...], b_full[0, at, :])
        extra = [dot_t(att[pl.ds(0, rows0), :], b_full[1 + j, at, :]) for j in range(tangents)]
        x = tok[place, :, at].astype(F32)
        state[pl.ds(0, rows0), at] = (x + out[:rows0]).astype(BF16)
        for j in range(tangents):
            state[pl.ds((1 + j) * rows0, rows0), at] = (
                out[(1 + j) * rows0 : (2 + j) * rows0] + extra[j]
            ).astype(BF16)


def group_of(sizes):
    micro, toks, width, hd, tangents = sizes
    return -(-micro * (1 + tangents) // 8) * 8


def stream_of(sizes, shape):
    return (lax.broadcasted_iota(jnp.int32, shape, 0) % group_of(sizes)) // sizes[0]


def lowered(sizes, parts):
    micro, tangents = sizes[0], sizes[4]
    stream = stream_of(sizes, parts[0].shape)
    total = parts[0]
    for j in range(tangents):
        moved = pltpu.roll(parts[1 + j], micro * (1 + j), 0)
        total = total + jnp.where(stream == 1 + j, moved, jnp.zeros_like(moved))
    return total


def primal_rows(sizes, x):
    micro, tangents = sizes[0], sizes[4]
    stream = stream_of(sizes, x.shape)
    spread = x
    for j in range(tangents):
        spread = jnp.where(stream == 1 + j, pltpu.roll(x, micro * (1 + j), 0), spread)
    return spread


def norm_group(sizes, x, gains):
    stream = stream_of(sizes, x.shape)
    centred, inverse, y = norm_rows(primal_rows(sizes, x), gains)
    dy = norm_tangent(x, centred, inverse, gains)
    return jnp.where(stream == 0, y, dy).astype(BF16)


def class_rows(sizes, state):
    micro, toks, width, hd, tangents = sizes
    streams = 1 + tangents
    rows = [
        state[pl.ds((s * micro + b) * toks, 16), :].astype(F32)[:1] for s in range(streams) for b in range(micro)
    ]
    return jnp.concatenate(rows + [jnp.zeros((group_of(sizes) - micro * streams, width), F32)], 0)


def last_norm(sizes, gain, state, normed):
    micro, toks, width, hd, tangents = sizes
    rows0 = micro * toks
    for b in range(micro):
        at = pl.ds(b * toks, toks)
        centred, inverse, y = norm_rows(state[at, :].astype(F32), gain)
        normed[0, at, :] = y.astype(BF16)
        for j in range(tangents):
            t = state[pl.ds((1 + j) * rows0 + b * toks, toks), :].astype(F32)
            normed[1 + j, at, :] = norm_tangent(t, centred, inverse, gain).astype(BF16)


def last_attend(sizes, u, normed):
    micro, toks, width, hd, tangents = sizes
    factor = HEAD ** (-0.5)
    shape = (u.shape[0], micro * toks)
    stream = stream_of(sizes, shape)
    image = (lax.broadcasted_iota(jnp.int32, shape, 0) % group_of(sizes)) % micro
    valid = lax.broadcasted_iota(jnp.int32, shape, 1) // toks == image
    parts = [dot_t(u, normed[s]) * factor for s in range(1 + tangents)]
    probs = softmax(jnp.where(valid, parts[0], -jnp.inf))
    weights = primal_rows(sizes, probs)
    scores = lowered(sizes, parts)
    dprobs = weights * (scores - jnp.sum(weights * scores, -1, keepdims=True))
    zero = jnp.zeros_like(weights)
    total = dot(jnp.where(stream == 0, weights, dprobs).astype(BF16), normed[0])
    for j in range(tangents):
        total = total + dot(jnp.where(stream == 1 + j, weights, zero).astype(BF16), normed[1 + j])
    return total.astype(BF16)


TOK, TOKY, TOKD, LA, LB, ATT, ATC, CLS, U, M, O1, O0, GAIN, FIRST, EARLY, STAGES = range(16)


def kernel(
    n, sizes, tokens, w_qkv, tangent_value, w_out, t_out, gain_in, final_in, head_in, logit_ref,
    a_stage, b_stage, a0, a1, b1, b_full, tok, normed_all, acc, att_out, att_in, state, normed,
    gains, final_gain, head, atc_out, atc_all, atc_in, cls_out, cls_in, cls_all, u_out, u_all, m_out, m_all, o_out, o_all, classes,
    loads, line, a_send, a_recv, stage_send, stage_recv, far_send, far_recv, b_send, b_recv,
):
    micro, toks, width, hd, tangents = sizes
    streams = 1 + tangents
    part = hd // 4
    share = part // HEAD
    g = Place(n)
    me, section, place, z, nz = g.me, g.section, g.place, g.z, g.nz
    other = 1 - section
    rows = width // n
    slab = 4 * rows
    group = group_of(sizes)
    own = at_rows(me, rows)

    barrier = pltpu.get_barrier_semaphore()

    def greet(target, sec):
        pl.semaphore_signal(
            barrier, inc=1, device_id={"section": sec, "dp": target}, device_id_type=MESH
        )

    pl.when(g.up)(lambda: greet(me + 4, section))
    pl.when(g.down)(lambda: greet(me - 4, section))
    for near in (g.diagonal, g.x_near, g.y_near):
        greet(near, section)
        greet(near, other)
    greet(me, other)

    def met():
        if nz > 1:
            middle = g.up & g.down
            pl.when(middle)(lambda: pl.semaphore_wait(barrier, 9))
            pl.when(jnp.logical_not(middle))(lambda: pl.semaphore_wait(barrier, 8))
        else:
            pl.semaphore_wait(barrier, 7)

    def column(p):
        return pl.ds(p * part, part) if isinstance(p, int) else at_rows(p, part)

    def load(i, src, dst):
        return pltpu.make_async_copy(src, dst, loads.at[i])

    def stage_loads():
        for p in range(4):
            for m in range(3):
                load(5, w_qkv.at[:, pl.ds(m * hd + p * part, part)], a_stage.at[p, :, pl.ds(m * part, part)]).start()
            for j in range(tangents):
                load(
                    5,
                    tangent_value.at[j, :, pl.ds(p * part, part)],
                    a_stage.at[p, :, pl.ds((3 + j) * part, part)],
                ).start()

    def own_loads():
        for m in range(3):
            load(6, w_qkv.at[:, column(m * 4 + place)], a1.at[own, pl.ds(m * part, part)]).start()
        for j in range(tangents):
            load(6, tangent_value.at[j, :, column(place)], a1.at[own, pl.ds((3 + j) * part, part)]).start()
        load(7, w_out.at[:, column(place)], b1.at[0, own, :]).start()
        load(7, t_out.at[:, :, column(place)], b1.at[pl.ds(1, tangents), own, :]).start()
        for p in range(4):
            load(8, w_out.at[:, pl.ds(p * part, part)], b_stage.at[p, 0]).start()
            load(8, t_out.at[:, :, pl.ds(p * part, part)], b_stage.at[p, pl.ds(1, tangents)]).start()

    def b_loads():
        load(4, w_out, b_full.at[0, own, :]).start()
        load(4, t_out, b_full.at[pl.ds(1, tangents), own, :]).start()

    def loaded(i, ref):
        load(i, ref, ref).wait()

    def gain_load():
        return load(0, gain_in, gains.at[section])

    def tok_load():
        return load(1, tokens, tok.at[place])

    def tail_loads():
        return [load(2, head_in, head), load(3, final_in, final_gain)]

    stage_loads()
    gain_load().start()
    tok_load().start()
    pl.when(section == 0)(b_loads)
    pl.when(section == 1)(own_loads)
    for move in tail_loads():
        move.start()
    met()

    def tell(way, level, target):
        pl.semaphore_signal(
            line.at[way, level], inc=1, device_id={"section": section, "dp": target}, device_id_type=MESH
        )

    if nz > 2:

        @pl.when(g.up & g.down)
        def _():
            tell(0, 1, me + 4)
            tell(1, 1, me - 4)

    def far_met():
        for level in range(1, nz - 1):

            @pl.when(z - 1 - level >= 0)
            def _():
                pl.semaphore_wait(line.at[0, level], 1)
                if level + 1 < nz - 1:
                    pl.when(g.up)(lambda: tell(0, level + 1, me + 4))

            @pl.when(z + 1 + level < nz)
            def _():
                pl.semaphore_wait(line.at[1, level], 1)
                if level + 1 < nz - 1:
                    pl.when(g.down)(lambda: tell(1, level + 1, me - 4))


    def xfer(stage, src, dst, target, sec):
        return pltpu.make_async_remote_copy(
            src_ref=src,
            dst_ref=dst,
            send_sem=stage_send.at[stage],
            recv_sem=stage_recv.at[stage],
            device_id={"section": sec, "dp": target},
            device_id_type=MESH,
        )

    def arrived(stage, ref):
        xfer(stage, ref, ref, me, other).wait_recv()

    sent = []

    FAR = (3, 1, 2, 0)

    def scatter(stage, src, dst, sec, total, skip_own=False):
        for i in FAR:
            if i > 0 or not skip_own:
                target = g.plane[i]
                xfer(stage, src(target % 4), dst, target, sec).start()
        sent.append((stage, total))

    def drain():
        for stage, ref in sent:
            xfer(stage, ref, ref, me, other).wait_send()
        sent.clear()

    def a_ref(src):
        return a0.at[at_rows(src, rows), :]

    def a_copy(src_ref, src, sem, target, sec):
        return pltpu.make_async_remote_copy(
            src_ref=src_ref,
            dst_ref=a_ref(src),
            send_sem=sem,
            recv_sem=a_recv.at[src],
            device_id={"section": sec, "dp": target},
            device_id_type=MESH,
        )

    @pl.when(section == 0)
    def _():
        loaded(5, a_stage)
        for i in range(4):
            target = g.plane[i]
            a_copy(a_stage.at[target % 4], me, stage_send.at[FIRST], target, other).start()
        sent.append((FIRST, a_stage))
        gain_load().wait()
        xfer(GAIN, gains.at[section], gains.at[section], me, other).start()
        sent.append((GAIN, gains.at[section]))
        loaded(4, b_full.at[:, own, :])
        gather = Gather(n, g, b_full, b_send, b_recv)
        lag = 2
        gather.along(False)
        for d in range(nz + lag):
            if d < nz:
                gather.pass_on(d)
                gather.direct(d)
                if d == 0:
                    far_met()
                    gather.along(True)
            if d >= lag:
                gather.relay(d - lag)
        tok_load().wait()
        gather.rest()
        arrived(ATC, atc_in)
        cls_out[...] = lowered(sizes, [dot_t(atc_in[...], b_full[s]) for s in range(streams)])
        xfer(CLS, cls_out, cls_in, me, other).start()
        sent.append((CLS, cls_out))
        arrived(ATT, att_in)
        first_out(sizes, tok, place, b_full, att_in, state)
        arrived(GAIN, gains.at[other])
        last_norm(sizes, gains[1], state, normed)
        arrived(U, u_all)
        u = jnp.concatenate([u_all[p] for p in range(4)], 0)
        m = last_attend(sizes, u, normed)
        for p in range(4):
            m_out[p] = m[p * share * group : (p + 1) * share * group]
        scatter(M, lambda p: m_out.at[p], m_all.at[place], other, m_out)
        classes[...] = class_rows(sizes, state)
        arrived(O0, o_all)
        drain()
        gather.drain()

    @pl.when(section == 1)
    def _():
        gain_load().wait()
        xfer(GAIN, gains.at[section], gains.at[section], me, other).start()
        sent.append((GAIN, gains.at[section]))
        tok_load().wait()

        def relay(d, some=g.plane):
            for near in some:
                for shift, cond in g.sources(d)[::-1]:

                    def step():
                        src = near + 4 * shift
                        a_copy(a_ref(src), src, a_send.at[d, 0], me, section).wait_recv()
                        if shift >= 0 and d < nz - 1:
                            pl.when(g.down)(
                                lambda: a_copy(a_ref(src), src, a_send.at[d, 1], me - 4, section).start()
                            )
                        if shift <= 0 and d < nz - 1:
                            pl.when(g.up)(
                                lambda: a_copy(a_ref(src), src, a_send.at[d, 0], me + 4, section).start()
                            )

                    step() if cond is None else pl.when(cond)(step)

        def relay_end(d):
            slab_ref = a0.at[pl.ds(0, slab), :]
            for shift, cond in g.sources(d):

                def end(way):
                    pltpu.make_async_remote_copy(
                        src_ref=slab_ref,
                        dst_ref=slab_ref,
                        send_sem=a_send.at[d, way],
                        recv_sem=a_recv.at[0],
                        device_id={"section": section, "dp": me},
                        device_id_type=MESH,
                    ).wait_send()

                if shift <= 0:
                    pl.when(g.up if cond is None else cond & g.up)(functools.partial(end, 0))
                if shift >= 0:
                    pl.when(g.down if cond is None else cond & g.down)(functools.partial(end, 1))

        def project(d):
            for shift, cond in g.sources(d):

                def step(shift=shift):
                    at = at_rows(z + shift, slab)
                    term = dot(normed_all[:, at], a0[at, :])
                    acc[...] = term if d == 0 else acc[...] + term

                step() if cond is None else pl.when(cond)(step)

        loaded(7, b1.at[:, own, :])
        early = b1.at[:, pl.ds(0, (nz - 1) * rows), :]

        def ahead(k):
            for way in (k, -k):
                there = (z + way >= 0) & (z + way < nz)

                def go():
                    xfer(EARLY, b1.at[:, own, :], b1.at[:, own, :], me + 4 * way, section).start()

                pl.when(there)(go)

        if nz > 1:
            ahead(1)
        if nz > 1:
            sent.append((EARLY, early))
        relay(0, g.plane[:1])
        for stage, near in ((TOK, g.x_near), (TOKY, g.y_near)):
            xfer(stage, tok.at[place], tok.at[place], near, section).start()
            sent.append((stage, tok.at[place]))
        loaded(5, a_stage)
        loaded(6, a1.at[own, :])
        scatter(LA, lambda p: a_stage.at[p], a1.at[own, :], section, a_stage.at[pl.ds(0, 3)], True)
        far_met()
        for k in range(2, nz):
            ahead(k)
        relay(0, g.plane[1:])
        arrived(GAIN, gains.at[other])
        first_norm(sizes, tok, gains[0], normed_all, place)
        relay(1)
        half = micro * toks // 2
        for stage, near, target, first in ((TOK, g.x_near, g.y_near, 0), (TOKY, g.y_near, g.x_near, half)):
            arrived(stage, tok.at[near % 4])
            piece = tok.at[near % 4, pl.ds(first, half), :]
            xfer(TOKD, piece, piece, target, section).start()
        sent.append((TOKD, tok.at[0]))
        loaded(8, b_stage)
        scatter(LB, lambda p: b_stage.at[p], b1.at[:, own, :], section, b_stage.at[pl.ds(0, 3)], True)

        def far_refs(kind, zc):
            at = at_rows(zc, slab)
            if kind == 0:
                return [a1.at[at, pl.ds(0, 2 * part)]]
            if kind == 1:
                return [a1.at[at, pl.ds(2 * part, streams * part)]]
            return [b1.at[:, at_rows(near + 4 * (zc - z), rows), :] for near in g.plane[1:]]

        def far_total(kind):
            return far_refs(kind, 0)[0] if kind < 2 else b1.at[:, pl.ds(0, 3 * rows), :]

        def far_copy(ref, kind, zc, slot, target):
            return pltpu.make_async_remote_copy(
                src_ref=ref,
                dst_ref=ref,
                send_sem=far_send.at[kind, slot],
                recv_sem=far_recv.at[kind, zc],
                device_id={"section": section, "dp": target},
                device_id_type=MESH,
            )

        def far_moves(kind):
            for k in range(1, nz):
                for way in (k, -k):
                    there = z + way
                    when = (there >= 0) & (there < nz) if kind in () else g.reaches(way)
                    yield when, None, z, there, me + 4 * way
            for k in () if kind in () else range(1, nz - 2):
                for way in (k, -k):
                    yield g.passes(way), way, z + way, nz + k, me - 4 if way > 0 else me + 4

        def far_start(kind):
            for when, way, zc, slot, target in far_moves(kind):

                def go():
                    for ref in far_refs(kind, zc):
                        far_copy(ref, kind, zc, slot, target).start()

                if way is None:
                    pl.when(when)(go)

        def far_pass(kind):
            for when, way, zc, slot, target in far_moves(kind):

                def step():
                    far_copy(far_total(kind), kind, zc, 0, me).wait_recv()
                    for ref in far_refs(kind, zc):
                        far_copy(ref, kind, zc, slot, target).start()

                if way is not None:
                    pl.when(when)(step)

        def far_wait(kind):
            for k in range(1, nz):
                for way in (k, -k):
                    there = z + way
                    when = (there >= 0) & (there < nz)
                    if kind not in () and g.passes(way) is not None:
                        when = when & jnp.logical_not(g.passes(way))
                    pl.when(when)(lambda: far_copy(far_total(kind), kind, there, 0, me).wait_recv())

        def far_end(kind):
            for when, way, zc, slot, target in far_moves(kind):
                pl.when(when)(lambda: far_copy(far_total(kind), kind, zc, slot, target).wait_send())

        def far_begin():
            arrived(LA, a1.at[pl.ds(0, 3 * rows), :])
            far_start(0)
            far_start(1)

        for near in (g.x_near, g.y_near):
            first_norm(sizes, tok, gains[0], normed_all, near % 4)
        for d in range(2, nz - 1):
            relay(d)
        far_begin()
        arrived(TOKD, tok.at[g.diagonal % 4])
        first_norm(sizes, tok, gains[0], normed_all, g.diagonal % 4)
        for d in range(nz - 1):
            project(d)
        if nz > 2:
            relay(nz - 1)
        project(nz - 1)
        def give(i):
            target = g.plane[i]
            xfer(ATT, att_out.at[target % 4], att_in.at[:, column(place)], target, other).start()

        for i in FAR:
            for b in range(micro):
                first_attend(sizes, acc, att_out, g.plane[i] % 4, b)
            if i == FAR[1]:
                arrived(LB, b1.at[:, pl.ds(0, 3 * rows), :])
                far_start(2)
        firsts = []
        for p in range(4):
            for i in range(group):
                at = pl.ds(i * toks, 16) if i < streams * micro else pl.ds(0, 16)
                firsts.append(att_out[p, at, :].astype(F32)[:1])
        atc_out[...] = jnp.concatenate(firsts, 0).astype(BF16)
        scatter(ATC, lambda p: atc_out, atc_in.at[:, column(place)], other, atc_all)
        for i in FAR:
            give(i)
        sent.append((ATT, att_out))
        far_pass(0)
        fresh = []
        blank = jnp.zeros((group - micro, width), F32)
        for p in range(4):
            fresh += [tok[p, pl.ds(b * toks, 16), :].astype(F32)[:1] for b in range(micro)] + [blank]
        fresh = jnp.concatenate(fresh, 0)
        far_wait(0)
        arrived(CLS, cls_in)
        x = (fresh + cls_in[...]).astype(BF16).astype(F32)
        for p in range(4):
            cls_all[p] = x[p * group : (p + 1) * group]
        q = dot(norm_group(sizes, x, gains[1]), a1[:, pl.ds(0, part)]).astype(BF16).astype(F32)
        owner = lax.broadcasted_iota(jnp.int32, (group, part), 1) // HEAD
        zero = jnp.zeros((group, part), F32)
        spread = [
            jnp.where(owner == h, q[p * group : (p + 1) * group], zero) for p in range(4) for h in range(share)
        ]
        u = dot_t(jnp.concatenate(spread, 0).astype(BF16), a1[:, pl.ds(part, part)]).astype(BF16)
        tall = share * group
        for p in range(4):
            u_out[p] = u[p * tall : (p + 1) * tall]
        scatter(U, lambda p: u_out.at[p], u_all.at[place], other, u_out)
        far_pass(1)
        far_pass(2)
        far_wait(1)
        arrived(M, m_all)
        m = jnp.concatenate([m_all[p] for p in range(4)], 0)
        r = dot(m, a1[:, pl.ds(2 * part, streams * part)])
        mixed = lowered(sizes, [r[:, s * part : (s + 1) * part] for s in range(streams)])
        chosen = []
        for p in range(4):
            block = zero
            for h in range(share):
                at = p * tall + h * group
                block = jnp.where(owner == h, mixed[at : at + group], block)
            chosen.append(block)
        attended = jnp.concatenate(chosen, 0).astype(BF16)
        far_wait(2)
        if nz > 1:
            arrived(EARLY, early)
        out = lowered(sizes, [dot_t(attended, b1[s]) for s in range(streams)])
        for p in range(4):
            o_out[p] = out[p * group : (p + 1) * group].astype(BF16)
        scatter(O1, lambda p: o_out.at[p], o_all.at[place], section, o_out.at[pl.ds(0, 3)], True)
        scatter(O0, lambda p: o_out.at[p], o_all.at[place], other, o_out)
        o_all[place] = o_out[place]
        classes[...] = cls_all[place]
        arrived(O1, o_all.at[pl.ds(0, 3)])
        drain()
        for d in range(nz - 1):
            relay_end(d)
        for kind in range(3):
            far_end(kind)

    for move in tail_loads():
        move.wait()
    total = sum(o_all[p].astype(F32) for p in range(4))
    final = (classes[...] + total).astype(BF16).astype(F32)
    features = norm_group(sizes, final, final_gain[...])
    logits = dot_t(features, head[...])
    for s in range(streams):
        logit_ref[s, :, 0, :] = logits[s * micro : (s + 1) * micro]


def two_sections(n):
    def shards(tokens, w_qkv, w_output, tangent_value, tangent_output, layer_gain, final_gain, head):
        micro, _, toks, width = tokens.shape
        tangents = tangent_value.shape[1]
        hd = w_output.shape[1]
        count = head.shape[1]
        rows = width // n
        part = hd // 4
        nz = n // 4
        sizes = (micro, toks, width, hd, tangents)
        streams = 1 + tangents
        rows0 = micro * toks
        group = group_of(sizes)
        tall = part // HEAD * group
        vmem = pl.BlockSpec(memory_space=pltpu.VMEM)
        anywhere = pl.BlockSpec(memory_space=pl.ANY)
        dma = pltpu.SemaphoreType.DMA
        logits = pl.pallas_call(
            functools.partial(kernel, n, sizes),
            out_shape=pltpu.VMEM((streams, micro, 1, count), F32),
            in_specs=[anywhere] * 8,
            out_specs=vmem,
            scratch_shapes=[
                pltpu.VMEM((4, rows, (2 + streams) * part), BF16),
                pltpu.VMEM((4, streams, rows, part), BF16),
                pltpu.VMEM((width, (2 + streams) * part), BF16),
                pltpu.VMEM((width, (2 + streams) * part), BF16),
                pltpu.VMEM((streams, width, part), BF16),
                pltpu.VMEM((streams, width, hd), BF16),
                pltpu.VMEM((4, rows0, width), BF16),
                pltpu.VMEM((4 * rows0, width), BF16),
                pltpu.VMEM((4 * rows0, (2 + streams) * part), F32),
                pltpu.VMEM((4, streams * rows0, part), BF16),
                pltpu.VMEM((streams * rows0, hd), BF16),
                pltpu.VMEM((streams * rows0, width), BF16),
                pltpu.VMEM((streams, rows0, width), BF16),
                pltpu.VMEM((2, 1, width), F32),
                pltpu.VMEM((1, width), F32),
                pltpu.VMEM((count, width), BF16),
                pltpu.VMEM((4 * group, part), BF16),
                pltpu.VMEM((16 * group, part), BF16),
                pltpu.VMEM((4 * group, hd), BF16),
                pltpu.VMEM((4 * group, width), F32),
                pltpu.VMEM((4 * group, width), F32),
                pltpu.VMEM((4, group, width), F32),
                pltpu.VMEM((4, tall, width), BF16),
                pltpu.VMEM((4, tall, width), BF16),
                pltpu.VMEM((4, tall, width), BF16),
                pltpu.VMEM((4, tall, width), BF16),
                pltpu.VMEM((4, group, width), BF16),
                pltpu.VMEM((4, group, width), BF16),
                pltpu.VMEM((group, width), F32),
                dma((9,)),
                pltpu.SemaphoreType.REGULAR((2, max(nz - 1, 1))),
                dma((nz, 2)),
                dma((n,)),
                dma((STAGES,)),
                dma((STAGES,)),
                dma((3, 2 * nz)),
                dma((3, nz)),
                dma((4 * nz,)),
                dma((n, 2)),
            ],
            compiler_params=pltpu.CompilerParams(
                collective_id=0, has_side_effects=True, vmem_limit_bytes=63 * 2**20
            ),
        )(
            tokens.reshape(rows0, width),
            w_qkv[0],
            tangent_value[0],
            jnp.swapaxes(w_output[0], 0, 1),
            jnp.swapaxes(tangent_output[0], 1, 2),
            layer_gain,
            final_gain[None],
            head.T,
        )
        return logits[0], sum(logits[1 + j] * logits[1 + j] for j in range(tangents))

    return shards


def solution(mesh):
    n = mesh.shape["dp"]
    fast = mesh.shape["section"] == 2 and n % 4 == 0
    return jax.shard_map(
        two_sections(n) if fast else relay_shards,
        mesh=mesh,
        in_specs=(
            P(None, "dp", None, None),
            P("section", "dp", None),
            P("section", None, "dp"),
            P("section", None, "dp", None),
            P("section", None, None, "dp"),
            P("section", None),
            P(),
            P(None, "section"),
        ),
        out_specs=(P(None, "dp", "section"), P(None, "dp", "section")),
        check_vma=False,
    )
```

```python
import functools

import jax
import jax.numpy as jnp
from jax import lax
from jax.experimental import pallas as pl
from jax.experimental.pallas import tpu as pltpu
from jax.sharding import PartitionSpec as P

HEAD = 64
epsilon = 1e-06
F32, BF16 = jnp.float32, jnp.bfloat16
MESH = pl.DeviceIdType.MESH


def contract(spec, left, right):
    return jnp.einsum(spec, left, right, preferred_element_type=jnp.float32)


def norm_jvp(primal, tangents, gains):
    average = jnp.mean(primal, -1, keepdims=True)
    centred = primal - average
    inverse = lax.rsqrt(jnp.mean(centred * centred, -1, keepdims=True) + epsilon)
    dcentred = tangents - jnp.mean(tangents, -1, keepdims=True)
    dinverse = -(inverse**3) * jnp.mean(centred * dcentred, -1, keepdims=True)
    return (centred * inverse * gains, (dcentred * inverse + centred * dinverse) * gains)


def layer_step(state, qkv_weight, out_weight, value_tangent, out_tangent, gains):
    hd = out_weight.shape[0]
    heads = hd // HEAD
    resid = state.astype(F32)
    normed_zero, normed_rest = norm_jvp(resid[0], resid[1:], gains)
    normed = jnp.concatenate([normed_zero[None], normed_rest]).astype(BF16)
    streams, batch, tokens_here, width = normed.shape
    projected = contract("sbtd,de->sbte", normed, qkv_weight)
    extra_value = contract("btd,kde->kbte", normed[0], value_tangent)
    queries = projected[..., :hd]
    key_rows = projected[..., hd : 2 * hd]
    values = projected[..., 2 * hd :]
    values = jnp.concatenate([values[:1], values[1:] + extra_value])
    shape_heads = (streams, batch, tokens_here, heads, HEAD)
    queries = queries.astype(BF16).reshape(shape_heads)
    key_rows = key_rows.astype(BF16).reshape(shape_heads)
    values = values.astype(BF16).reshape(shape_heads)
    factor = HEAD ** (-0.5)
    scores = contract("bqhe,bkhe->bhqk", queries[0], key_rows[0]) * factor
    probs = jax.nn.softmax(scores, -1)
    dscores = (
        contract("sbqhe,bkhe->sbhqk", queries[1:], key_rows[0])
        + contract("bqhe,sbkhe->sbhqk", queries[0], key_rows[1:])
    ) * factor
    dprobs = probs * (dscores - jnp.sum(probs * dscores, -1, keepdims=True))
    probs_low = probs.astype(BF16)
    dprobs_low = dprobs.astype(BF16)
    attended_zero = contract("bhqk,bkhe->bqhe", probs_low, values[0])
    attended_rest = contract("sbhqk,bkhe->sbqhe", dprobs_low, values[0]) + contract(
        "bhqk,sbkhe->sbqhe", probs_low, values[1:]
    )
    attended = jnp.concatenate([attended_zero[None], attended_rest]).astype(BF16)
    attended = attended.reshape(streams, batch, tokens_here, hd)
    output = contract("sbte,ed->sbtd", attended, out_weight)
    extra_out = contract("bte,ked->kbtd", attended[0], out_tangent)
    output = jnp.concatenate([output[:1], output[1:] + extra_out])
    return (resid + output).astype(BF16)


def relay_shards(tokens, w_qkv, w_output, tangent_value, tangent_output, layer_gain, final_gain, head):
    full_qkv, full_output, full_value_tan, full_output_tan = (
        lax.all_gather(w_qkv, "dp", axis=1, tiled=True),
        lax.all_gather(w_output, "dp", axis=2, tiled=True),
        lax.all_gather(tangent_value, "dp", axis=2, tiled=True),
        lax.all_gather(tangent_output, "dp", axis=3, tiled=True),
    )
    tangents = tangent_value.shape[1]

    def advance_layer(state):
        return layer_step(
            state, full_qkv[0], full_output[0], full_value_tan[0], full_output_tan[0], layer_gain[0]
        )

    section_index = lax.axis_index("section")
    section_count = lax.axis_size("section")
    route = [(i, i + 1) for i in range(section_count - 1)]
    micro, _, toks, width = tokens.shape
    entering = jnp.concatenate(
        [tokens.reshape(1, micro, toks, width), jnp.zeros((tangents, micro, toks, width), BF16)]
    )

    def advance(step, outgoing):
        incoming = lax.ppermute(outgoing, "section", route)
        source = jnp.where(step == 0, entering, incoming)
        return lax.cond(section_index == step, advance_layer, jnp.zeros_like, source)

    finished = lax.fori_loop(0, section_count, advance, jnp.zeros_like(entering))
    collected = finished[:, :, 0, :]
    mine = section_index == section_count - 1
    features = lax.psum(jnp.where(mine, collected, jnp.zeros_like(collected)), "section")
    widened = features.astype(F32)
    final_zero, final_rest = norm_jvp(widened[0], widened[1:], final_gain)
    normed_final = jnp.concatenate([final_zero[None], final_rest]).astype(BF16)
    logits = contract("sbd,dc->sbc", normed_final, head)
    return (logits[0][:, None, :], jnp.sum(logits[1:] * logits[1:], 0)[:, None, :])


def dot(a, b):
    return lax.dot_general(a, b, (((1,), (0,)), ((), ())), preferred_element_type=F32)


def dot_t(a, b):
    return lax.dot_general(a, b, (((1,), (1,)), ((), ())), preferred_element_type=F32)


class Gather:
    def __init__(self, n, g, full, send, recv):
        self.nz = n // 4
        self.full, self.send, self.recv = full, send, recv
        self.rows = full.shape[1] // n
        self.g = g

    def remote(self, ref, target, sem, recv):
        return pltpu.make_async_remote_copy(
            src_ref=ref,
            dst_ref=ref,
            send_sem=self.send.at[sem],
            recv_sem=self.recv.at[recv],
            device_id={"section": self.g.section, "dp": target},
            device_id_type=MESH,
        )

    def half(self, src, half):
        depth = self.rows // 2
        return self.full.at[:, pl.ds(pl.multiple_of(src * self.rows + half * depth, depth), depth), :]

    def total(self, pieces):
        return self.full.at[:, pl.ds(0, pieces * self.rows), :]

    def line(self, plane, half):
        return 2 * plane + half

    def turn(self, plane, way):
        return 2 * self.nz + 2 * plane + way

    def forward(self, cond, src, half, target, sem, recv):
        def go():
            self.remote(self.half(src, half), target, sem, recv).start()

        go() if cond is None else pl.when(cond)(go)

    def arrived(self, src, half, recv):
        self.remote(self.half(src, half), self.g.me, 0, recv).wait_recv()

    def along(self, far):
        g, nz = self.g, self.nz
        for k in range(2, nz) if far else range(1, min(nz, 2)):
            for way in (k, -k):
                for half in range(2):
                    self.forward(g.reaches(way), g.me, half, g.me + 4 * way, 0, self.line(g.z, half))

    def pass_on(self, d):
        g = self.g
        for shift, cond in g.sources(d):
            passed = g.passes(shift)
            if passed is not None:
                src, plane = g.me + 4 * shift, g.z + shift
                for half in range(2):
                    pl.when(passed)(functools.partial(self.arrived, src, half, self.line(plane, half)))
                    target = g.me - 4 if shift > 0 else g.me + 4
                    self.forward(passed, src, half, target, 0, self.line(plane, half))

    def direct(self, d):
        g = self.g
        for shift, cond in g.sources(d):
            src, plane = g.me + 4 * shift, g.z + shift
            passed = g.passes(shift)
            for half in range(2):
                if d > 0:
                    fresh = cond if passed is None else cond & jnp.logical_not(passed)
                    pl.when(fresh)(functools.partial(self.arrived, src, half, self.line(plane, half)))
                for way in (1 - half, half):
                    recv = self.turn(plane, way) if way == half else 4 * self.nz
                    self.forward(cond, src, half, (g.x_near, g.y_near)[way], 1, recv)

    def relay(self, d):
        g = self.g
        for shift, cond in g.sources(d):
            for way, near, target in ((0, g.x_near, g.y_near), (1, g.y_near, g.x_near)):
                src = near + 4 * shift
                wait = functools.partial(self.arrived, src, way, self.turn(g.z + shift, way))
                wait() if cond is None else pl.when(cond)(wait)
                self.forward(cond, src, way, target, 1, 4 * self.nz)

    def rest(self):
        self.remote(self.total(2 * self.nz), self.g.me, 0, 4 * self.nz).wait_recv()

    def drain(self):
        if self.nz > 1:
            self.remote(self.total(self.nz - 1), self.g.me, 0, 0).wait_send()
        self.remote(self.total(3 * self.nz), self.g.me, 1, 0).wait_send()


class Place:
    def __init__(self, n):
        self.nz = n // 4
        self.me = lax.axis_index("dp")
        self.section = lax.axis_index("section")
        me = self.me
        self.x_near = me + 1 - 2 * (me % 2)
        self.y_near = me + 2 - 4 * ((me // 2) % 2)
        self.diagonal = self.x_near + self.y_near - me
        self.z = me // 4
        self.place = me % 4
        self.up, self.down = self.z + 1 < self.nz, self.z >= 1
        self.plane = (me, self.x_near, self.y_near, self.diagonal)

    def sources(self, d):
        if d == 0:
            return [(0, None)]
        return [(-d, self.z >= d), (d, self.z + d < self.nz)]

    def reaches(self, way):
        z, nz = self.z, self.nz
        there = z + way
        when = (there >= 0) & (there < nz)
        if abs(way) > 1:
            when = when & ((z == 0) | (z == nz - 1) | ((there > 0) & (there < nz - 1)))
        return when

    def passes(self, shift):
        z, nz = self.z, self.nz
        if not 0 < abs(shift) < nz - 2:
            return None
        return (z == 1) & (z + shift < nz - 1) if shift > 0 else (z == nz - 2) & (z + shift > 0)


def norm_rows(x, gains):
    average = jnp.mean(x, -1, keepdims=True)
    centred = x - average
    inverse = lax.rsqrt(jnp.mean(centred * centred, -1, keepdims=True) + epsilon)
    return centred, inverse, centred * inverse * gains


def norm_tangent(t, centred, inverse, gains):
    dcentred = t - jnp.mean(t, -1, keepdims=True)
    dinverse = -(inverse * inverse * inverse) * jnp.mean(centred * dcentred, -1, keepdims=True)
    return (dcentred * inverse + centred * dinverse) * gains


def softmax(scores):
    e = jnp.exp(scores - jnp.max(scores, -1, keepdims=True))
    return e / jnp.sum(e, -1, keepdims=True)


def at_rows(i, count):
    return pl.ds(pl.multiple_of(i * count, count), count)


def first_norm(sizes, tok, gain, normed, slot):
    micro, toks, width, hd, tangents = sizes
    for b in range(micro):
        x = tok[slot, pl.ds(b * toks, toks), :].astype(F32)
        normed[at_rows(slot * micro + b, toks), :] = norm_rows(x, gain)[2].astype(BF16)


def first_attend(sizes, acc, att, slot, b):
    micro, toks, width, hd, tangents = sizes
    factor = HEAD ** (-0.5)
    part = 2 * HEAD
    streams = 1 + tangents
    even = lax.broadcasted_iota(jnp.int32, (toks, part), 1) < HEAD
    rows = at_rows(slot * micro + b, toks)
    q = acc[rows, pl.ds(0, part)]
    k = acc[rows, pl.ds(part, part)].astype(BF16)
    v = acc[rows, pl.ds(2 * part, streams * part)].astype(BF16)
    zero = jnp.zeros_like(q)
    both = jnp.concatenate([jnp.where(even, q, zero), jnp.where(even, zero, q)], 0).astype(BF16)
    scores = dot_t(both, k) * factor
    low = jnp.exp(scores - jnp.max(scores, -1, keepdims=True)).astype(BF16)
    out = dot(low, jnp.concatenate([v, jnp.ones((toks, part), BF16)], 1))

    def joined(s):
        at = slice(s * part, (s + 1) * part)
        return jnp.where(even, out[:toks, at], out[toks:, at])

    scale = 1.0 / joined(streams)
    for s in range(streams):
        att[slot, pl.ds((s * micro + b) * toks, toks), :] = (joined(s) * scale).astype(BF16)


def first_out(sizes, tok, place, b_full, att, state):
    micro, toks, width, hd, tangents = sizes
    rows0 = micro * toks
    tile = 256
    for c in range(width // tile):
        at = pl.ds(c * tile, tile)
        out = dot_t(att[...], b_full[0, at, :])
        extra = [dot_t(att[pl.ds(0, rows0), :], b_full[1 + j, at, :]) for j in range(tangents)]
        x = tok[place, :, at].astype(F32)
        state[pl.ds(0, rows0), at] = (x + out[:rows0]).astype(BF16)
        for j in range(tangents):
            state[pl.ds((1 + j) * rows0, rows0), at] = (
                out[(1 + j) * rows0 : (2 + j) * rows0] + extra[j]
            ).astype(BF16)


def group_of(sizes):
    micro, toks, width, hd, tangents = sizes
    return -(-micro * (1 + tangents) // 8) * 8


def stream_of(sizes, shape):
    return (lax.broadcasted_iota(jnp.int32, shape, 0) % group_of(sizes)) // sizes[0]


def lowered(sizes, parts):
    micro, tangents = sizes[0], sizes[4]
    stream = stream_of(sizes, parts[0].shape)
    total = parts[0]
    for j in range(tangents):
        moved = pltpu.roll(parts[1 + j], micro * (1 + j), 0)
        total = total + jnp.where(stream == 1 + j, moved, jnp.zeros_like(moved))
    return total


def primal_rows(sizes, x):
    micro, tangents = sizes[0], sizes[4]
    stream = stream_of(sizes, x.shape)
    spread = x
    for j in range(tangents):
        spread = jnp.where(stream == 1 + j, pltpu.roll(x, micro * (1 + j), 0), spread)
    return spread


def norm_group(sizes, x, gains):
    stream = stream_of(sizes, x.shape)
    centred, inverse, y = norm_rows(primal_rows(sizes, x), gains)
    dy = norm_tangent(x, centred, inverse, gains)
    return jnp.where(stream == 0, y, dy).astype(BF16)


def class_rows(sizes, state):
    micro, toks, width, hd, tangents = sizes
    streams = 1 + tangents
    rows = [
        state[pl.ds((s * micro + b) * toks, 16), :].astype(F32)[:1] for s in range(streams) for b in range(micro)
    ]
    return jnp.concatenate(rows + [jnp.zeros((group_of(sizes) - micro * streams, width), F32)], 0)


def last_norm(sizes, gain, state, normed):
    micro, toks, width, hd, tangents = sizes
    rows0 = micro * toks
    for b in range(micro):
        at = pl.ds(b * toks, toks)
        centred, inverse, y = norm_rows(state[at, :].astype(F32), gain)
        normed[0, at, :] = y.astype(BF16)
        for j in range(tangents):
            t = state[pl.ds((1 + j) * rows0 + b * toks, toks), :].astype(F32)
            normed[1 + j, at, :] = norm_tangent(t, centred, inverse, gain).astype(BF16)


def last_attend(sizes, u, normed):
    micro, toks, width, hd, tangents = sizes
    factor = HEAD ** (-0.5)
    shape = (u.shape[0], micro * toks)
    stream = stream_of(sizes, shape)
    image = (lax.broadcasted_iota(jnp.int32, shape, 0) % group_of(sizes)) % micro
    valid = lax.broadcasted_iota(jnp.int32, shape, 1) // toks == image
    parts = [dot_t(u, normed[s]) * factor for s in range(1 + tangents)]
    probs = softmax(jnp.where(valid, parts[0], -jnp.inf))
    weights = primal_rows(sizes, probs)
    scores = lowered(sizes, parts)
    dprobs = weights * (scores - jnp.sum(weights * scores, -1, keepdims=True))
    zero = jnp.zeros_like(weights)
    total = dot(jnp.where(stream == 0, weights, dprobs).astype(BF16), normed[0])
    for j in range(tangents):
        total = total + dot(jnp.where(stream == 1 + j, weights, zero).astype(BF16), normed[1 + j])
    return total.astype(BF16)


TOK, TOKY, TOKD, LA, LB, ATT, ATC, CLS, U, M, O1, O0, GAIN, FIRST, EARLY, STAGES = range(16)


def kernel(
    n, sizes, tokens, w_qkv, tangent_value, w_out, t_out, gain_in, final_in, head_in, logit_ref,
    a_stage, b_stage, a0, a1, b1, b_full, tok, normed_all, acc, att_out, att_in, state, normed,
    gains, final_gain, head, atc_out, atc_all, atc_in, cls_out, cls_in, cls_all, u_out, u_all, m_out, m_all, o_out, o_all, classes,
    loads, line, a_send, a_recv, stage_send, stage_recv, far_send, far_recv, b_send, b_recv,
):
    micro, toks, width, hd, tangents = sizes
    streams = 1 + tangents
    part = hd // 4
    share = part // HEAD
    g = Place(n)
    me, section, place, z, nz = g.me, g.section, g.place, g.z, g.nz
    other = 1 - section
    rows = width // n
    slab = 4 * rows
    group = group_of(sizes)
    own = at_rows(me, rows)

    barrier = pltpu.get_barrier_semaphore()

    def greet(target, sec):
        pl.semaphore_signal(
            barrier, inc=1, device_id={"section": sec, "dp": target}, device_id_type=MESH
        )

    pl.when(g.up)(lambda: greet(me + 4, section))
    pl.when(g.down)(lambda: greet(me - 4, section))
    for near in (g.diagonal, g.x_near, g.y_near):
        greet(near, section)
        greet(near, other)
    greet(me, other)

    def met():
        if nz > 1:
            middle = g.up & g.down
            pl.when(middle)(lambda: pl.semaphore_wait(barrier, 9))
            pl.when(jnp.logical_not(middle))(lambda: pl.semaphore_wait(barrier, 8))
        else:
            pl.semaphore_wait(barrier, 7)

    def column(p):
        return pl.ds(p * part, part) if isinstance(p, int) else at_rows(p, part)

    def load(i, src, dst):
        return pltpu.make_async_copy(src, dst, loads.at[i])

    def stage_loads():
        for p in range(4):
            for m in range(3):
                load(5, w_qkv.at[:, pl.ds(m * hd + p * part, part)], a_stage.at[p, :, pl.ds(m * part, part)]).start()
            for j in range(tangents):
                load(
                    5,
                    tangent_value.at[j, :, pl.ds(p * part, part)],
                    a_stage.at[p, :, pl.ds((3 + j) * part, part)],
                ).start()

    def own_loads():
        for m in range(3):
            load(6, w_qkv.at[:, column(m * 4 + place)], a1.at[own, pl.ds(m * part, part)]).start()
        for j in range(tangents):
            load(6, tangent_value.at[j, :, column(place)], a1.at[own, pl.ds((3 + j) * part, part)]).start()
        load(7, w_out.at[:, column(place)], b1.at[0, own, :]).start()
        load(7, t_out.at[:, :, column(place)], b1.at[pl.ds(1, tangents), own, :]).start()
        for p in range(4):
            load(8, w_out.at[:, pl.ds(p * part, part)], b_stage.at[p, 0]).start()
            load(8, t_out.at[:, :, pl.ds(p * part, part)], b_stage.at[p, pl.ds(1, tangents)]).start()

    def b_loads():
        load(4, w_out, b_full.at[0, own, :]).start()
        load(4, t_out, b_full.at[pl.ds(1, tangents), own, :]).start()

    def loaded(i, ref):
        load(i, ref, ref).wait()

    def gain_load():
        return load(0, gain_in, gains.at[section])

    def tok_load():
        return load(1, tokens, tok.at[place])

    def tail_loads():
        return [load(2, head_in, head), load(3, final_in, final_gain)]

    stage_loads()
    gain_load().start()
    tok_load().start()
    pl.when(section == 0)(b_loads)
    pl.when(section == 1)(own_loads)
    for move in tail_loads():
        move.start()
    met()

    def tell(way, level, target):
        pl.semaphore_signal(
            line.at[way, level], inc=1, device_id={"section": section, "dp": target}, device_id_type=MESH
        )

    if nz > 2:

        @pl.when(g.up & g.down)
        def _():
            tell(0, 1, me + 4)
            tell(1, 1, me - 4)

    def far_met():
        for level in range(1, nz - 1):

            @pl.when(z - 1 - level >= 0)
            def _():
                pl.semaphore_wait(line.at[0, level], 1)
                if level + 1 < nz - 1:
                    pl.when(g.up)(lambda: tell(0, level + 1, me + 4))

            @pl.when(z + 1 + level < nz)
            def _():
                pl.semaphore_wait(line.at[1, level], 1)
                if level + 1 < nz - 1:
                    pl.when(g.down)(lambda: tell(1, level + 1, me - 4))


    def xfer(stage, src, dst, target, sec):
        return pltpu.make_async_remote_copy(
            src_ref=src,
            dst_ref=dst,
            send_sem=stage_send.at[stage],
            recv_sem=stage_recv.at[stage],
            device_id={"section": sec, "dp": target},
            device_id_type=MESH,
        )

    def arrived(stage, ref):
        xfer(stage, ref, ref, me, other).wait_recv()

    sent = []

    FAR = (3, 1, 2, 0)

    def scatter(stage, src, dst, sec, total, skip_own=False):
        for i in FAR:
            if i > 0 or not skip_own:
                target = g.plane[i]
                xfer(stage, src(target % 4), dst, target, sec).start()
        sent.append((stage, total))

    def drain():
        for stage, ref in sent:
            xfer(stage, ref, ref, me, other).wait_send()
        sent.clear()

    def a_ref(src):
        return a0.at[at_rows(src, rows), :]

    def a_copy(src_ref, src, sem, target, sec):
        return pltpu.make_async_remote_copy(
            src_ref=src_ref,
            dst_ref=a_ref(src),
            send_sem=sem,
            recv_sem=a_recv.at[src],
            device_id={"section": sec, "dp": target},
            device_id_type=MESH,
        )

    @pl.when(section == 0)
    def _():
        loaded(5, a_stage)
        for i in range(4):
            target = g.plane[i]
            a_copy(a_stage.at[target % 4], me, stage_send.at[FIRST], target, other).start()
        sent.append((FIRST, a_stage))
        gain_load().wait()
        xfer(GAIN, gains.at[section], gains.at[section], me, other).start()
        sent.append((GAIN, gains.at[section]))
        loaded(4, b_full.at[:, own, :])
        gather = Gather(n, g, b_full, b_send, b_recv)
        lag = 2
        gather.along(False)
        for d in range(nz + lag):
            if d < nz:
                gather.pass_on(d)
                gather.direct(d)
                if d == 0:
                    far_met()
                    gather.along(True)
            if d >= lag:
                gather.relay(d - lag)
        tok_load().wait()
        gather.rest()
        arrived(ATC, atc_in)
        cls_out[...] = lowered(sizes, [dot_t(atc_in[...], b_full[s]) for s in range(streams)])
        xfer(CLS, cls_out, cls_in, me, other).start()
        sent.append((CLS, cls_out))
        arrived(ATT, att_in)
        first_out(sizes, tok, place, b_full, att_in, state)
        arrived(GAIN, gains.at[other])
        last_norm(sizes, gains[1], state, normed)
        arrived(U, u_all)
        u = jnp.concatenate([u_all[p] for p in range(4)], 0)
        m = last_attend(sizes, u, normed)
        for p in range(4):
            m_out[p] = m[p * share * group : (p + 1) * share * group]
        scatter(M, lambda p: m_out.at[p], m_all.at[place], other, m_out)
        classes[...] = class_rows(sizes, state)
        gather.drain()
        drain()
        arrived(O0, o_all)

    @pl.when(section == 1)
    def _():
        gain_load().wait()
        xfer(GAIN, gains.at[section], gains.at[section], me, other).start()
        sent.append((GAIN, gains.at[section]))
        tok_load().wait()

        def relay(d, some=g.plane):
            for near in some:
                for shift, cond in g.sources(d)[::-1]:

                    def step():
                        src = near + 4 * shift
                        a_copy(a_ref(src), src, a_send.at[d, 0], me, section).wait_recv()
                        if shift >= 0 and d < nz - 1:
                            pl.when(g.down)(
                                lambda: a_copy(a_ref(src), src, a_send.at[d, 1], me - 4, section).start()
                            )
                        if shift <= 0 and d < nz - 1:
                            pl.when(g.up)(
                                lambda: a_copy(a_ref(src), src, a_send.at[d, 0], me + 4, section).start()
                            )

                    step() if cond is None else pl.when(cond)(step)

        def relay_end(d):
            slab_ref = a0.at[pl.ds(0, slab), :]
            for shift, cond in g.sources(d):

                def end(way):
                    pltpu.make_async_remote_copy(
                        src_ref=slab_ref,
                        dst_ref=slab_ref,
                        send_sem=a_send.at[d, way],
                        recv_sem=a_recv.at[0],
                        device_id={"section": section, "dp": me},
                        device_id_type=MESH,
                    ).wait_send()

                if shift <= 0:
                    pl.when(g.up if cond is None else cond & g.up)(functools.partial(end, 0))
                if shift >= 0:
                    pl.when(g.down if cond is None else cond & g.down)(functools.partial(end, 1))

        def project(d):
            for shift, cond in g.sources(d):

                def step(shift=shift):
                    at = at_rows(z + shift, slab)
                    term = dot(normed_all[:, at], a0[at, :])
                    acc[...] = term if d == 0 else acc[...] + term

                step() if cond is None else pl.when(cond)(step)

        loaded(7, b1.at[:, own, :])
        early = b1.at[:, pl.ds(0, (nz - 1) * rows), :]

        def ahead(k):
            for way in (k, -k):
                there = (z + way >= 0) & (z + way < nz)

                def go():
                    xfer(EARLY, b1.at[:, own, :], b1.at[:, own, :], me + 4 * way, section).start()

                pl.when(there)(go)

        if nz > 1:
            ahead(1)
        if nz > 1:
            sent.append((EARLY, early))
        relay(0, g.plane[:1])
        for stage, near in ((TOK, g.x_near), (TOKY, g.y_near)):
            xfer(stage, tok.at[place], tok.at[place], near, section).start()
            sent.append((stage, tok.at[place]))
        loaded(5, a_stage)
        loaded(6, a1.at[own, :])
        scatter(LA, lambda p: a_stage.at[p], a1.at[own, :], section, a_stage.at[pl.ds(0, 3)], True)
        far_met()
        for k in range(2, nz):
            ahead(k)
        relay(0, g.plane[1:])
        arrived(GAIN, gains.at[other])
        first_norm(sizes, tok, gains[0], normed_all, place)
        relay(1)
        half = micro * toks // 2
        for stage, near, target, first in ((TOK, g.x_near, g.y_near, 0), (TOKY, g.y_near, g.x_near, half)):
            arrived(stage, tok.at[near % 4])
            piece = tok.at[near % 4, pl.ds(first, half), :]
            xfer(TOKD, piece, piece, target, section).start()
        sent.append((TOKD, tok.at[0]))
        loaded(8, b_stage)
        scatter(LB, lambda p: b_stage.at[p], b1.at[:, own, :], section, b_stage.at[pl.ds(0, 3)], True)

        def far_refs(kind, zc):
            at = at_rows(zc, slab)
            if kind == 0:
                return [a1.at[at, pl.ds(0, 2 * part)]]
            if kind == 1:
                return [a1.at[at, pl.ds(2 * part, streams * part)]]
            return [b1.at[:, at_rows(near + 4 * (zc - z), rows), :] for near in g.plane[1:]]

        def far_total(kind):
            return far_refs(kind, 0)[0] if kind < 2 else b1.at[:, pl.ds(0, 3 * rows), :]

        def far_copy(ref, kind, zc, target):
            return pltpu.make_async_remote_copy(
                src_ref=ref,
                dst_ref=ref,
                send_sem=far_send.at[kind],
                recv_sem=far_recv.at[kind, zc],
                device_id={"section": section, "dp": target},
                device_id_type=MESH,
            )

        def far_moves(kind):
            for k in range(1, nz):
                for way in (k, -k):
                    yield g.reaches(way), None, z, me + 4 * way
            for k in range(1, nz - 2):
                for way in (k, -k):
                    yield g.passes(way), way, z + way, me - 4 if way > 0 else me + 4

        def far_start(kind):
            for when, way, zc, target in far_moves(kind):

                def go():
                    for ref in far_refs(kind, zc):
                        far_copy(ref, kind, zc, target).start()

                if way is None:
                    pl.when(when)(go)

        def far_pass(kind):
            for when, way, zc, target in far_moves(kind):

                def step():
                    far_copy(far_total(kind), kind, zc, me).wait_recv()
                    for ref in far_refs(kind, zc):
                        far_copy(ref, kind, zc, target).start()

                if way is not None:
                    pl.when(when)(step)

        def far_wait(kind):
            for k in range(1, nz):
                for way in (k, -k):
                    there = z + way
                    when = (there >= 0) & (there < nz)
                    if g.passes(way) is not None:
                        when = when & jnp.logical_not(g.passes(way))
                    pl.when(when)(lambda: far_copy(far_total(kind), kind, there, me).wait_recv())

        def far_end(kind):
            count = nz - 1
            if kind < 2:
                first, last = ((0, 2), (2, 2 + streams))[kind]
                ref = a1.at[pl.ds(0, count * slab), pl.ds(first * part, (last - first) * part)]
            else:
                ref = b1.at[:, pl.ds(0, count * 3 * rows), :]
            if count > 0:
                far_copy(ref, kind, 0, me).wait_send()

        def far_begin():
            arrived(LA, a1.at[pl.ds(0, 3 * rows), :])
            far_start(0)
            far_start(1)

        for near in (g.x_near, g.y_near):
            first_norm(sizes, tok, gains[0], normed_all, near % 4)
        for d in range(2, nz - 1):
            relay(d)
        far_begin()
        arrived(TOKD, tok.at[g.diagonal % 4])
        first_norm(sizes, tok, gains[0], normed_all, g.diagonal % 4)
        for d in range(nz - 1):
            project(d)
        if nz > 2:
            relay(nz - 1)
        project(nz - 1)
        def give(i):
            target = g.plane[i]
            xfer(ATT, att_out.at[target % 4], att_in.at[:, column(place)], target, other).start()

        for i in FAR:
            for b in range(micro):
                first_attend(sizes, acc, att_out, g.plane[i] % 4, b)
            if i == FAR[1]:
                arrived(LB, b1.at[:, pl.ds(0, 3 * rows), :])
                far_start(2)
        firsts = []
        for p in range(4):
            for i in range(group):
                at = pl.ds(i * toks, 16) if i < streams * micro else pl.ds(0, 16)
                firsts.append(att_out[p, at, :].astype(F32)[:1])
        atc_out[...] = jnp.concatenate(firsts, 0).astype(BF16)
        scatter(ATC, lambda p: atc_out, atc_in.at[:, column(place)], other, atc_all)
        for i in FAR:
            give(i)
        sent.append((ATT, att_out))
        far_pass(0)
        fresh = []
        blank = jnp.zeros((group - micro, width), F32)
        for p in range(4):
            fresh += [tok[p, pl.ds(b * toks, 16), :].astype(F32)[:1] for b in range(micro)] + [blank]
        fresh = jnp.concatenate(fresh, 0)
        far_wait(0)
        arrived(CLS, cls_in)
        x = (fresh + cls_in[...]).astype(BF16).astype(F32)
        for p in range(4):
            cls_all[p] = x[p * group : (p + 1) * group]
        q = dot(norm_group(sizes, x, gains[1]), a1[:, pl.ds(0, part)]).astype(BF16).astype(F32)
        owner = lax.broadcasted_iota(jnp.int32, (group, part), 1) // HEAD
        zero = jnp.zeros((group, part), F32)
        spread = [
            jnp.where(owner == h, q[p * group : (p + 1) * group], zero) for p in range(4) for h in range(share)
        ]
        u = dot_t(jnp.concatenate(spread, 0).astype(BF16), a1[:, pl.ds(part, part)]).astype(BF16)
        tall = share * group
        for p in range(4):
            u_out[p] = u[p * tall : (p + 1) * tall]
        scatter(U, lambda p: u_out.at[p], u_all.at[place], other, u_out)
        far_pass(1)
        far_pass(2)
        far_wait(1)
        arrived(M, m_all)
        m = jnp.concatenate([m_all[p] for p in range(4)], 0)
        r = dot(m, a1[:, pl.ds(2 * part, streams * part)])
        mixed = lowered(sizes, [r[:, s * part : (s + 1) * part] for s in range(streams)])
        chosen = []
        for p in range(4):
            block = zero
            for h in range(share):
                at = p * tall + h * group
                block = jnp.where(owner == h, mixed[at : at + group], block)
            chosen.append(block)
        attended = jnp.concatenate(chosen, 0).astype(BF16)
        far_wait(2)
        if nz > 1:
            arrived(EARLY, early)
        out = lowered(sizes, [dot_t(attended, b1[s]) for s in range(streams)])
        for p in range(4):
            o_out[p] = out[p * group : (p + 1) * group].astype(BF16)
        scatter(O0, lambda p: o_out.at[p], o_all.at[place], other, o_out)
        scatter(O1, lambda p: o_out.at[p], o_all.at[place], section, o_out.at[pl.ds(0, 3)], True)
        o_all[place] = o_out[place]
        classes[...] = cls_all[place]
        for d in range(nz - 1):
            relay_end(d)
        for kind in range(3):
            far_end(kind)
        drain()
        arrived(O1, o_all.at[pl.ds(0, 3)])

    for move in tail_loads():
        move.wait()
    total = sum(o_all[p].astype(F32) for p in range(4))
    final = (classes[...] + total).astype(BF16).astype(F32)
    features = norm_group(sizes, final, final_gain[...])
    logits = dot_t(features, head[...])
    for s in range(streams):
        logit_ref[s, :, 0, :] = logits[s * micro : (s + 1) * micro]


def two_sections(n):
    def shards(tokens, w_qkv, w_output, tangent_value, tangent_output, layer_gain, final_gain, head):
        micro, _, toks, width = tokens.shape
        tangents = tangent_value.shape[1]
        hd = w_output.shape[1]
        count = head.shape[1]
        rows = width // n
        part = hd // 4
        nz = n // 4
        sizes = (micro, toks, width, hd, tangents)
        streams = 1 + tangents
        rows0 = micro * toks
        group = group_of(sizes)
        tall = part // HEAD * group
        vmem = pl.BlockSpec(memory_space=pltpu.VMEM)
        anywhere = pl.BlockSpec(memory_space=pl.ANY)
        dma = pltpu.SemaphoreType.DMA
        logits = pl.pallas_call(
            functools.partial(kernel, n, sizes),
            out_shape=pltpu.VMEM((streams, micro, 1, count), F32),
            in_specs=[anywhere] * 8,
            out_specs=vmem,
            scratch_shapes=[
                pltpu.VMEM((4, rows, (2 + streams) * part), BF16),
                pltpu.VMEM((4, streams, rows, part), BF16),
                pltpu.VMEM((width, (2 + streams) * part), BF16),
                pltpu.VMEM((width, (2 + streams) * part), BF16),
                pltpu.VMEM((streams, width, part), BF16),
                pltpu.VMEM((streams, width, hd), BF16),
                pltpu.VMEM((4, rows0, width), BF16),
                pltpu.VMEM((4 * rows0, width), BF16),
                pltpu.VMEM((4 * rows0, (2 + streams) * part), F32),
                pltpu.VMEM((4, streams * rows0, part), BF16),
                pltpu.VMEM((streams * rows0, hd), BF16),
                pltpu.VMEM((streams * rows0, width), BF16),
                pltpu.VMEM((streams, rows0, width), BF16),
                pltpu.VMEM((2, 1, width), F32),
                pltpu.VMEM((1, width), F32),
                pltpu.VMEM((count, width), BF16),
                pltpu.VMEM((4 * group, part), BF16),
                pltpu.VMEM((16 * group, part), BF16),
                pltpu.VMEM((4 * group, hd), BF16),
                pltpu.VMEM((4 * group, width), F32),
                pltpu.VMEM((4 * group, width), F32),
                pltpu.VMEM((4, group, width), F32),
                pltpu.VMEM((4, tall, width), BF16),
                pltpu.VMEM((4, tall, width), BF16),
                pltpu.VMEM((4, tall, width), BF16),
                pltpu.VMEM((4, tall, width), BF16),
                pltpu.VMEM((4, group, width), BF16),
                pltpu.VMEM((4, group, width), BF16),
                pltpu.VMEM((group, width), F32),
                dma((9,)),
                pltpu.SemaphoreType.REGULAR((2, max(nz - 1, 1))),
                dma((nz, 2)),
                dma((n,)),
                dma((STAGES,)),
                dma((STAGES,)),
                dma((3,)),
                dma((3, nz)),
                dma((2,)),
                dma((4 * nz + 1,)),
            ],
            compiler_params=pltpu.CompilerParams(
                collective_id=0, has_side_effects=True, vmem_limit_bytes=63 * 2**20
            ),
        )(
            tokens.reshape(rows0, width),
            w_qkv[0],
            tangent_value[0],
            jnp.swapaxes(w_output[0], 0, 1),
            jnp.swapaxes(tangent_output[0], 1, 2),
            layer_gain,
            final_gain[None],
            head.T,
        )
        return logits[0], sum(logits[1 + j] * logits[1 + j] for j in range(tangents))

    return shards


def solution(mesh):
    n = mesh.shape["dp"]
    fast = mesh.shape["section"] == 2 and n % 4 == 0 and n // 4 <= 4
    return jax.shard_map(
        two_sections(n) if fast else relay_shards,
        mesh=mesh,
        in_specs=(
            P(None, "dp", None, None),
            P("section", "dp", None),
            P("section", None, "dp"),
            P("section", None, "dp", None),
            P("section", None, None, "dp"),
            P("section", None),
            P(),
            P(None, "section"),
        ),
        out_specs=(P(None, "dp", "section"), P(None, "dp", "section")),
        check_vma=False,
    )
```

```python
import functools

import jax
import jax.numpy as jnp
from jax import lax
from jax.experimental import pallas as pl
from jax.experimental.pallas import tpu as pltpu
from jax.sharding import PartitionSpec as P

HEAD = 64
epsilon = 1e-06
F32, BF16 = jnp.float32, jnp.bfloat16
MESH = pl.DeviceIdType.MESH


def contract(spec, left, right):
    return jnp.einsum(spec, left, right, preferred_element_type=jnp.float32)


def norm_jvp(primal, tangents, gains):
    average = jnp.mean(primal, -1, keepdims=True)
    centred = primal - average
    inverse = lax.rsqrt(jnp.mean(centred * centred, -1, keepdims=True) + epsilon)
    dcentred = tangents - jnp.mean(tangents, -1, keepdims=True)
    dinverse = -(inverse**3) * jnp.mean(centred * dcentred, -1, keepdims=True)
    return (centred * inverse * gains, (dcentred * inverse + centred * dinverse) * gains)


def layer_step(state, qkv_weight, out_weight, value_tangent, out_tangent, gains):
    hd = out_weight.shape[0]
    heads = hd // HEAD
    resid = state.astype(F32)
    normed_zero, normed_rest = norm_jvp(resid[0], resid[1:], gains)
    normed = jnp.concatenate([normed_zero[None], normed_rest]).astype(BF16)
    streams, batch, tokens_here, width = normed.shape
    projected = contract("sbtd,de->sbte", normed, qkv_weight)
    extra_value = contract("btd,kde->kbte", normed[0], value_tangent)
    queries = projected[..., :hd]
    key_rows = projected[..., hd : 2 * hd]
    values = projected[..., 2 * hd :]
    values = jnp.concatenate([values[:1], values[1:] + extra_value])
    shape_heads = (streams, batch, tokens_here, heads, HEAD)
    queries = queries.astype(BF16).reshape(shape_heads)
    key_rows = key_rows.astype(BF16).reshape(shape_heads)
    values = values.astype(BF16).reshape(shape_heads)
    factor = HEAD ** (-0.5)
    scores = contract("bqhe,bkhe->bhqk", queries[0], key_rows[0]) * factor
    probs = jax.nn.softmax(scores, -1)
    dscores = (
        contract("sbqhe,bkhe->sbhqk", queries[1:], key_rows[0])
        + contract("bqhe,sbkhe->sbhqk", queries[0], key_rows[1:])
    ) * factor
    dprobs = probs * (dscores - jnp.sum(probs * dscores, -1, keepdims=True))
    probs_low = probs.astype(BF16)
    dprobs_low = dprobs.astype(BF16)
    attended_zero = contract("bhqk,bkhe->bqhe", probs_low, values[0])
    attended_rest = contract("sbhqk,bkhe->sbqhe", dprobs_low, values[0]) + contract(
        "bhqk,sbkhe->sbqhe", probs_low, values[1:]
    )
    attended = jnp.concatenate([attended_zero[None], attended_rest]).astype(BF16)
    attended = attended.reshape(streams, batch, tokens_here, hd)
    output = contract("sbte,ed->sbtd", attended, out_weight)
    extra_out = contract("bte,ked->kbtd", attended[0], out_tangent)
    output = jnp.concatenate([output[:1], output[1:] + extra_out])
    return (resid + output).astype(BF16)


def relay_shards(tokens, w_qkv, w_output, tangent_value, tangent_output, layer_gain, final_gain, head):
    full_qkv, full_output, full_value_tan, full_output_tan = (
        lax.all_gather(w_qkv, "dp", axis=1, tiled=True),
        lax.all_gather(w_output, "dp", axis=2, tiled=True),
        lax.all_gather(tangent_value, "dp", axis=2, tiled=True),
        lax.all_gather(tangent_output, "dp", axis=3, tiled=True),
    )
    tangents = tangent_value.shape[1]

    def advance_layer(state):
        return layer_step(
            state, full_qkv[0], full_output[0], full_value_tan[0], full_output_tan[0], layer_gain[0]
        )

    section_index = lax.axis_index("section")
    section_count = lax.axis_size("section")
    route = [(i, i + 1) for i in range(section_count - 1)]
    micro, _, toks, width = tokens.shape
    entering = jnp.concatenate(
        [tokens.reshape(1, micro, toks, width), jnp.zeros((tangents, micro, toks, width), BF16)]
    )

    def advance(step, outgoing):
        incoming = lax.ppermute(outgoing, "section", route)
        source = jnp.where(step == 0, entering, incoming)
        return lax.cond(section_index == step, advance_layer, jnp.zeros_like, source)

    finished = lax.fori_loop(0, section_count, advance, jnp.zeros_like(entering))
    collected = finished[:, :, 0, :]
    mine = section_index == section_count - 1
    features = lax.psum(jnp.where(mine, collected, jnp.zeros_like(collected)), "section")
    widened = features.astype(F32)
    final_zero, final_rest = norm_jvp(widened[0], widened[1:], final_gain)
    normed_final = jnp.concatenate([final_zero[None], final_rest]).astype(BF16)
    logits = contract("sbd,dc->sbc", normed_final, head)
    return (logits[0][:, None, :], jnp.sum(logits[1:] * logits[1:], 0)[:, None, :])


def dot(a, b):
    return lax.dot_general(a, b, (((1,), (0,)), ((), ())), preferred_element_type=F32)


def dot_t(a, b):
    return lax.dot_general(a, b, (((1,), (1,)), ((), ())), preferred_element_type=F32)


class Gather:
    def __init__(self, n, g, full, send, recv):
        self.nz = n // 4
        self.full, self.send, self.recv = full, send, recv
        self.rows = full.shape[1] // n
        self.g = g

    def remote(self, ref, target, sem, recv):
        return pltpu.make_async_remote_copy(
            src_ref=ref,
            dst_ref=ref,
            send_sem=self.send.at[sem],
            recv_sem=self.recv.at[recv],
            device_id={"section": self.g.section, "dp": target},
            device_id_type=MESH,
        )

    def half(self, src, half):
        depth = self.rows // 2
        return self.full.at[:, pl.ds(pl.multiple_of(src * self.rows + half * depth, depth), depth), :]

    def total(self, pieces):
        return self.full.at[:, pl.ds(0, pieces * self.rows), :]

    def line(self, plane, half):
        return 2 * plane + half

    def turn(self, plane, way):
        return 2 * self.nz + 2 * plane + way

    def forward(self, cond, src, half, target, sem, recv):
        def go():
            self.remote(self.half(src, half), target, sem, recv).start()

        go() if cond is None else pl.when(cond)(go)

    def arrived(self, src, half, recv):
        self.remote(self.half(src, half), self.g.me, 0, recv).wait_recv()

    def along(self, far):
        g, nz = self.g, self.nz
        for k in range(2, nz) if far else range(1, min(nz, 2)):
            for way in (k, -k):
                for half in range(2):
                    self.forward(g.reaches(way), g.me, half, g.me + 4 * way, 0, self.line(g.z, half))

    def pass_on(self, d):
        g = self.g
        for shift, cond in g.sources(d):
            passed = g.passes(shift)
            if passed is not None:
                src, plane = g.me + 4 * shift, g.z + shift
                for half in range(2):
                    pl.when(passed)(functools.partial(self.arrived, src, half, self.line(plane, half)))
                    target = g.me - 4 if shift > 0 else g.me + 4
                    self.forward(passed, src, half, target, 0, self.line(plane, half))

    def direct(self, d):
        g = self.g
        for shift, cond in g.sources(d):
            src, plane = g.me + 4 * shift, g.z + shift
            passed = g.passes(shift)
            for half in range(2):
                if d > 0:
                    fresh = cond if passed is None else cond & jnp.logical_not(passed)
                    pl.when(fresh)(functools.partial(self.arrived, src, half, self.line(plane, half)))
                for way in (1 - half, half):
                    recv = self.turn(plane, way) if way == half else 4 * self.nz
                    self.forward(cond, src, half, (g.x_near, g.y_near)[way], 1, recv)

    def relay(self, d):
        g = self.g
        for shift, cond in g.sources(d):
            for way, near, target in ((0, g.x_near, g.y_near), (1, g.y_near, g.x_near)):
                src = near + 4 * shift
                wait = functools.partial(self.arrived, src, way, self.turn(g.z + shift, way))
                wait() if cond is None else pl.when(cond)(wait)
                self.forward(cond, src, way, target, 1, 4 * self.nz)

    def rest(self):
        self.remote(self.total(2 * self.nz), self.g.me, 0, 4 * self.nz).wait_recv()

    def drain(self):
        if self.nz > 1:
            self.remote(self.total(self.nz - 1), self.g.me, 0, 0).wait_send()
        self.remote(self.total(3 * self.nz), self.g.me, 1, 0).wait_send()


class Place:
    def __init__(self, n):
        self.nz = n // 4
        self.me = lax.axis_index("dp")
        self.section = lax.axis_index("section")
        me = self.me
        self.x_near = me + 1 - 2 * (me % 2)
        self.y_near = me + 2 - 4 * ((me // 2) % 2)
        self.diagonal = self.x_near + self.y_near - me
        self.z = me // 4
        self.place = me % 4
        self.up, self.down = self.z + 1 < self.nz, self.z >= 1
        self.plane = (me, self.x_near, self.y_near, self.diagonal)

    def sources(self, d):
        if d == 0:
            return [(0, None)]
        return [(-d, self.z >= d), (d, self.z + d < self.nz)]

    def reaches(self, way):
        z, nz = self.z, self.nz
        there = z + way
        when = (there >= 0) & (there < nz)
        if abs(way) > 1:
            when = when & ((z == 0) | (z == nz - 1) | ((there > 0) & (there < nz - 1)))
        return when

    def passes(self, shift):
        z, nz = self.z, self.nz
        if not 0 < abs(shift) < nz - 2:
            return None
        return (z == 1) & (z + shift < nz - 1) if shift > 0 else (z == nz - 2) & (z + shift > 0)


def norm_rows(x, gains):
    average = jnp.mean(x, -1, keepdims=True)
    centred = x - average
    inverse = lax.rsqrt(jnp.mean(centred * centred, -1, keepdims=True) + epsilon)
    return centred, inverse, centred * inverse * gains


def norm_tangent(t, centred, inverse, gains):
    dcentred = t - jnp.mean(t, -1, keepdims=True)
    dinverse = -(inverse * inverse * inverse) * jnp.mean(centred * dcentred, -1, keepdims=True)
    return (dcentred * inverse + centred * dinverse) * gains


def softmax(scores):
    e = jnp.exp(scores - jnp.max(scores, -1, keepdims=True))
    return e / jnp.sum(e, -1, keepdims=True)


def at_rows(i, count):
    return pl.ds(pl.multiple_of(i * count, count), count)


def first_norm(sizes, tok, gain, normed, slot):
    micro, toks, width, hd, tangents = sizes
    for b in range(micro):
        x = tok[slot, pl.ds(b * toks, toks), :].astype(F32)
        normed[at_rows(slot * micro + b, toks), :] = norm_rows(x, gain)[2].astype(BF16)


def first_attend(sizes, acc, att, slot, b):
    micro, toks, width, hd, tangents = sizes
    factor = HEAD ** (-0.5)
    part = 2 * HEAD
    streams = 1 + tangents
    even = lax.broadcasted_iota(jnp.int32, (toks, part), 1) < HEAD
    rows = at_rows(slot * micro + b, toks)
    q = acc[rows, pl.ds(0, part)]
    k = acc[rows, pl.ds(part, part)].astype(BF16)
    v = acc[rows, pl.ds(2 * part, streams * part)].astype(BF16)
    zero = jnp.zeros_like(q)
    both = jnp.concatenate([jnp.where(even, q, zero), jnp.where(even, zero, q)], 0).astype(BF16)
    scores = dot_t(both, k) * factor
    low = jnp.exp(scores - jnp.max(scores, -1, keepdims=True)).astype(BF16)
    out = dot(low, jnp.concatenate([v, jnp.ones((toks, part), BF16)], 1))

    def joined(s):
        at = slice(s * part, (s + 1) * part)
        return jnp.where(even, out[:toks, at], out[toks:, at])

    scale = 1.0 / joined(streams)
    for s in range(streams):
        att[slot, pl.ds((s * micro + b) * toks, toks), :] = (joined(s) * scale).astype(BF16)


def class_attend(sizes, acc):
    micro, toks, width, hd, tangents = sizes
    factor = HEAD ** (-0.5)
    part = 2 * HEAD
    streams = 1 + tangents
    images = acc.shape[0] // toks
    even = lax.broadcasted_iota(jnp.int32, (images, part), 1) < HEAD
    q = jnp.concatenate([acc[pl.ds(i * toks, 8), pl.ds(0, part)][:1] for i in range(images)], 0)
    zero = jnp.zeros_like(q)
    both = jnp.concatenate([jnp.where(even, q, zero), jnp.where(even, zero, q)], 0).astype(BF16)
    k = acc[:, pl.ds(part, part)].astype(BF16)
    v = acc[:, pl.ds(2 * part, streams * part)].astype(BF16)
    scores = dot_t(both, k) * factor
    image = lax.broadcasted_iota(jnp.int32, scores.shape, 0) % images
    own = lax.broadcasted_iota(jnp.int32, scores.shape, 1) // toks == image
    scores = jnp.where(own, scores, -jnp.inf)
    low = jnp.exp(scores - jnp.max(scores, -1, keepdims=True)).astype(BF16)
    out = dot(low, jnp.concatenate([v, jnp.ones((acc.shape[0], part), BF16)], 1))

    def joined(s):
        at = slice(s * part, (s + 1) * part)
        return jnp.where(even, out[:images, at], out[images:, at])

    scale = 1.0 / joined(streams)
    parts = [joined(s) * scale for s in range(streams)]
    blank = jnp.zeros((group_of(sizes) - micro * streams, part), F32)
    rows = []
    for p in range(images // micro):
        rows += [x[p * micro : (p + 1) * micro] for x in parts] + [blank] * (blank.shape[0] > 0)
    return jnp.concatenate(rows, 0).astype(BF16)


def first_out(sizes, tok, place, b_full, att, state):
    micro, toks, width, hd, tangents = sizes
    rows0 = micro * toks
    tile = 256
    for c in range(width // tile):
        at = pl.ds(c * tile, tile)
        out = dot_t(att[...], b_full[0, at, :])
        extra = [dot_t(att[pl.ds(0, rows0), :], b_full[1 + j, at, :]) for j in range(tangents)]
        x = tok[place, :, at].astype(F32)
        state[pl.ds(0, rows0), at] = (x + out[:rows0]).astype(BF16)
        for j in range(tangents):
            state[pl.ds((1 + j) * rows0, rows0), at] = (
                out[(1 + j) * rows0 : (2 + j) * rows0] + extra[j]
            ).astype(BF16)


def group_of(sizes):
    micro, toks, width, hd, tangents = sizes
    return -(-micro * (1 + tangents) // 8) * 8


def stream_of(sizes, shape):
    return (lax.broadcasted_iota(jnp.int32, shape, 0) % group_of(sizes)) // sizes[0]


def lowered(sizes, parts):
    micro, tangents = sizes[0], sizes[4]
    stream = stream_of(sizes, parts[0].shape)
    total = parts[0]
    for j in range(tangents):
        moved = pltpu.roll(parts[1 + j], micro * (1 + j), 0)
        total = total + jnp.where(stream == 1 + j, moved, jnp.zeros_like(moved))
    return total


def primal_rows(sizes, x):
    micro, tangents = sizes[0], sizes[4]
    stream = stream_of(sizes, x.shape)
    spread = x
    for j in range(tangents):
        spread = jnp.where(stream == 1 + j, pltpu.roll(x, micro * (1 + j), 0), spread)
    return spread


def norm_group(sizes, x, gains):
    stream = stream_of(sizes, x.shape)
    centred, inverse, y = norm_rows(primal_rows(sizes, x), gains)
    dy = norm_tangent(x, centred, inverse, gains)
    return jnp.where(stream == 0, y, dy).astype(BF16)


def class_rows(sizes, state):
    micro, toks, width, hd, tangents = sizes
    streams = 1 + tangents
    rows = [
        state[pl.ds((s * micro + b) * toks, 16), :].astype(F32)[:1] for s in range(streams) for b in range(micro)
    ]
    return jnp.concatenate(rows + [jnp.zeros((group_of(sizes) - micro * streams, width), F32)], 0)


def last_norm(sizes, gain, state, normed):
    micro, toks, width, hd, tangents = sizes
    rows0 = micro * toks
    for b in range(micro):
        at = pl.ds(b * toks, toks)
        centred, inverse, y = norm_rows(state[at, :].astype(F32), gain)
        normed[0, at, :] = y.astype(BF16)
        for j in range(tangents):
            t = state[pl.ds((1 + j) * rows0 + b * toks, toks), :].astype(F32)
            normed[1 + j, at, :] = norm_tangent(t, centred, inverse, gain).astype(BF16)


def last_attend(sizes, u, normed):
    micro, toks, width, hd, tangents = sizes
    factor = HEAD ** (-0.5)
    shape = (u.shape[0], micro * toks)
    stream = stream_of(sizes, shape)
    image = (lax.broadcasted_iota(jnp.int32, shape, 0) % group_of(sizes)) % micro
    valid = lax.broadcasted_iota(jnp.int32, shape, 1) // toks == image
    parts = [dot_t(u, normed[s]) * factor for s in range(1 + tangents)]
    probs = softmax(jnp.where(valid, parts[0], -jnp.inf))
    weights = primal_rows(sizes, probs)
    scores = lowered(sizes, parts)
    dprobs = weights * (scores - jnp.sum(weights * scores, -1, keepdims=True))
    zero = jnp.zeros_like(weights)
    total = dot(jnp.where(stream == 0, weights, dprobs).astype(BF16), normed[0])
    for j in range(tangents):
        total = total + dot(jnp.where(stream == 1 + j, weights, zero).astype(BF16), normed[1 + j])
    return total.astype(BF16)


TOK, TOKY, TOKD, LA, LB, ATT, ATC, CLS, U, M, O1, O0, GAIN, FIRST, EARLY, STAGES = range(16)


def kernel(
    n, sizes, tokens, w_qkv, tangent_value, w_out, t_out, gain_in, final_in, head_in, logit_ref,
    a_stage, b_stage, a0, a1, b1, b_full, tok, normed_all, acc, att_out, att_in, state, normed,
    gains, final_gain, head, atc_out, atc_all, atc_in, cls_out, cls_in, cls_all, u_out, u_all, m_out, m_all, o_out, o_all, classes,
    loads, line, a_send, a_recv, stage_send, stage_recv, far_send, far_recv, b_send, b_recv,
):
    micro, toks, width, hd, tangents = sizes
    streams = 1 + tangents
    part = hd // 4
    share = part // HEAD
    g = Place(n)
    me, section, place, z, nz = g.me, g.section, g.place, g.z, g.nz
    other = 1 - section
    rows = width // n
    slab = 4 * rows
    group = group_of(sizes)
    own = at_rows(me, rows)

    barrier = pltpu.get_barrier_semaphore()

    def greet(target, sec):
        pl.semaphore_signal(
            barrier, inc=1, device_id={"section": sec, "dp": target}, device_id_type=MESH
        )

    pl.when(g.up)(lambda: greet(me + 4, section))
    pl.when(g.down)(lambda: greet(me - 4, section))
    for near in (g.diagonal, g.x_near, g.y_near):
        greet(near, section)
        greet(near, other)
    greet(me, other)

    def met():
        if nz > 1:
            middle = g.up & g.down
            pl.when(middle)(lambda: pl.semaphore_wait(barrier, 9))
            pl.when(jnp.logical_not(middle))(lambda: pl.semaphore_wait(barrier, 8))
        else:
            pl.semaphore_wait(barrier, 7)

    def column(p):
        return pl.ds(p * part, part) if isinstance(p, int) else at_rows(p, part)

    def load(i, src, dst):
        return pltpu.make_async_copy(src, dst, loads.at[i])

    def stage_loads():
        for p in range(4):
            for m in range(3):
                load(5, w_qkv.at[:, pl.ds(m * hd + p * part, part)], a_stage.at[p, :, pl.ds(m * part, part)]).start()
            for j in range(tangents):
                load(
                    5,
                    tangent_value.at[j, :, pl.ds(p * part, part)],
                    a_stage.at[p, :, pl.ds((3 + j) * part, part)],
                ).start()

    def own_loads():
        for m in range(3):
            load(6, w_qkv.at[:, column(m * 4 + place)], a1.at[own, pl.ds(m * part, part)]).start()
        for j in range(tangents):
            load(6, tangent_value.at[j, :, column(place)], a1.at[own, pl.ds((3 + j) * part, part)]).start()
        load(7, w_out.at[:, column(place)], b1.at[0, own, :]).start()
        load(7, t_out.at[:, :, column(place)], b1.at[pl.ds(1, tangents), own, :]).start()
        for p in range(4):
            load(8, w_out.at[:, pl.ds(p * part, part)], b_stage.at[p, 0]).start()
            load(8, t_out.at[:, :, pl.ds(p * part, part)], b_stage.at[p, pl.ds(1, tangents)]).start()

    def b_loads():
        load(4, w_out, b_full.at[0, own, :]).start()
        load(4, t_out, b_full.at[pl.ds(1, tangents), own, :]).start()

    def loaded(i, ref):
        load(i, ref, ref).wait()

    def gain_load():
        return load(0, gain_in, gains.at[section])

    def tok_load():
        return load(1, tokens, tok.at[place])

    def tail_loads():
        return [load(2, head_in, head), load(3, final_in, final_gain)]

    stage_loads()
    gain_load().start()
    tok_load().start()
    pl.when(section == 0)(b_loads)
    pl.when(section == 1)(own_loads)
    for move in tail_loads():
        move.start()
    met()

    def tell(way, level, target):
        pl.semaphore_signal(
            line.at[way, level], inc=1, device_id={"section": section, "dp": target}, device_id_type=MESH
        )

    if nz > 2:

        @pl.when(g.up & g.down)
        def _():
            tell(0, 1, me + 4)
            tell(1, 1, me - 4)

    def far_met():
        for level in range(1, nz - 1):

            @pl.when(z - 1 - level >= 0)
            def _():
                pl.semaphore_wait(line.at[0, level], 1)
                if level + 1 < nz - 1:
                    pl.when(g.up)(lambda: tell(0, level + 1, me + 4))

            @pl.when(z + 1 + level < nz)
            def _():
                pl.semaphore_wait(line.at[1, level], 1)
                if level + 1 < nz - 1:
                    pl.when(g.down)(lambda: tell(1, level + 1, me - 4))


    def xfer(stage, src, dst, target, sec):
        return pltpu.make_async_remote_copy(
            src_ref=src,
            dst_ref=dst,
            send_sem=stage_send.at[stage],
            recv_sem=stage_recv.at[stage],
            device_id={"section": sec, "dp": target},
            device_id_type=MESH,
        )

    def arrived(stage, ref):
        xfer(stage, ref, ref, me, other).wait_recv()

    sent = []

    FAR = (3, 1, 2, 0)

    def scatter(stage, src, dst, sec, total, skip_own=False):
        for i in FAR:
            if i > 0 or not skip_own:
                target = g.plane[i]
                xfer(stage, src(target % 4), dst, target, sec).start()
        sent.append((stage, total))

    def drain():
        for stage, ref in sent:
            xfer(stage, ref, ref, me, other).wait_send()
        sent.clear()

    def a_ref(src):
        return a0.at[at_rows(src, rows), :]

    def a_copy(src_ref, src, sem, target, sec):
        return pltpu.make_async_remote_copy(
            src_ref=src_ref,
            dst_ref=a_ref(src),
            send_sem=sem,
            recv_sem=a_recv.at[src],
            device_id={"section": sec, "dp": target},
            device_id_type=MESH,
        )

    @pl.when(section == 0)
    def _():
        loaded(5, a_stage)
        for i in range(4):
            target = g.plane[i]
            a_copy(a_stage.at[target % 4], me, stage_send.at[FIRST], target, other).start()
        sent.append((FIRST, a_stage))
        gain_load().wait()
        xfer(GAIN, gains.at[section], gains.at[section], me, other).start()
        sent.append((GAIN, gains.at[section]))
        loaded(4, b_full.at[:, own, :])
        gather = Gather(n, g, b_full, b_send, b_recv)
        lag = 2
        gather.along(False)
        for d in range(nz + lag):
            if d < nz:
                gather.pass_on(d)
                gather.direct(d)
                if d == 0:
                    far_met()
                    gather.along(True)
            if d >= lag:
                gather.relay(d - lag)
        tok_load().wait()
        gather.rest()
        arrived(ATC, atc_in)
        cls_out[...] = lowered(sizes, [dot_t(atc_in[...], b_full[s]) for s in range(streams)])
        xfer(CLS, cls_out, cls_in, me, other).start()
        sent.append((CLS, cls_out))
        arrived(ATT, att_in)
        first_out(sizes, tok, place, b_full, att_in, state)
        arrived(GAIN, gains.at[other])
        last_norm(sizes, gains[1], state, normed)
        arrived(U, u_all)
        u = jnp.concatenate([u_all[p] for p in range(4)], 0)
        m = last_attend(sizes, u, normed)
        for p in range(4):
            m_out[p] = m[p * share * group : (p + 1) * share * group]
        scatter(M, lambda p: m_out.at[p], m_all.at[place], other, m_out)
        classes[...] = class_rows(sizes, state)
        gather.drain()
        drain()
        arrived(O0, o_all)

    @pl.when(section == 1)
    def _():
        gain_load().wait()
        xfer(GAIN, gains.at[section], gains.at[section], me, other).start()
        sent.append((GAIN, gains.at[section]))
        tok_load().wait()

        def relay(d, some=g.plane):
            for near in some:
                for shift, cond in g.sources(d)[::-1]:

                    def step():
                        src = near + 4 * shift
                        a_copy(a_ref(src), src, a_send.at[d, 0], me, section).wait_recv()
                        if shift >= 0 and d < nz - 1:
                            pl.when(g.down)(
                                lambda: a_copy(a_ref(src), src, a_send.at[d, 1], me - 4, section).start()
                            )
                        if shift <= 0 and d < nz - 1:
                            pl.when(g.up)(
                                lambda: a_copy(a_ref(src), src, a_send.at[d, 0], me + 4, section).start()
                            )

                    step() if cond is None else pl.when(cond)(step)

        def relay_end(d):
            slab_ref = a0.at[pl.ds(0, slab), :]
            for shift, cond in g.sources(d):

                def end(way):
                    pltpu.make_async_remote_copy(
                        src_ref=slab_ref,
                        dst_ref=slab_ref,
                        send_sem=a_send.at[d, way],
                        recv_sem=a_recv.at[0],
                        device_id={"section": section, "dp": me},
                        device_id_type=MESH,
                    ).wait_send()

                if shift <= 0:
                    pl.when(g.up if cond is None else cond & g.up)(functools.partial(end, 0))
                if shift >= 0:
                    pl.when(g.down if cond is None else cond & g.down)(functools.partial(end, 1))

        def project(d):
            for shift, cond in g.sources(d):

                def step(shift=shift):
                    at = at_rows(z + shift, slab)
                    term = dot(normed_all[:, at], a0[at, :])
                    acc[...] = term if d == 0 else acc[...] + term

                step() if cond is None else pl.when(cond)(step)

        loaded(7, b1.at[:, own, :])
        early = b1.at[:, pl.ds(0, (nz - 1) * rows), :]

        def ahead(k):
            for way in (k, -k):
                there = (z + way >= 0) & (z + way < nz)

                def go():
                    xfer(EARLY, b1.at[:, own, :], b1.at[:, own, :], me + 4 * way, section).start()

                pl.when(there)(go)

        if nz > 1:
            ahead(1)
        if nz > 1:
            sent.append((EARLY, early))
        relay(0, g.plane[:1])
        for stage, near in ((TOK, g.x_near), (TOKY, g.y_near)):
            xfer(stage, tok.at[place], tok.at[place], near, section).start()
            sent.append((stage, tok.at[place]))
        loaded(5, a_stage)
        loaded(6, a1.at[own, :])
        scatter(LA, lambda p: a_stage.at[p], a1.at[own, :], section, a_stage.at[pl.ds(0, 3)], True)
        far_met()
        for k in range(2, nz):
            ahead(k)
        relay(0, g.plane[1:])
        arrived(GAIN, gains.at[other])
        first_norm(sizes, tok, gains[0], normed_all, place)
        relay(1)
        half = micro * toks // 2
        for stage, near, target, first in ((TOK, g.x_near, g.y_near, 0), (TOKY, g.y_near, g.x_near, half)):
            arrived(stage, tok.at[near % 4])
            piece = tok.at[near % 4, pl.ds(first, half), :]
            xfer(TOKD, piece, piece, target, section).start()
        sent.append((TOKD, tok.at[0]))
        loaded(8, b_stage)
        scatter(LB, lambda p: b_stage.at[p], b1.at[:, own, :], section, b_stage.at[pl.ds(0, 3)], True)

        def far_refs(kind, zc):
            at = at_rows(zc, slab)
            if kind == 0:
                return [a1.at[at, pl.ds(0, 2 * part)]]
            if kind == 1:
                return [a1.at[at, pl.ds(2 * part, streams * part)]]
            return [b1.at[:, at_rows(near + 4 * (zc - z), rows), :] for near in g.plane[1:]]

        def far_total(kind):
            return far_refs(kind, 0)[0] if kind < 2 else b1.at[:, pl.ds(0, 3 * rows), :]

        def far_copy(ref, kind, zc, target):
            return pltpu.make_async_remote_copy(
                src_ref=ref,
                dst_ref=ref,
                send_sem=far_send.at[kind],
                recv_sem=far_recv.at[kind, zc],
                device_id={"section": section, "dp": target},
                device_id_type=MESH,
            )

        def far_moves(kind):
            for k in range(1, nz):
                for way in (k, -k):
                    yield g.reaches(way), None, z, me + 4 * way
            for k in range(1, nz - 2):
                for way in (k, -k):
                    yield g.passes(way), way, z + way, me - 4 if way > 0 else me + 4

        def far_start(kind):
            for when, way, zc, target in far_moves(kind):

                def go():
                    for ref in far_refs(kind, zc):
                        far_copy(ref, kind, zc, target).start()

                if way is None:
                    pl.when(when)(go)

        def far_pass(kind):
            for when, way, zc, target in far_moves(kind):

                def step():
                    far_copy(far_total(kind), kind, zc, me).wait_recv()
                    for ref in far_refs(kind, zc):
                        far_copy(ref, kind, zc, target).start()

                if way is not None:
                    pl.when(when)(step)

        def far_wait(kind):
            for k in range(1, nz):
                for way in (k, -k):
                    there = z + way
                    when = (there >= 0) & (there < nz)
                    if g.passes(way) is not None:
                        when = when & jnp.logical_not(g.passes(way))
                    pl.when(when)(lambda: far_copy(far_total(kind), kind, there, me).wait_recv())

        def far_end(kind):
            count = nz - 1
            if kind < 2:
                first, last = ((0, 2), (2, 2 + streams))[kind]
                ref = a1.at[pl.ds(0, count * slab), pl.ds(first * part, (last - first) * part)]
            else:
                ref = b1.at[:, pl.ds(0, count * 3 * rows), :]
            if count > 0:
                far_copy(ref, kind, 0, me).wait_send()

        def far_begin():
            arrived(LA, a1.at[pl.ds(0, 3 * rows), :])
            far_start(0)
            far_start(1)

        for near in (g.x_near, g.y_near):
            first_norm(sizes, tok, gains[0], normed_all, near % 4)
        for d in range(2, nz - 1):
            relay(d)
        far_begin()
        arrived(TOKD, tok.at[g.diagonal % 4])
        first_norm(sizes, tok, gains[0], normed_all, g.diagonal % 4)
        for d in range(nz - 1):
            project(d)
        if nz > 2:
            relay(nz - 1)
        project(nz - 1)
        atc_out[...] = class_attend(sizes, acc)
        scatter(ATC, lambda p: atc_out, atc_in.at[:, column(place)], other, atc_all)

        def give(i):
            target = g.plane[i]
            xfer(ATT, att_out.at[target % 4], att_in.at[:, column(place)], target, other).start()

        for i in FAR:
            for b in range(micro):
                first_attend(sizes, acc, att_out, g.plane[i] % 4, b)
            if i == FAR[1]:
                arrived(LB, b1.at[:, pl.ds(0, 3 * rows), :])
                far_start(2)
        far_pass(0)
        for i in FAR:
            give(i)
        sent.append((ATT, att_out))
        fresh = []
        blank = jnp.zeros((group - micro, width), F32)
        for p in range(4):
            fresh += [tok[p, pl.ds(b * toks, 16), :].astype(F32)[:1] for b in range(micro)] + [blank]
        fresh = jnp.concatenate(fresh, 0)
        far_wait(0)
        arrived(CLS, cls_in)
        x = (fresh + cls_in[...]).astype(BF16).astype(F32)
        for p in range(4):
            cls_all[p] = x[p * group : (p + 1) * group]
        q = dot(norm_group(sizes, x, gains[1]), a1[:, pl.ds(0, part)]).astype(BF16).astype(F32)
        owner = lax.broadcasted_iota(jnp.int32, (group, part), 1) // HEAD
        zero = jnp.zeros((group, part), F32)
        spread = [
            jnp.where(owner == h, q[p * group : (p + 1) * group], zero) for p in range(4) for h in range(share)
        ]
        u = dot_t(jnp.concatenate(spread, 0).astype(BF16), a1[:, pl.ds(part, part)]).astype(BF16)
        tall = share * group
        for p in range(4):
            u_out[p] = u[p * tall : (p + 1) * tall]
        scatter(U, lambda p: u_out.at[p], u_all.at[place], other, u_out)
        far_pass(1)
        far_pass(2)
        far_wait(1)
        arrived(M, m_all)
        m = jnp.concatenate([m_all[p] for p in range(4)], 0)
        r = dot(m, a1[:, pl.ds(2 * part, streams * part)])
        mixed = lowered(sizes, [r[:, s * part : (s + 1) * part] for s in range(streams)])
        chosen = []
        for p in range(4):
            block = zero
            for h in range(share):
                at = p * tall + h * group
                block = jnp.where(owner == h, mixed[at : at + group], block)
            chosen.append(block)
        attended = jnp.concatenate(chosen, 0).astype(BF16)
        far_wait(2)
        if nz > 1:
            arrived(EARLY, early)
        out = lowered(sizes, [dot_t(attended, b1[s]) for s in range(streams)])
        for p in range(4):
            o_out[p] = out[p * group : (p + 1) * group].astype(BF16)
        scatter(O0, lambda p: o_out.at[p], o_all.at[place], other, o_out)
        scatter(O1, lambda p: o_out.at[p], o_all.at[place], section, o_out.at[pl.ds(0, 3)], True)
        o_all[place] = o_out[place]
        classes[...] = cls_all[place]
        for d in range(nz - 1):
            relay_end(d)
        for kind in range(3):
            far_end(kind)
        drain()
        arrived(O1, o_all.at[pl.ds(0, 3)])

    for move in tail_loads():
        move.wait()
    total = sum(o_all[p].astype(F32) for p in range(4))
    final = (classes[...] + total).astype(BF16).astype(F32)
    features = norm_group(sizes, final, final_gain[...])
    logits = dot_t(features, head[...])
    for s in range(streams):
        logit_ref[s, :, 0, :] = logits[s * micro : (s + 1) * micro]


def two_sections(n):
    def shards(tokens, w_qkv, w_output, tangent_value, tangent_output, layer_gain, final_gain, head):
        micro, _, toks, width = tokens.shape
        tangents = tangent_value.shape[1]
        hd = w_output.shape[1]
        count = head.shape[1]
        rows = width // n
        part = hd // 4
        nz = n // 4
        sizes = (micro, toks, width, hd, tangents)
        streams = 1 + tangents
        rows0 = micro * toks
        group = group_of(sizes)
        tall = part // HEAD * group
        vmem = pl.BlockSpec(memory_space=pltpu.VMEM)
        anywhere = pl.BlockSpec(memory_space=pl.ANY)
        dma = pltpu.SemaphoreType.DMA
        logits = pl.pallas_call(
            functools.partial(kernel, n, sizes),
            out_shape=pltpu.VMEM((streams, micro, 1, count), F32),
            in_specs=[anywhere] * 8,
            out_specs=vmem,
            scratch_shapes=[
                pltpu.VMEM((4, rows, (2 + streams) * part), BF16),
                pltpu.VMEM((4, streams, rows, part), BF16),
                pltpu.VMEM((width, (2 + streams) * part), BF16),
                pltpu.VMEM((width, (2 + streams) * part), BF16),
                pltpu.VMEM((streams, width, part), BF16),
                pltpu.VMEM((streams, width, hd), BF16),
                pltpu.VMEM((4, rows0, width), BF16),
                pltpu.VMEM((4 * rows0, width), BF16),
                pltpu.VMEM((4 * rows0, (2 + streams) * part), F32),
                pltpu.VMEM((4, streams * rows0, part), BF16),
                pltpu.VMEM((streams * rows0, hd), BF16),
                pltpu.VMEM((streams * rows0, width), BF16),
                pltpu.VMEM((streams, rows0, width), BF16),
                pltpu.VMEM((2, 1, width), F32),
                pltpu.VMEM((1, width), F32),
                pltpu.VMEM((count, width), BF16),
                pltpu.VMEM((4 * group, part), BF16),
                pltpu.VMEM((16 * group, part), BF16),
                pltpu.VMEM((4 * group, hd), BF16),
                pltpu.VMEM((4 * group, width), F32),
                pltpu.VMEM((4 * group, width), F32),
                pltpu.VMEM((4, group, width), F32),
                pltpu.VMEM((4, tall, width), BF16),
                pltpu.VMEM((4, tall, width), BF16),
                pltpu.VMEM((4, tall, width), BF16),
                pltpu.VMEM((4, tall, width), BF16),
                pltpu.VMEM((4, group, width), BF16),
                pltpu.VMEM((4, group, width), BF16),
                pltpu.VMEM((group, width), F32),
                dma((9,)),
                pltpu.SemaphoreType.REGULAR((2, max(nz - 1, 1))),
                dma((nz, 2)),
                dma((n,)),
                dma((STAGES,)),
                dma((STAGES,)),
                dma((3,)),
                dma((3, nz)),
                dma((2,)),
                dma((4 * nz + 1,)),
            ],
            compiler_params=pltpu.CompilerParams(
                collective_id=0, has_side_effects=True, vmem_limit_bytes=63 * 2**20
            ),
        )(
            tokens.reshape(rows0, width),
            w_qkv[0],
            tangent_value[0],
            jnp.swapaxes(w_output[0], 0, 1),
            jnp.swapaxes(tangent_output[0], 1, 2),
            layer_gain,
            final_gain[None],
            head.T,
        )
        return logits[0], sum(logits[1 + j] * logits[1 + j] for j in range(tangents))

    return shards


def solution(mesh):
    n = mesh.shape["dp"]
    fast = mesh.shape["section"] == 2 and n % 4 == 0 and n // 4 <= 4
    return jax.shard_map(
        two_sections(n) if fast else relay_shards,
        mesh=mesh,
        in_specs=(
            P(None, "dp", None, None),
            P("section", "dp", None),
            P("section", None, "dp"),
            P("section", None, "dp", None),
            P("section", None, None, "dp"),
            P("section", None),
            P(),
            P(None, "section"),
        ),
        out_specs=(P(None, "dp", "section"), P(None, "dp", "section")),
        check_vma=False,
    )
```

```python
import functools

import jax
import jax.numpy as jnp
from jax import lax
from jax.experimental import pallas as pl
from jax.experimental.pallas import tpu as pltpu
from jax.sharding import PartitionSpec as P

HEAD = 64
epsilon = 1e-06
F32, BF16 = jnp.float32, jnp.bfloat16
MESH = pl.DeviceIdType.MESH


def contract(spec, left, right):
    return jnp.einsum(spec, left, right, preferred_element_type=jnp.float32)


def norm_jvp(primal, tangents, gains):
    average = jnp.mean(primal, -1, keepdims=True)
    centred = primal - average
    inverse = lax.rsqrt(jnp.mean(centred * centred, -1, keepdims=True) + epsilon)
    dcentred = tangents - jnp.mean(tangents, -1, keepdims=True)
    dinverse = -(inverse**3) * jnp.mean(centred * dcentred, -1, keepdims=True)
    return (centred * inverse * gains, (dcentred * inverse + centred * dinverse) * gains)


def layer_step(state, qkv_weight, out_weight, value_tangent, out_tangent, gains):
    hd = out_weight.shape[0]
    heads = hd // HEAD
    resid = state.astype(F32)
    normed_zero, normed_rest = norm_jvp(resid[0], resid[1:], gains)
    normed = jnp.concatenate([normed_zero[None], normed_rest]).astype(BF16)
    streams, batch, tokens_here, width = normed.shape
    projected = contract("sbtd,de->sbte", normed, qkv_weight)
    extra_value = contract("btd,kde->kbte", normed[0], value_tangent)
    queries = projected[..., :hd]
    key_rows = projected[..., hd : 2 * hd]
    values = projected[..., 2 * hd :]
    values = jnp.concatenate([values[:1], values[1:] + extra_value])
    shape_heads = (streams, batch, tokens_here, heads, HEAD)
    queries = queries.astype(BF16).reshape(shape_heads)
    key_rows = key_rows.astype(BF16).reshape(shape_heads)
    values = values.astype(BF16).reshape(shape_heads)
    factor = HEAD ** (-0.5)
    scores = contract("bqhe,bkhe->bhqk", queries[0], key_rows[0]) * factor
    probs = jax.nn.softmax(scores, -1)
    dscores = (
        contract("sbqhe,bkhe->sbhqk", queries[1:], key_rows[0])
        + contract("bqhe,sbkhe->sbhqk", queries[0], key_rows[1:])
    ) * factor
    dprobs = probs * (dscores - jnp.sum(probs * dscores, -1, keepdims=True))
    probs_low = probs.astype(BF16)
    dprobs_low = dprobs.astype(BF16)
    attended_zero = contract("bhqk,bkhe->bqhe", probs_low, values[0])
    attended_rest = contract("sbhqk,bkhe->sbqhe", dprobs_low, values[0]) + contract(
        "bhqk,sbkhe->sbqhe", probs_low, values[1:]
    )
    attended = jnp.concatenate([attended_zero[None], attended_rest]).astype(BF16)
    attended = attended.reshape(streams, batch, tokens_here, hd)
    output = contract("sbte,ed->sbtd", attended, out_weight)
    extra_out = contract("bte,ked->kbtd", attended[0], out_tangent)
    output = jnp.concatenate([output[:1], output[1:] + extra_out])
    return (resid + output).astype(BF16)


def relay_shards(tokens, w_qkv, w_output, tangent_value, tangent_output, layer_gain, final_gain, head):
    full_qkv, full_output, full_value_tan, full_output_tan = (
        lax.all_gather(w_qkv, "dp", axis=1, tiled=True),
        lax.all_gather(w_output, "dp", axis=2, tiled=True),
        lax.all_gather(tangent_value, "dp", axis=2, tiled=True),
        lax.all_gather(tangent_output, "dp", axis=3, tiled=True),
    )
    tangents = tangent_value.shape[1]

    def advance_layer(state):
        return layer_step(
            state, full_qkv[0], full_output[0], full_value_tan[0], full_output_tan[0], layer_gain[0]
        )

    section_index = lax.axis_index("section")
    section_count = lax.axis_size("section")
    route = [(i, i + 1) for i in range(section_count - 1)]
    micro, _, toks, width = tokens.shape
    entering = jnp.concatenate(
        [tokens.reshape(1, micro, toks, width), jnp.zeros((tangents, micro, toks, width), BF16)]
    )

    def advance(step, outgoing):
        incoming = lax.ppermute(outgoing, "section", route)
        source = jnp.where(step == 0, entering, incoming)
        return lax.cond(section_index == step, advance_layer, jnp.zeros_like, source)

    finished = lax.fori_loop(0, section_count, advance, jnp.zeros_like(entering))
    collected = finished[:, :, 0, :]
    mine = section_index == section_count - 1
    features = lax.psum(jnp.where(mine, collected, jnp.zeros_like(collected)), "section")
    widened = features.astype(F32)
    final_zero, final_rest = norm_jvp(widened[0], widened[1:], final_gain)
    normed_final = jnp.concatenate([final_zero[None], final_rest]).astype(BF16)
    logits = contract("sbd,dc->sbc", normed_final, head)
    return (logits[0][:, None, :], jnp.sum(logits[1:] * logits[1:], 0)[:, None, :])


def dot(a, b):
    return lax.dot_general(a, b, (((1,), (0,)), ((), ())), preferred_element_type=F32)


def dot_t(a, b):
    return lax.dot_general(a, b, (((1,), (1,)), ((), ())), preferred_element_type=F32)


class Gather:
    def __init__(self, n, g, full, send, recv):
        self.nz = n // 4
        self.full, self.send, self.recv = full, send, recv
        self.rows = full.shape[1] // n
        self.g = g

    def remote(self, ref, target, sem, recv):
        return pltpu.make_async_remote_copy(
            src_ref=ref,
            dst_ref=ref,
            send_sem=self.send.at[sem],
            recv_sem=self.recv.at[recv],
            device_id={"section": self.g.section, "dp": target},
            device_id_type=MESH,
        )

    def half(self, src, half):
        depth = self.rows // 2
        return self.full.at[:, pl.ds(pl.multiple_of(src * self.rows + half * depth, depth), depth), :]

    def total(self, pieces):
        return self.full.at[:, pl.ds(0, pieces * self.rows), :]

    def line(self, plane, half):
        return 2 * plane + half

    def turn(self, plane, way):
        return 2 * self.nz + 2 * plane + way

    def forward(self, cond, src, half, target, sem, recv):
        def go():
            self.remote(self.half(src, half), target, sem, recv).start()

        go() if cond is None else pl.when(cond)(go)

    def arrived(self, src, half, recv):
        self.remote(self.half(src, half), self.g.me, 0, recv).wait_recv()

    def along(self, far):
        g, nz = self.g, self.nz
        for k in range(2, nz) if far else range(1, min(nz, 2)):
            for way in (k, -k):
                for half in range(2):
                    self.forward(g.reaches(way), g.me, half, g.me + 4 * way, 0, self.line(g.z, half))

    def pass_on(self, d):
        g = self.g
        for shift, cond in g.sources(d):
            passed = g.passes(shift)
            if passed is not None:
                src, plane = g.me + 4 * shift, g.z + shift
                for half in range(2):
                    pl.when(passed)(functools.partial(self.arrived, src, half, self.line(plane, half)))
                    target = g.me - 4 if shift > 0 else g.me + 4
                    self.forward(passed, src, half, target, 0, self.line(plane, half))

    def direct(self, d):
        g = self.g
        for shift, cond in g.sources(d):
            src, plane = g.me + 4 * shift, g.z + shift
            passed = g.passes(shift)
            for half in range(2):
                if d > 0:
                    fresh = cond if passed is None else cond & jnp.logical_not(passed)
                    pl.when(fresh)(functools.partial(self.arrived, src, half, self.line(plane, half)))
                for way in (1 - half, half):
                    recv = self.turn(plane, way) if way == half else 4 * self.nz
                    self.forward(cond, src, half, (g.x_near, g.y_near)[way], 1, recv)

    def relay(self, d):
        g = self.g
        for shift, cond in g.sources(d):
            for way, near, target in ((0, g.x_near, g.y_near), (1, g.y_near, g.x_near)):
                src = near + 4 * shift
                wait = functools.partial(self.arrived, src, way, self.turn(g.z + shift, way))
                wait() if cond is None else pl.when(cond)(wait)
                self.forward(cond, src, way, target, 1, 4 * self.nz)

    def rest(self):
        self.remote(self.total(2 * self.nz), self.g.me, 0, 4 * self.nz).wait_recv()

    def drain(self):
        if self.nz > 1:
            self.remote(self.total(self.nz - 1), self.g.me, 0, 0).wait_send()
        self.remote(self.total(3 * self.nz), self.g.me, 1, 0).wait_send()


class Place:
    def __init__(self, n):
        self.nz = n // 4
        self.me = lax.axis_index("dp")
        self.section = lax.axis_index("section")
        me = self.me
        self.x_near = me + 1 - 2 * (me % 2)
        self.y_near = me + 2 - 4 * ((me // 2) % 2)
        self.diagonal = self.x_near + self.y_near - me
        self.z = me // 4
        self.place = me % 4
        self.up, self.down = self.z + 1 < self.nz, self.z >= 1
        self.plane = (me, self.x_near, self.y_near, self.diagonal)

    def sources(self, d):
        if d == 0:
            return [(0, None)]
        return [(-d, self.z >= d), (d, self.z + d < self.nz)]

    def reaches(self, way):
        z, nz = self.z, self.nz
        there = z + way
        when = (there >= 0) & (there < nz)
        if abs(way) > 1:
            when = when & ((z == 0) | (z == nz - 1) | ((there > 0) & (there < nz - 1)))
        return when

    def passes(self, shift):
        z, nz = self.z, self.nz
        if not 0 < abs(shift) < nz - 2:
            return None
        return (z == 1) & (z + shift < nz - 1) if shift > 0 else (z == nz - 2) & (z + shift > 0)


def norm_rows(x, gains):
    average = jnp.mean(x, -1, keepdims=True)
    centred = x - average
    inverse = lax.rsqrt(jnp.mean(centred * centred, -1, keepdims=True) + epsilon)
    return centred, inverse, centred * inverse * gains


def norm_tangent(t, centred, inverse, gains):
    dcentred = t - jnp.mean(t, -1, keepdims=True)
    dinverse = -(inverse * inverse * inverse) * jnp.mean(centred * dcentred, -1, keepdims=True)
    return (dcentred * inverse + centred * dinverse) * gains


def softmax(scores):
    e = jnp.exp(scores - jnp.max(scores, -1, keepdims=True))
    return e / jnp.sum(e, -1, keepdims=True)


def at_rows(i, count):
    return pl.ds(pl.multiple_of(i * count, count), count)


def first_norm(sizes, tok, gain, normed, slot):
    micro, toks, width, hd, tangents = sizes
    for b in range(micro):
        x = tok[slot, pl.ds(b * toks, toks), :].astype(F32)
        normed[at_rows(slot * micro + b, toks), :] = norm_rows(x, gain)[2].astype(BF16)


def first_attend(sizes, acc, att, slot, b):
    micro, toks, width, hd, tangents = sizes
    factor = HEAD ** (-0.5)
    part = 2 * HEAD
    streams = 1 + tangents
    even = lax.broadcasted_iota(jnp.int32, (toks, part), 1) < HEAD
    rows = at_rows(slot * micro + b, toks)
    q = acc[rows, pl.ds(0, part)]
    k = acc[rows, pl.ds(part, part)].astype(BF16)
    v = acc[rows, pl.ds(2 * part, streams * part)].astype(BF16)
    zero = jnp.zeros_like(q)
    both = jnp.concatenate([jnp.where(even, q, zero), jnp.where(even, zero, q)], 0).astype(BF16)
    scores = dot_t(both, k) * factor
    low = jnp.exp(scores - jnp.max(scores, -1, keepdims=True)).astype(BF16)
    out = dot(low, jnp.concatenate([v, jnp.ones((toks, part), BF16)], 1))

    def joined(s):
        at = slice(s * part, (s + 1) * part)
        return jnp.where(even, out[:toks, at], out[toks:, at])

    scale = 1.0 / joined(streams)
    for s in range(streams):
        att[slot, pl.ds((s * micro + b) * toks, toks), :] = (joined(s) * scale).astype(BF16)


def class_attend(sizes, acc):
    micro, toks, width, hd, tangents = sizes
    factor = HEAD ** (-0.5)
    part = 2 * HEAD
    streams = 1 + tangents
    images = acc.shape[0] // toks
    even = lax.broadcasted_iota(jnp.int32, (images, part), 1) < HEAD
    q = jnp.concatenate([acc[pl.ds(i * toks, 8), pl.ds(0, part)][:1] for i in range(images)], 0)
    zero = jnp.zeros_like(q)
    both = jnp.concatenate([jnp.where(even, q, zero), jnp.where(even, zero, q)], 0).astype(BF16)
    k = acc[:, pl.ds(part, part)].astype(BF16)
    v = acc[:, pl.ds(2 * part, streams * part)].astype(BF16)
    scores = dot_t(both, k) * factor
    image = lax.broadcasted_iota(jnp.int32, scores.shape, 0) % images
    own = lax.broadcasted_iota(jnp.int32, scores.shape, 1) // toks == image
    scores = jnp.where(own, scores, -jnp.inf)
    low = jnp.exp(scores - jnp.max(scores, -1, keepdims=True)).astype(BF16)
    out = dot(low, jnp.concatenate([v, jnp.ones((acc.shape[0], part), BF16)], 1))

    def joined(s):
        at = slice(s * part, (s + 1) * part)
        return jnp.where(even, out[:images, at], out[images:, at])

    scale = 1.0 / joined(streams)
    parts = [joined(s) * scale for s in range(streams)]
    blank = jnp.zeros((group_of(sizes) - micro * streams, part), F32)
    rows = []
    for p in range(images // micro):
        rows += [x[p * micro : (p + 1) * micro] for x in parts] + [blank] * (blank.shape[0] > 0)
    return jnp.concatenate(rows, 0).astype(BF16)


def first_out(sizes, tok, place, b_full, att, state):
    micro, toks, width, hd, tangents = sizes
    rows0 = micro * toks
    tile = 256
    for c in range(width // tile):
        at = pl.ds(c * tile, tile)
        out = dot_t(att[...], b_full[0, at, :])
        extra = [dot_t(att[pl.ds(0, rows0), :], b_full[1 + j, at, :]) for j in range(tangents)]
        x = tok[place, :, at].astype(F32)
        state[pl.ds(0, rows0), at] = (x + out[:rows0]).astype(BF16)
        for j in range(tangents):
            state[pl.ds((1 + j) * rows0, rows0), at] = (
                out[(1 + j) * rows0 : (2 + j) * rows0] + extra[j]
            ).astype(BF16)


def group_of(sizes):
    micro, toks, width, hd, tangents = sizes
    return -(-micro * (1 + tangents) // 8) * 8


def stream_of(sizes, shape):
    return (lax.broadcasted_iota(jnp.int32, shape, 0) % group_of(sizes)) // sizes[0]


def lowered(sizes, parts):
    micro, tangents = sizes[0], sizes[4]
    stream = stream_of(sizes, parts[0].shape)
    total = parts[0]
    for j in range(tangents):
        moved = pltpu.roll(parts[1 + j], micro * (1 + j), 0)
        total = total + jnp.where(stream == 1 + j, moved, jnp.zeros_like(moved))
    return total


def primal_rows(sizes, x):
    micro, tangents = sizes[0], sizes[4]
    stream = stream_of(sizes, x.shape)
    spread = x
    for j in range(tangents):
        spread = jnp.where(stream == 1 + j, pltpu.roll(x, micro * (1 + j), 0), spread)
    return spread


def norm_group(sizes, x, gains):
    stream = stream_of(sizes, x.shape)
    centred, inverse, y = norm_rows(primal_rows(sizes, x), gains)
    dy = norm_tangent(x, centred, inverse, gains)
    return jnp.where(stream == 0, y, dy).astype(BF16)


def class_rows(sizes, state):
    micro, toks, width, hd, tangents = sizes
    streams = 1 + tangents
    rows = [
        state[pl.ds((s * micro + b) * toks, 16), :].astype(F32)[:1] for s in range(streams) for b in range(micro)
    ]
    return jnp.concatenate(rows + [jnp.zeros((group_of(sizes) - micro * streams, width), F32)], 0)


def last_norm(sizes, gain, state, normed):
    micro, toks, width, hd, tangents = sizes
    rows0 = micro * toks
    for b in range(micro):
        at = pl.ds(b * toks, toks)
        centred, inverse, y = norm_rows(state[at, :].astype(F32), gain)
        normed[0, at, :] = y.astype(BF16)
        for j in range(tangents):
            t = state[pl.ds((1 + j) * rows0 + b * toks, toks), :].astype(F32)
            normed[1 + j, at, :] = norm_tangent(t, centred, inverse, gain).astype(BF16)


def last_attend(sizes, u, normed):
    micro, toks, width, hd, tangents = sizes
    factor = HEAD ** (-0.5)
    shape = (u.shape[0], micro * toks)
    stream = stream_of(sizes, shape)
    image = (lax.broadcasted_iota(jnp.int32, shape, 0) % group_of(sizes)) % micro
    valid = lax.broadcasted_iota(jnp.int32, shape, 1) // toks == image
    parts = [dot_t(u, normed[s]) * factor for s in range(1 + tangents)]
    probs = softmax(jnp.where(valid, parts[0], -jnp.inf))
    weights = primal_rows(sizes, probs)
    scores = lowered(sizes, parts)
    dprobs = weights * (scores - jnp.sum(weights * scores, -1, keepdims=True))
    zero = jnp.zeros_like(weights)
    total = dot(jnp.where(stream == 0, weights, dprobs).astype(BF16), normed[0])
    for j in range(tangents):
        total = total + dot(jnp.where(stream == 1 + j, weights, zero).astype(BF16), normed[1 + j])
    return total.astype(BF16)


TOK, TOKY, TOKD, LA, LB, ATT, ATC, CLS, U, M, O1, O0, GAIN, FIRST, EARLY, STAGES = range(16)


def kernel(
    n, sizes, tokens, w_qkv, tangent_value, w_out, t_out, gain_in, final_in, head_in, logit_ref,
    a_stage, b_stage, a0, a1, b1, b_full, tok, normed_all, acc, att_out, att_in, state, normed,
    gains, final_gain, head, atc_out, atc_all, atc_in, cls_out, cls_in, cls_all, u_out, u_all, m_out, m_all, o_out, o_all, classes,
    loads, line, a_send, a_recv, stage_send, stage_recv, far_send, far_recv, b_send, b_recv,
):
    micro, toks, width, hd, tangents = sizes
    streams = 1 + tangents
    part = hd // 4
    share = part // HEAD
    g = Place(n)
    me, section, place, z, nz = g.me, g.section, g.place, g.z, g.nz
    other = 1 - section
    rows = width // n
    slab = 4 * rows
    group = group_of(sizes)
    own = at_rows(me, rows)

    barrier = pltpu.get_barrier_semaphore()

    def greet(target, sec):
        pl.semaphore_signal(
            barrier, inc=1, device_id={"section": sec, "dp": target}, device_id_type=MESH
        )

    pl.when(g.up)(lambda: greet(me + 4, section))
    pl.when(g.down)(lambda: greet(me - 4, section))
    for near in (g.diagonal, g.x_near, g.y_near):
        greet(near, section)
        greet(near, other)
    greet(me, other)

    def met():
        if nz > 1:
            middle = g.up & g.down
            pl.when(middle)(lambda: pl.semaphore_wait(barrier, 9))
            pl.when(jnp.logical_not(middle))(lambda: pl.semaphore_wait(barrier, 8))
        else:
            pl.semaphore_wait(barrier, 7)

    def column(p):
        return pl.ds(p * part, part) if isinstance(p, int) else at_rows(p, part)

    def load(i, src, dst):
        return pltpu.make_async_copy(src, dst, loads.at[i])

    def stage_loads():
        for p in range(4):
            for m in range(3):
                load(5, w_qkv.at[:, pl.ds(m * hd + p * part, part)], a_stage.at[p, :, pl.ds(m * part, part)]).start()
            for j in range(tangents):
                load(
                    5,
                    tangent_value.at[j, :, pl.ds(p * part, part)],
                    a_stage.at[p, :, pl.ds((3 + j) * part, part)],
                ).start()

    def own_loads():
        for m in range(3):
            load(6, w_qkv.at[:, column(m * 4 + place)], a1.at[own, pl.ds(m * part, part)]).start()
        for j in range(tangents):
            load(6, tangent_value.at[j, :, column(place)], a1.at[own, pl.ds((3 + j) * part, part)]).start()
        load(7, w_out.at[:, column(place)], b1.at[0, own, :]).start()
        load(7, t_out.at[:, :, column(place)], b1.at[pl.ds(1, tangents), own, :]).start()
        for p in range(4):
            load(8, w_out.at[:, pl.ds(p * part, part)], b_stage.at[p, 0]).start()
            load(8, t_out.at[:, :, pl.ds(p * part, part)], b_stage.at[p, pl.ds(1, tangents)]).start()

    def b_loads():
        load(4, w_out, b_full.at[0, own, :]).start()
        load(4, t_out, b_full.at[pl.ds(1, tangents), own, :]).start()

    def loaded(i, ref):
        load(i, ref, ref).wait()

    def gain_load():
        return load(0, gain_in, gains.at[section])

    def tok_load():
        return load(1, tokens, tok.at[place])

    def tail_loads():
        return [load(2, head_in, head), load(3, final_in, final_gain)]

    stage_loads()
    gain_load().start()
    tok_load().start()
    pl.when(section == 0)(b_loads)
    pl.when(section == 1)(own_loads)
    for move in tail_loads():
        move.start()
    met()

    def tell(way, level, target):
        pl.semaphore_signal(
            line.at[way, level], inc=1, device_id={"section": section, "dp": target}, device_id_type=MESH
        )

    if nz > 2:

        @pl.when(g.up & g.down)
        def _():
            tell(0, 1, me + 4)
            tell(1, 1, me - 4)

    def far_met():
        for level in range(1, nz - 1):

            @pl.when(z - 1 - level >= 0)
            def _():
                pl.semaphore_wait(line.at[0, level], 1)
                if level + 1 < nz - 1:
                    pl.when(g.up)(lambda: tell(0, level + 1, me + 4))

            @pl.when(z + 1 + level < nz)
            def _():
                pl.semaphore_wait(line.at[1, level], 1)
                if level + 1 < nz - 1:
                    pl.when(g.down)(lambda: tell(1, level + 1, me - 4))


    def xfer(stage, src, dst, target, sec):
        return pltpu.make_async_remote_copy(
            src_ref=src,
            dst_ref=dst,
            send_sem=stage_send.at[stage],
            recv_sem=stage_recv.at[stage],
            device_id={"section": sec, "dp": target},
            device_id_type=MESH,
        )

    def arrived(stage, ref):
        xfer(stage, ref, ref, me, other).wait_recv()

    sent = []

    FAR = (3, 1, 2, 0)

    def scatter(stage, src, dst, sec, total, skip_own=False):
        for i in FAR:
            if i > 0 or not skip_own:
                target = g.plane[i]
                xfer(stage, src(target % 4), dst, target, sec).start()
        sent.append((stage, total))

    def drain():
        for stage, ref in sent:
            xfer(stage, ref, ref, me, other).wait_send()
        sent.clear()

    def a_ref(src):
        return a0.at[at_rows(src, rows), :]

    def a_copy(src_ref, src, sem, target, sec):
        return pltpu.make_async_remote_copy(
            src_ref=src_ref,
            dst_ref=a_ref(src),
            send_sem=sem,
            recv_sem=a_recv.at[src],
            device_id={"section": sec, "dp": target},
            device_id_type=MESH,
        )

    @pl.when(section == 0)
    def _():
        loaded(5, a_stage)
        for i in range(4):
            target = g.plane[i]
            a_copy(a_stage.at[target % 4], me, stage_send.at[FIRST], target, other).start()
        sent.append((FIRST, a_stage))
        gain_load().wait()
        xfer(GAIN, gains.at[section], gains.at[section], me, other).start()
        sent.append((GAIN, gains.at[section]))
        loaded(4, b_full.at[:, own, :])
        gather = Gather(n, g, b_full, b_send, b_recv)
        lag = 1
        gather.along(False)
        for d in range(nz + lag):
            if d < nz:
                gather.pass_on(d)
                gather.direct(d)
                if d == 0:
                    far_met()
                    gather.along(True)
            if d >= lag:
                gather.relay(d - lag)
        tok_load().wait()
        gather.rest()
        arrived(ATC, atc_in)
        cls_out[...] = lowered(sizes, [dot_t(atc_in[...], b_full[s]) for s in range(streams)])
        xfer(CLS, cls_out, cls_in, me, other).start()
        sent.append((CLS, cls_out))
        arrived(ATT, att_in)
        first_out(sizes, tok, place, b_full, att_in, state)
        arrived(GAIN, gains.at[other])
        last_norm(sizes, gains[1], state, normed)
        arrived(U, u_all)
        u = jnp.concatenate([u_all[p] for p in range(4)], 0)
        m = last_attend(sizes, u, normed)
        for p in range(4):
            m_out[p] = m[p * share * group : (p + 1) * share * group]
        scatter(M, lambda p: m_out.at[p], m_all.at[place], other, m_out)
        classes[...] = class_rows(sizes, state)
        gather.drain()
        drain()
        arrived(O0, o_all)

    @pl.when(section == 1)
    def _():
        gain_load().wait()
        xfer(GAIN, gains.at[section], gains.at[section], me, other).start()
        sent.append((GAIN, gains.at[section]))
        tok_load().wait()

        def relay(d, some=g.plane):
            for near in some:
                for shift, cond in g.sources(d)[::-1]:

                    def step():
                        src = near + 4 * shift
                        a_copy(a_ref(src), src, a_send.at[d, 0], me, section).wait_recv()
                        if shift >= 0 and d < nz - 1:
                            pl.when(g.down)(
                                lambda: a_copy(a_ref(src), src, a_send.at[d, 1], me - 4, section).start()
                            )
                        if shift <= 0 and d < nz - 1:
                            pl.when(g.up)(
                                lambda: a_copy(a_ref(src), src, a_send.at[d, 0], me + 4, section).start()
                            )

                    step() if cond is None else pl.when(cond)(step)

        def relay_end(d):
            slab_ref = a0.at[pl.ds(0, slab), :]
            for shift, cond in g.sources(d):

                def end(way):
                    pltpu.make_async_remote_copy(
                        src_ref=slab_ref,
                        dst_ref=slab_ref,
                        send_sem=a_send.at[d, way],
                        recv_sem=a_recv.at[0],
                        device_id={"section": section, "dp": me},
                        device_id_type=MESH,
                    ).wait_send()

                if shift <= 0:
                    pl.when(g.up if cond is None else cond & g.up)(functools.partial(end, 0))
                if shift >= 0:
                    pl.when(g.down if cond is None else cond & g.down)(functools.partial(end, 1))

        def project(d):
            for shift, cond in g.sources(d):

                def step(shift=shift):
                    at = at_rows(z + shift, slab)
                    term = dot(normed_all[:, at], a0[at, :])
                    acc[...] = term if d == 0 else acc[...] + term

                step() if cond is None else pl.when(cond)(step)

        loaded(7, b1.at[:, own, :])
        early = b1.at[:, pl.ds(0, (nz - 1) * rows), :]

        def ahead(k):
            for way in (k, -k):
                there = (z + way >= 0) & (z + way < nz)

                def go():
                    xfer(EARLY, b1.at[:, own, :], b1.at[:, own, :], me + 4 * way, section).start()

                pl.when(there)(go)

        if nz > 1:
            ahead(1)
        if nz > 1:
            sent.append((EARLY, early))
        relay(0, g.plane[:1])
        for stage, near in ((TOK, g.x_near), (TOKY, g.y_near)):
            xfer(stage, tok.at[place], tok.at[place], near, section).start()
            sent.append((stage, tok.at[place]))
        loaded(5, a_stage)
        loaded(6, a1.at[own, :])
        scatter(LA, lambda p: a_stage.at[p], a1.at[own, :], section, a_stage.at[pl.ds(0, 3)], True)
        far_met()
        for k in range(2, nz):
            ahead(k)
        relay(0, g.plane[1:])
        arrived(GAIN, gains.at[other])
        first_norm(sizes, tok, gains[0], normed_all, place)
        relay(1)
        half = micro * toks // 2
        for stage, near, target, first in ((TOK, g.x_near, g.y_near, 0), (TOKY, g.y_near, g.x_near, half)):
            arrived(stage, tok.at[near % 4])
            piece = tok.at[near % 4, pl.ds(first, half), :]
            xfer(TOKD, piece, piece, target, section).start()
        sent.append((TOKD, tok.at[0]))
        loaded(8, b_stage)
        scatter(LB, lambda p: b_stage.at[p], b1.at[:, own, :], section, b_stage.at[pl.ds(0, 3)], True)

        def far_refs(kind, zc):
            at = at_rows(zc, slab)
            if kind == 0:
                return [a1.at[at, pl.ds(0, 2 * part)]]
            if kind == 1:
                return [a1.at[at, pl.ds(2 * part, streams * part)]]
            return [b1.at[:, at_rows(near + 4 * (zc - z), rows), :] for near in g.plane[1:]]

        def far_total(kind):
            return far_refs(kind, 0)[0] if kind < 2 else b1.at[:, pl.ds(0, 3 * rows), :]

        def far_copy(ref, kind, zc, target):
            return pltpu.make_async_remote_copy(
                src_ref=ref,
                dst_ref=ref,
                send_sem=far_send.at[kind],
                recv_sem=far_recv.at[kind, zc],
                device_id={"section": section, "dp": target},
                device_id_type=MESH,
            )

        def far_moves(kind):
            for k in range(1, nz):
                for way in (k, -k):
                    yield g.reaches(way), None, z, me + 4 * way
            for k in range(1, nz - 2):
                for way in (k, -k):
                    yield g.passes(way), way, z + way, me - 4 if way > 0 else me + 4

        def far_start(kind):
            for when, way, zc, target in far_moves(kind):

                def go():
                    for ref in far_refs(kind, zc):
                        far_copy(ref, kind, zc, target).start()

                if way is None:
                    pl.when(when)(go)

        def far_pass(kind):
            for when, way, zc, target in far_moves(kind):

                def step():
                    far_copy(far_total(kind), kind, zc, me).wait_recv()
                    for ref in far_refs(kind, zc):
                        far_copy(ref, kind, zc, target).start()

                if way is not None:
                    pl.when(when)(step)

        def far_wait(kind):
            for k in range(1, nz):
                for way in (k, -k):
                    there = z + way
                    when = (there >= 0) & (there < nz)
                    if g.passes(way) is not None:
                        when = when & jnp.logical_not(g.passes(way))
                    pl.when(when)(lambda: far_copy(far_total(kind), kind, there, me).wait_recv())

        def far_end(kind):
            count = nz - 1
            if kind < 2:
                first, last = ((0, 2), (2, 2 + streams))[kind]
                ref = a1.at[pl.ds(0, count * slab), pl.ds(first * part, (last - first) * part)]
            else:
                ref = b1.at[:, pl.ds(0, count * 3 * rows), :]
            if count > 0:
                far_copy(ref, kind, 0, me).wait_send()

        def far_begin():
            arrived(LA, a1.at[pl.ds(0, 3 * rows), :])
            far_start(0)
            far_start(1)

        for near in (g.x_near, g.y_near):
            first_norm(sizes, tok, gains[0], normed_all, near % 4)
        for d in range(2, nz - 1):
            relay(d)
        far_begin()
        arrived(TOKD, tok.at[g.diagonal % 4])
        first_norm(sizes, tok, gains[0], normed_all, g.diagonal % 4)
        for d in range(nz - 1):
            project(d)
        if nz > 2:
            relay(nz - 1)
        project(nz - 1)
        atc_out[...] = class_attend(sizes, acc)
        scatter(ATC, lambda p: atc_out, atc_in.at[:, column(place)], other, atc_all)

        def give(i):
            target = g.plane[i]
            xfer(ATT, att_out.at[target % 4], att_in.at[:, column(place)], target, other).start()

        for i in FAR:
            for b in range(micro):
                first_attend(sizes, acc, att_out, g.plane[i] % 4, b)
            if i == FAR[0]:
                arrived(LB, b1.at[:, pl.ds(0, 3 * rows), :])
                far_start(2)
        far_pass(0)
        for i in FAR:
            give(i)
        sent.append((ATT, att_out))
        fresh = []
        blank = jnp.zeros((group - micro, width), F32)
        for p in range(4):
            fresh += [tok[p, pl.ds(b * toks, 16), :].astype(F32)[:1] for b in range(micro)] + [blank]
        fresh = jnp.concatenate(fresh, 0)
        far_wait(0)
        arrived(CLS, cls_in)
        x = (fresh + cls_in[...]).astype(BF16).astype(F32)
        for p in range(4):
            cls_all[p] = x[p * group : (p + 1) * group]
        q = dot(norm_group(sizes, x, gains[1]), a1[:, pl.ds(0, part)]).astype(BF16).astype(F32)
        owner = lax.broadcasted_iota(jnp.int32, (group, part), 1) // HEAD
        zero = jnp.zeros((group, part), F32)
        spread = [
            jnp.where(owner == h, q[p * group : (p + 1) * group], zero) for p in range(4) for h in range(share)
        ]
        u = dot_t(jnp.concatenate(spread, 0).astype(BF16), a1[:, pl.ds(part, part)]).astype(BF16)
        tall = share * group
        for p in range(4):
            u_out[p] = u[p * tall : (p + 1) * tall]
        scatter(U, lambda p: u_out.at[p], u_all.at[place], other, u_out)
        far_pass(1)
        far_pass(2)
        far_wait(1)
        arrived(M, m_all)
        m = jnp.concatenate([m_all[p] for p in range(4)], 0)
        r = dot(m, a1[:, pl.ds(2 * part, streams * part)])
        mixed = lowered(sizes, [r[:, s * part : (s + 1) * part] for s in range(streams)])
        chosen = []
        for p in range(4):
            block = zero
            for h in range(share):
                at = p * tall + h * group
                block = jnp.where(owner == h, mixed[at : at + group], block)
            chosen.append(block)
        attended = jnp.concatenate(chosen, 0).astype(BF16)
        far_wait(2)
        if nz > 1:
            arrived(EARLY, early)
        out = lowered(sizes, [dot_t(attended, b1[s]) for s in range(streams)])
        for p in range(4):
            o_out[p] = out[p * group : (p + 1) * group].astype(BF16)
        scatter(O0, lambda p: o_out.at[p], o_all.at[place], other, o_out)
        scatter(O1, lambda p: o_out.at[p], o_all.at[place], section, o_out.at[pl.ds(0, 3)], True)
        o_all[place] = o_out[place]
        classes[...] = cls_all[place]
        for d in range(nz - 1):
            relay_end(d)
        for kind in range(3):
            far_end(kind)
        drain()
        arrived(O1, o_all.at[pl.ds(0, 3)])

    for move in tail_loads():
        move.wait()
    total = sum(o_all[p].astype(F32) for p in range(4))
    final = (classes[...] + total).astype(BF16).astype(F32)
    features = norm_group(sizes, final, final_gain[...])
    logits = dot_t(features, head[...])
    for s in range(streams):
        logit_ref[s, :, 0, :] = logits[s * micro : (s + 1) * micro]


def two_sections(n):
    def shards(tokens, w_qkv, w_output, tangent_value, tangent_output, layer_gain, final_gain, head):
        micro, _, toks, width = tokens.shape
        tangents = tangent_value.shape[1]
        hd = w_output.shape[1]
        count = head.shape[1]
        rows = width // n
        part = hd // 4
        nz = n // 4
        sizes = (micro, toks, width, hd, tangents)
        streams = 1 + tangents
        rows0 = micro * toks
        group = group_of(sizes)
        tall = part // HEAD * group
        vmem = pl.BlockSpec(memory_space=pltpu.VMEM)
        anywhere = pl.BlockSpec(memory_space=pl.ANY)
        dma = pltpu.SemaphoreType.DMA
        logits = pl.pallas_call(
            functools.partial(kernel, n, sizes),
            out_shape=pltpu.VMEM((streams, micro, 1, count), F32),
            in_specs=[anywhere] * 8,
            out_specs=vmem,
            scratch_shapes=[
                pltpu.VMEM((4, rows, (2 + streams) * part), BF16),
                pltpu.VMEM((4, streams, rows, part), BF16),
                pltpu.VMEM((width, (2 + streams) * part), BF16),
                pltpu.VMEM((width, (2 + streams) * part), BF16),
                pltpu.VMEM((streams, width, part), BF16),
                pltpu.VMEM((streams, width, hd), BF16),
                pltpu.VMEM((4, rows0, width), BF16),
                pltpu.VMEM((4 * rows0, width), BF16),
                pltpu.VMEM((4 * rows0, (2 + streams) * part), F32),
                pltpu.VMEM((4, streams * rows0, part), BF16),
                pltpu.VMEM((streams * rows0, hd), BF16),
                pltpu.VMEM((streams * rows0, width), BF16),
                pltpu.VMEM((streams, rows0, width), BF16),
                pltpu.VMEM((2, 1, width), F32),
                pltpu.VMEM((1, width), F32),
                pltpu.VMEM((count, width), BF16),
                pltpu.VMEM((4 * group, part), BF16),
                pltpu.VMEM((16 * group, part), BF16),
                pltpu.VMEM((4 * group, hd), BF16),
                pltpu.VMEM((4 * group, width), F32),
                pltpu.VMEM((4 * group, width), F32),
                pltpu.VMEM((4, group, width), F32),
                pltpu.VMEM((4, tall, width), BF16),
                pltpu.VMEM((4, tall, width), BF16),
                pltpu.VMEM((4, tall, width), BF16),
                pltpu.VMEM((4, tall, width), BF16),
                pltpu.VMEM((4, group, width), BF16),
                pltpu.VMEM((4, group, width), BF16),
                pltpu.VMEM((group, width), F32),
                dma((9,)),
                pltpu.SemaphoreType.REGULAR((2, max(nz - 1, 1))),
                dma((nz, 2)),
                dma((n,)),
                dma((STAGES,)),
                dma((STAGES,)),
                dma((3,)),
                dma((3, nz)),
                dma((2,)),
                dma((4 * nz + 1,)),
            ],
            compiler_params=pltpu.CompilerParams(
                collective_id=0, has_side_effects=True, vmem_limit_bytes=63 * 2**20
            ),
        )(
            tokens.reshape(rows0, width),
            w_qkv[0],
            tangent_value[0],
            jnp.swapaxes(w_output[0], 0, 1),
            jnp.swapaxes(tangent_output[0], 1, 2),
            layer_gain,
            final_gain[None],
            head.T,
        )
        return logits[0], sum(logits[1 + j] * logits[1 + j] for j in range(tangents))

    return shards


def solution(mesh):
    n = mesh.shape["dp"]
    fast = mesh.shape["section"] == 2 and n % 4 == 0 and n // 4 <= 4
    return jax.shard_map(
        two_sections(n) if fast else relay_shards,
        mesh=mesh,
        in_specs=(
            P(None, "dp", None, None),
            P("section", "dp", None),
            P("section", None, "dp"),
            P("section", None, "dp", None),
            P("section", None, None, "dp"),
            P("section", None),
            P(),
            P(None, "section"),
        ),
        out_specs=(P(None, "dp", "section"), P(None, "dp", "section")),
        check_vma=False,
    )
```
